8 devices in a mesh: dp: 1 (over z), cp: 8 (over y, x, core).
Axes of the slice: x: 2, y: 2, z: 1, core: 2. Of those that a mesh axis runs over, the one named last changes fastest.
Arguments:
- x_in: bfloat16 [512, 3584], P(('dp', 'cp'))
- cache_k1: bfloat16 [16384, 4, 128], P(('dp', 'cp'))
- cache_v1: bfloat16 [16384, 4, 128], P(('dp', 'cp'))
- w_q1: bfloat16 [3584, 3584], replicated
- b_q1: bfloat16 [3584], replicated
- w_k1: bfloat16 [3584, 512], replicated
- b_k1: bfloat16 [512], replicated
- w_v1: bfloat16 [3584, 512], replicated
- w_o1: bfloat16 [3584, 3584], replicated
- w_gate: bfloat16 [3584, 18944], replicated
- w_up: bfloat16 [3584, 18944], replicated
- w_down: bfloat16 [18944, 3584], replicated
- cache_k2: bfloat16 [16384, 4, 128], P(('dp', 'cp'))
- cache_v2: bfloat16 [16384, 4, 128], P(('dp', 'cp'))
- w_q2: bfloat16 [3584, 3584], replicated
- b_q2: bfloat16 [3584], replicated
- w_k2: bfloat16 [3584, 512], replicated
- b_k2: bfloat16 [512], replicated
- w_v2: bfloat16 [3584, 512], replicated
- w_o2: bfloat16 [3584, 3584], replicated
Outputs:
- output 1: bfloat16 [512, 3584], P(('dp', 'cp'))
- output 2: bfloat16 [512, 3584], P(('dp', 'cp'))
- output 3: bfloat16 [512, 4, 128], P(('dp', 'cp'))
- output 4: bfloat16 [512, 4, 128], P(('dp', 'cp'))
- output 5: bfloat16 [512, 4, 128], P(('dp', 'cp'))
- output 6: bfloat16 [512, 4, 128], P(('dp', 'cp'))
All inputs are finite; a program needn't handle non-finite values.
Results may differ from the reference program's by a relative error of at most 0.0144252.
Values are sent between devices in bfloat16 or wider.
A program may use at most 2 GiB of HBM per device.

```python
import math
import jax
import jax.numpy as jnp
from jax import lax

D_MODEL = 3584
HEADS = 28
KV_HEADS = 4
HEAD = 128
FF = 18944
CHUNK = 512
CACHE = 16384
SHARDS = 8
QBLK = 64

GROUP = HEADS // KV_HEADS
SHARD_LEN = CACHE // SHARDS


def draw_matrix(key, rows, cols):
    return (jax.random.normal(key, (rows, cols), jnp.float32) * rows ** -0.5).astype(jnp.bfloat16)


def draw_cache(key_k, key_s, key_v, key_m):
    shard_scale = jax.random.uniform(key_s, (SHARDS, 1, 1, 1), jnp.float32, 0.6, 1.6)
    cache_keys = jax.random.normal(key_k, (SHARDS, SHARD_LEN, KV_HEADS, HEAD), jnp.float32) * shard_scale
    shard_mean = jax.random.normal(key_m, (SHARDS, 1, KV_HEADS, HEAD), jnp.float32)
    cache_vals = 0.5 * jax.random.normal(key_v, (SHARDS, SHARD_LEN, KV_HEADS, HEAD), jnp.float32) + shard_mean
    return (cache_keys.reshape(CACHE, KV_HEADS, HEAD).astype(jnp.bfloat16),
            cache_vals.reshape(CACHE, KV_HEADS, HEAD).astype(jnp.bfloat16))


def draw_bias(key_dir, key_q, key_k):
    half_dim = HEAD // 2
    lane_idx = jnp.arange(HEAD) % half_dim
    low_mask = (lane_idx >= (7 * half_dim) // 8).astype(jnp.float32)
    raw_dir = jax.random.normal(key_dir, (KV_HEADS, HEAD), jnp.float32) * low_mask
    unit_dir = raw_dir / jnp.sqrt(jnp.sum(raw_dir * raw_dir, axis=-1, keepdims=True))
    mean_score = max(math.log(CACHE / CHUNK) + 0.5, 0.5)
    bias_amp = math.sqrt(mean_score * math.sqrt(HEAD))
    jitter_q = jax.random.uniform(key_q, (HEADS, 1), jnp.float32, 0.9, 1.1)
    jitter_k = jax.random.uniform(key_k, (KV_HEADS, 1), jnp.float32, 0.9, 1.1)
    bias_q = bias_amp * jnp.repeat(unit_dir, GROUP, axis=0) * jitter_q
    bias_k = bias_amp * unit_dir * jitter_k
    return (bias_q.reshape(HEADS * HEAD).astype(jnp.bfloat16),
            bias_k.reshape(KV_HEADS * HEAD).astype(jnp.bfloat16))


def setup_inputs(seed: int = 0, part: int = 0) -> dict:
    shared_root, part_root = jax.random.split(jax.random.key(seed))
    part_keys = jax.random.split(jax.random.fold_in(part_root, part), 9)
    weight_keys = jax.random.split(shared_root, 17)
    x_in = jax.random.normal(part_keys[0], (CHUNK, D_MODEL), jnp.float32).astype(jnp.bfloat16)
    cache_k1, cache_v1 = draw_cache(part_keys[1], part_keys[2], part_keys[3], part_keys[4])
    cache_k2, cache_v2 = draw_cache(part_keys[5], part_keys[6], part_keys[7], part_keys[8])
    b_q1, b_k1 = draw_bias(weight_keys[0], weight_keys[1], weight_keys[2])
    b_q2, b_k2 = draw_bias(weight_keys[3], weight_keys[4], weight_keys[5])
    return {
        'x_in': x_in,
        'cache_k1': cache_k1,
        'cache_v1': cache_v1,
        'w_q1': draw_matrix(weight_keys[6], D_MODEL, HEADS * HEAD),
        'b_q1': b_q1,
        'w_k1': draw_matrix(weight_keys[7], D_MODEL, KV_HEADS * HEAD),
        'b_k1': b_k1,
        'w_v1': draw_matrix(weight_keys[8], D_MODEL, KV_HEADS * HEAD),
        'w_o1': draw_matrix(weight_keys[9], HEADS * HEAD, D_MODEL),
        'w_gate': draw_matrix(weight_keys[10], D_MODEL, FF),
        'w_up': draw_matrix(weight_keys[11], D_MODEL, FF),
        'w_down': draw_matrix(weight_keys[12], FF, D_MODEL),
        'cache_k2': cache_k2,
        'cache_v2': cache_v2,
        'w_q2': draw_matrix(weight_keys[13], D_MODEL, HEADS * HEAD),
        'b_q2': b_q2,
        'w_k2': draw_matrix(weight_keys[14], D_MODEL, KV_HEADS * HEAD),
        'b_k2': b_k2,
        'w_v2': draw_matrix(weight_keys[15], D_MODEL, KV_HEADS * HEAD),
        'w_o2': draw_matrix(weight_keys[16], HEADS * HEAD, D_MODEL),
    }


def rms_norm(vals):
    wide = vals.astype(jnp.float32)
    return (wide * lax.rsqrt(jnp.mean(wide * wide, axis=-1, keepdims=True) + 1e-5)).astype(jnp.bfloat16)


def rope_tables(positions):
    half_dim = HEAD // 2
    inv_freq = 1.0 / (500000.0 ** (jnp.arange(half_dim, dtype=jnp.float32) * (2.0 / HEAD)))
    angles = positions.astype(jnp.float32)[:, None] * inv_freq[None, :]
    return jnp.cos(angles)[:, None, :], jnp.sin(angles)[:, None, :]


def apply_rope(vals, cos_t, sin_t):
    half_dim = HEAD // 2
    first = vals[..., :half_dim]
    second = vals[..., half_dim:]
    return jnp.concatenate([first * cos_t - second * sin_t, second * cos_t + first * sin_t], axis=-1)


def attention_layer(layer_in, cache_k, cache_v, w_q, b_q, w_k, b_k, w_v, w_o):
    cos_t, sin_t = rope_tables(CACHE + jnp.arange(CHUNK))
    q_pre = (jnp.dot(layer_in, w_q, preferred_element_type=jnp.float32) + b_q.astype(jnp.float32)).astype(jnp.bfloat16)
    k_pre = (jnp.dot(layer_in, w_k, preferred_element_type=jnp.float32) + b_k.astype(jnp.float32)).astype(jnp.bfloat16)
    v_new = jnp.dot(layer_in, w_v, preferred_element_type=jnp.float32).astype(jnp.bfloat16).reshape(CHUNK, KV_HEADS, HEAD)
    q_rot = apply_rope(q_pre.reshape(CHUNK, HEADS, HEAD).astype(jnp.float32), cos_t, sin_t).astype(jnp.bfloat16)
    k_new = apply_rope(k_pre.reshape(CHUNK, KV_HEADS, HEAD).astype(jnp.float32), cos_t, sin_t).astype(jnp.bfloat16)
    keys_all = jnp.concatenate([cache_k, k_new], axis=0).astype(jnp.float32)
    vals_all = jnp.concatenate([cache_v, v_new], axis=0).astype(jnp.float32)
    key_pos = jnp.arange(CACHE + CHUNK)
    scale = HEAD ** -0.5
    q_blocks = q_rot.reshape(CHUNK // QBLK, QBLK, KV_HEADS, GROUP, HEAD)
    starts = jnp.arange(CHUNK // QBLK) * QBLK

    def one_block(blk_in):
        q_blk, start = blk_in
        scores = jnp.einsum('tkgd,skd->tkgs', q_blk.astype(jnp.float32), keys_all) * scale
        q_pos = CACHE + start + jnp.arange(QBLK)
        visible = key_pos[None, :] <= q_pos[:, None]
        scores = jnp.where(visible[:, None, None, :], scores, -jnp.inf)
        peak = jnp.max(scores, axis=-1, keepdims=True)
        prob_w = jnp.exp(scores - peak)
        total = jnp.sum(prob_w, axis=-1, keepdims=True)
        summed = jnp.einsum('tkgs,skd->tkgd', prob_w.astype(jnp.bfloat16).astype(jnp.float32), vals_all)
        return summed / total

    o_all = lax.map(one_block, (q_blocks, starts))
    o_half = o_all.reshape(CHUNK, HEADS * HEAD).astype(jnp.bfloat16)
    y_out = jnp.dot(o_half, w_o, preferred_element_type=jnp.float32).astype(jnp.bfloat16)
    return y_out, k_new, v_new


def reference(x_in, cache_k1, cache_v1, w_q1, b_q1, w_k1, b_k1, w_v1, w_o1, w_gate, w_up, w_down, cache_k2, cache_v2, w_q2, b_q2, w_k2, b_k2, w_v2, w_o2):
    y_one, k_one, v_one = attention_layer(x_in, cache_k1, cache_v1, w_q1, b_q1, w_k1, b_k1, w_v1, w_o1)
    resid_h = (x_in.astype(jnp.float32) + y_one.astype(jnp.float32)).astype(jnp.bfloat16)
    normed = rms_norm(resid_h)
    gate_act = jnp.dot(normed, w_gate, preferred_element_type=jnp.float32).astype(jnp.bfloat16)
    up_proj = jnp.dot(normed, w_up, preferred_element_type=jnp.float32).astype(jnp.bfloat16)
    mixed = (jax.nn.silu(gate_act.astype(jnp.float32)) * up_proj.astype(jnp.float32)).astype(jnp.bfloat16)
    hidden = (resid_h.astype(jnp.float32) + jnp.dot(mixed, w_down, preferred_element_type=jnp.float32)).astype(jnp.bfloat16)
    y_two, k_two, v_two = attention_layer(rms_norm(hidden), cache_k2, cache_v2, w_q2, b_q2, w_k2, b_k2, w_v2, w_o2)
    return (hidden, y_two, k_one, v_one, k_two, v_two)
```

```python
import functools

import jax
import jax.numpy as jnp
from jax import lax
from jax.experimental import pallas as pl
from jax.experimental.pallas import tpu as pltpu
from jax.sharding import PartitionSpec as P

ROPE_THETA = 500000.0
NORM_EPS = 1e-5
LOG2E = 1.4426950408889634
KV_HEADS = 4
HEAD = 128
GROUP = 7
CHIPS = 4
FF_BLK = 256


def rms_norm(vals):
    wide = vals.astype(jnp.float32)
    return (wide * lax.rsqrt(jnp.mean(wide * wide, axis=-1, keepdims=True) + NORM_EPS)).astype(jnp.bfloat16)


def rope_tables(positions, head_dim):
    half_dim = head_dim // 2
    inv_freq = 1.0 / (ROPE_THETA ** (jnp.arange(half_dim, dtype=jnp.float32) * (2.0 / head_dim)))
    angles = positions.astype(jnp.float32)[:, None] * inv_freq[None, :]
    return jnp.cos(angles)[:, None, :], jnp.sin(angles)[:, None, :]


def apply_rope(vals, cos_t, sin_t):
    half_dim = vals.shape[-1] // 2
    first = vals[..., :half_dim]
    second = vals[..., half_dim:]
    return jnp.concatenate([first * cos_t - second * sin_t, second * cos_t + first * sin_t], axis=-1)


def project_rows(layer_in, w_q, b_q, w_k, b_k, w_v, cos_t, sin_t):
    rows = layer_in.shape[0]
    q_pre = (jnp.dot(layer_in, w_q, preferred_element_type=jnp.float32) + b_q.astype(jnp.float32)).astype(jnp.bfloat16)
    k_pre = (jnp.dot(layer_in, w_k, preferred_element_type=jnp.float32) + b_k.astype(jnp.float32)).astype(jnp.bfloat16)
    v_new = jnp.dot(layer_in, w_v, preferred_element_type=jnp.float32).astype(jnp.bfloat16).reshape(rows, -1, HEAD)
    q_rot = apply_rope(q_pre.reshape(rows, -1, HEAD).astype(jnp.float32), cos_t, sin_t).astype(jnp.bfloat16)
    k_new = apply_rope(k_pre.reshape(rows, -1, HEAD).astype(jnp.float32), cos_t, sin_t).astype(jnp.bfloat16)
    return q_rot, k_new, v_new


def chip_perm(step):
    return [(j, j ^ (2 * step)) for j in range(2 * CHIPS)]


PAIR_PERM = [(j, j ^ 1) for j in range(2 * CHIPS)]


def take_head(arr, idx):
    return lax.dynamic_index_in_dim(arr, idx, axis=0, keepdims=False)


def reshard_cache(cache_k, cache_v, chip):
    k_heads = jnp.transpose(cache_k, (1, 0, 2))
    v_heads = jnp.transpose(cache_v, (1, 2, 0))
    keys, vals = [take_head(k_heads, chip)], [take_head(v_heads, chip)]
    for step in range(1, CHIPS):
        keys.append(lax.ppermute(take_head(k_heads, chip ^ step), 'cp', chip_perm(step)))
        vals.append(lax.ppermute(take_head(v_heads, chip ^ step), 'cp', chip_perm(step)))
    all_k, all_v = [], []
    for step in range(CHIPS):
        all_k += [keys[step], lax.ppermute(keys[step], 'cp', PAIR_PERM)]
        all_v += [vals[step], lax.ppermute(vals[step], 'cp', PAIR_PERM)]
    return all_k, all_v


def exchange_rows(msgs, chip):
    got = [take_head(msgs, chip)]
    for step in range(1, CHIPS):
        got.append(lax.ppermute(take_head(msgs, chip ^ step), 'cp', chip_perm(step)))
    return jnp.stack(got)


def attend_kernel(n_chunks, pos_ref, q_ref, *refs):
    k_hbm = refs[:n_chunks]
    v_hbm = refs[n_chunks:2 * n_chunks]
    newk_ref, newv_ref, o_ref = refs[2 * n_chunks:2 * n_chunks + 3]
    kbuf, vbuf, qt, s_even, s_odd, m_even, m_odd, acc, m_run, l_run, sem = refs[2 * n_chunks + 3:]
    scale2 = HEAD ** -0.5 * LOG2E
    chunk = kbuf.shape[1]
    rows = qt.shape[2]
    n_items = n_chunks * GROUP

    for j in range(n_chunks):
        pltpu.make_async_copy(k_hbm[j], kbuf.at[j], sem.at[0, j]).start()
        pltpu.make_async_copy(v_hbm[j], vbuf.at[j], sem.at[1, j]).start()
    for g in range(GROUP):
        qt[g] = q_ref[:, g * HEAD:(g + 1) * HEAD].T
    acc[...] = jnp.zeros_like(acc)
    m_run[...] = jnp.full_like(m_run, -1e30)
    l_run[...] = jnp.zeros_like(l_run)

    def wait_chunk(j):
        pltpu.make_async_copy(kbuf.at[j], kbuf.at[j], sem.at[0, j]).wait()
        pltpu.make_async_copy(vbuf.at[j], vbuf.at[j], sem.at[1, j]).wait()

    def score(item, s_dst, m_dst):
        j, g = item // GROUP, item % GROUP
        part = jnp.full((8, rows), -jnp.inf, jnp.float32)
        for t in range(chunk // 256):
            s_blk = jnp.dot(kbuf[j, t * 256:(t + 1) * 256, :], qt[g], preferred_element_type=jnp.float32)
            s_dst[t * 256:(t + 1) * 256, :] = s_blk
            part = jnp.maximum(part, jnp.max(s_blk.reshape(32, 8, rows), axis=0))
        m_dst[...] = part

    def absorb(item, s_src, m_src):
        j, g = item // GROUP, item % GROUP
        m_old = m_run[g]
        m_new = jnp.maximum(m_old, jnp.max(m_src[...], axis=0, keepdims=True))
        alpha = jnp.exp2((m_old - m_new) * scale2)
        shift = m_new * scale2
        l_part = jnp.zeros((8, rows), jnp.float32)
        out = jnp.zeros((HEAD, rows), jnp.float32)
        for t in range(chunk // 256):
            p = jnp.exp2(s_src[t * 256:(t + 1) * 256, :] * scale2 - shift)
            l_part = l_part + jnp.sum(p.reshape(32, 8, rows), axis=0)
            out = out + jnp.dot(vbuf[j, :, t * 256:(t + 1) * 256], p.astype(jnp.bfloat16),
                                preferred_element_type=jnp.float32)
        acc[g] = acc[g] * alpha + out
        l_run[g] = l_run[g] * alpha + l_part
        m_run[g] = m_new

    wait_chunk(0)
    score(0, s_even, m_even)

    def pair(i, carry):
        first = 2 * i
        nxt = first + 2

        @pl.when((first + 1) % GROUP == 0)
        def _():
            wait_chunk((first + 1) // GROUP)

        @pl.when((nxt % GROUP == 0) & (nxt < n_items))
        def _():
            wait_chunk(nxt // GROUP)

        score(first + 1, s_odd, m_odd)
        absorb(first, s_even, m_even)
        score(jnp.minimum(nxt, n_items - 1), s_even, m_even)
        absorb(first + 1, s_odd, m_odd)
        return carry

    lax.fori_loop(0, n_items // 2, pair, 0)

    chip = pos_ref[0]
    core = pos_ref[1]
    new_len = newk_ref.shape[0]
    key_i = lax.broadcasted_iota(jnp.int32, (new_len, rows), 0)
    qry_i = lax.broadcasted_iota(jnp.int32, (new_len, rows), 1)
    blk = key_i // 64
    k_pos = (2 * (chip ^ (blk % CHIPS)) + (core ^ (blk // CHIPS))) * 64 + key_i % 64
    q_pos = (2 * (chip ^ (qry_i // 64)) + core) * 64 + qry_i % 64
    visible = k_pos <= q_pos

    def tail(g, carry):
        s = jnp.dot(newk_ref[...], qt[g], preferred_element_type=jnp.float32)
        s = jnp.where(visible, s, -jnp.inf)
        m_old = m_run[g]
        m_new = jnp.maximum(m_old, jnp.max(s, axis=0, keepdims=True))
        alpha = jnp.exp2((m_old - m_new) * scale2)
        p = jnp.exp2(s * scale2 - m_new * scale2)
        total = jnp.sum(l_run[g] * alpha, axis=0, keepdims=True) + jnp.sum(p, axis=0, keepdims=True)
        out = acc[g] * alpha + jnp.dot(newv_ref[...], p.astype(jnp.bfloat16), preferred_element_type=jnp.float32)
        acc[g] = out / total
        return carry

    lax.fori_loop(0, GROUP, tail, 0)
    for g in range(GROUP):
        o_ref[:, g * HEAD:(g + 1) * HEAD] = acc[g].T.astype(jnp.bfloat16)


def attend(pos, q_all, keys, vals, new_k, new_vt):
    n_chunks = len(keys)
    rows = q_all.shape[0]
    chunk = keys[0].shape[0]
    vmem = pl.BlockSpec(memory_space=pltpu.VMEM)
    hbm = pl.BlockSpec(memory_space=pl.ANY)
    n_keys = n_chunks * chunk + new_k.shape[0]
    return pl.pallas_call(
        functools.partial(attend_kernel, n_chunks),
        out_shape=jax.ShapeDtypeStruct((rows, GROUP * HEAD), jnp.bfloat16),
        in_specs=[pl.BlockSpec(memory_space=pltpu.SMEM), vmem] + [hbm] * (2 * n_chunks) + [vmem, vmem],
        out_specs=vmem,
        scratch_shapes=[
            pltpu.VMEM((n_chunks, chunk, HEAD), jnp.bfloat16),
            pltpu.VMEM((n_chunks, HEAD, chunk), jnp.bfloat16),
            pltpu.VMEM((GROUP, HEAD, rows), jnp.bfloat16),
            pltpu.VMEM((chunk, rows), jnp.float32),
            pltpu.VMEM((chunk, rows), jnp.float32),
            pltpu.VMEM((8, rows), jnp.float32),
            pltpu.VMEM((8, rows), jnp.float32),
            pltpu.VMEM((GROUP, HEAD, rows), jnp.float32),
            pltpu.VMEM((GROUP, 1, rows), jnp.float32),
            pltpu.VMEM((GROUP, 8, rows), jnp.float32),
            pltpu.SemaphoreType.DMA((2, n_chunks)),
        ],
        compiler_params=pltpu.CompilerParams(vmem_limit_bytes=40 * 1024 * 1024),
        cost_estimate=pl.CostEstimate(flops=4 * rows * GROUP * HEAD * n_keys,
                                      bytes_accessed=n_keys * HEAD * 4,
                                      transcendentals=rows * GROUP * n_keys),
        name="attend",
    )(pos, q_all, *keys, *vals, new_k, new_vt)


def mlp_kernel(core_ref, u_ref, gate_ref, up_ref, down_ref, out_ref):
    gate = jnp.dot(u_ref[...], gate_ref[...], preferred_element_type=jnp.float32).astype(jnp.bfloat16).astype(jnp.float32)
    up = jnp.dot(u_ref[...], up_ref[...], preferred_element_type=jnp.float32).astype(jnp.bfloat16).astype(jnp.float32)
    mixed = (gate * jax.nn.sigmoid(gate) * up).astype(jnp.bfloat16)
    part = jnp.dot(mixed, down_ref[...], preferred_element_type=jnp.float32)

    @pl.when(pl.program_id(0) == 0)
    def _():
        out_ref[...] = part

    @pl.when(pl.program_id(0) > 0)
    def _():
        out_ref[...] += part


def mlp_partial(core, normed, w_gate, w_up, w_down):
    rows, width = normed.shape
    ff = w_gate.shape[1]
    steps = ff // 2 // FF_BLK
    return pl.pallas_call(
        mlp_kernel,
        out_shape=jax.ShapeDtypeStruct((rows, width), jnp.float32),
        grid_spec=pltpu.PrefetchScalarGridSpec(
            num_scalar_prefetch=1,
            grid=(steps,),
            in_specs=[
                pl.BlockSpec((rows, width), lambda i, core: (0, 0)),
                pl.BlockSpec((width, FF_BLK), lambda i, core: (0, core[0] * steps + i)),
                pl.BlockSpec((width, FF_BLK), lambda i, core: (0, core[0] * steps + i)),
                pl.BlockSpec((FF_BLK, width), lambda i, core: (core[0] * steps + i, 0)),
            ],
            out_specs=pl.BlockSpec((rows, width), lambda i, core: (0, 0)),
        ),
        compiler_params=pltpu.CompilerParams(dimension_semantics=("arbitrary",), vmem_limit_bytes=40 * 1024 * 1024),
        cost_estimate=pl.CostEstimate(flops=3 * rows * width * ff, bytes_accessed=3 * width * ff, transcendentals=0),
        name="mlp_partial",
    )(core[None], normed, w_gate, w_up, w_down)


def attention_layer(layer_in, keys, vals, chip, core, weights, tables):
    w_q, b_q, w_k, b_k, w_v, w_o = weights
    tok = layer_in.shape[0]
    q_rot, k_new, v_new = project_rows(layer_in, w_q, b_q, w_k, b_k, w_v, *tables)
    q_msg = q_rot.reshape(tok, KV_HEADS, GROUP * HEAD)
    msgs = jnp.transpose(jnp.concatenate([q_msg, k_new, v_new], axis=-1), (1, 0, 2))
    got = exchange_rows(msgs, chip).reshape(CHIPS * tok, -1)
    q_all = got[:, :GROUP * HEAD]
    kv_mine = got[:, GROUP * HEAD:]
    kv_all = jnp.concatenate([kv_mine, lax.ppermute(kv_mine, 'cp', PAIR_PERM)], axis=0)
    pos = jnp.stack([chip, core]).astype(jnp.int32)
    o_mine = attend(pos, q_all, keys, vals, kv_all[:, :HEAD], kv_all[:, HEAD:].T)
    o_msgs = o_mine.reshape(CHIPS, tok, GROUP * HEAD)
    parts = [o_msgs[0]]
    for step in range(1, CHIPS):
        parts.append(lax.ppermute(o_msgs[step], 'cp', chip_perm(step)))
    by_step = jnp.stack(parts)
    ordered = jnp.concatenate([take_head(by_step, chip ^ c) for c in range(CHIPS)], axis=-1)
    y_out = jnp.dot(ordered, w_o, preferred_element_type=jnp.float32).astype(jnp.bfloat16)
    return y_out, k_new, v_new


def solution(mesh):
    axis_size = mesh.shape['cp']
    rows_spec = P(('dp', 'cp'), None)
    cache_spec = P(('dp', 'cp'), None, None)
    mat_spec = P(None, None)
    vec_spec = P(None)
    layer_specs = (cache_spec, cache_spec, mat_spec, vec_spec, mat_spec, vec_spec, mat_spec, mat_spec)
    in_specs = (rows_spec,) + layer_specs + (mat_spec, mat_spec, mat_spec) + layer_specs
    out_specs = (rows_spec, rows_spec, cache_spec, cache_spec, cache_spec, cache_spec)

    def forward(x_in, cache_k1, cache_v1, w_q1, b_q1, w_k1, b_k1, w_v1, w_o1, w_gate, w_up, w_down, cache_k2, cache_v2, w_q2, b_q2, w_k2, b_k2, w_v2, w_o2):
        me = lax.axis_index('cp')
        chip, core = me // 2, me % 2
        tok = x_in.shape[0]
        positions = axis_size * cache_k1.shape[0] + me * tok + jnp.arange(tok)
        tables = rope_tables(positions, HEAD)
        keys1, vals1 = reshard_cache(cache_k1, cache_v1, chip)
        y_one, k_one, v_one = attention_layer(x_in, keys1, vals1, chip, core, (w_q1, b_q1, w_k1, b_k1, w_v1, w_o1), tables)
        y_one, cache_k2, cache_v2 = lax.optimization_barrier((y_one, cache_k2, cache_v2))
        keys2, vals2 = reshard_cache(cache_k2, cache_v2, chip)
        resid_h = (x_in.astype(jnp.float32) + y_one.astype(jnp.float32)).astype(jnp.bfloat16)
        normed = rms_norm(resid_h)
        both = jnp.concatenate([normed, lax.ppermute(normed, 'cp', PAIR_PERM)], axis=0)
        part = mlp_partial(core, both, w_gate, w_up, w_down)
        other = lax.ppermute(part[tok:], 'cp', PAIR_PERM)
        hidden = (resid_h.astype(jnp.float32) + (part[:tok] + other)).astype(jnp.bfloat16)
        y_two, k_two, v_two = attention_layer(rms_norm(hidden), keys2, vals2, chip, core, (w_q2, b_q2, w_k2, b_k2, w_v2, w_o2), tables)
        return hidden, y_two, k_one, v_one, k_two, v_two

    return jax.shard_map(forward, mesh=mesh, in_specs=in_specs, out_specs=out_specs, check_vma=False)
```

```python
import functools

import jax
import jax.numpy as jnp
from jax import lax
from jax.experimental import pallas as pl
from jax.experimental.pallas import tpu as pltpu
from jax.sharding import PartitionSpec as P

ROPE_THETA = 500000.0
NORM_EPS = 1e-5
LOG2E = 1.4426950408889634
KV_HEADS = 4
HEAD = 128
GROUP = 7
CHIPS = 4
COL = 256
SLOTS = 2 * CHIPS
MIB = 1024 * 1024
MESH = pl.DeviceIdType.MESH


def rope_tables(positions):
    half_dim = HEAD // 2
    inv_freq = 1.0 / (ROPE_THETA ** (jnp.arange(half_dim, dtype=jnp.float32) * (2.0 / HEAD)))
    angles = positions.astype(jnp.float32)[:, None] * inv_freq[None, :]
    cos_t, sin_t = jnp.cos(angles), jnp.sin(angles)
    return jnp.concatenate([cos_t, cos_t], axis=-1), jnp.concatenate([-sin_t, sin_t], axis=-1)


def norm_rows(wide):
    return (wide * lax.rsqrt(jnp.mean(wide * wide, axis=-1, keepdims=True) + NORM_EPS)).astype(jnp.bfloat16)


def peers():
    me = lax.axis_index('cp')
    chip, core = me // 2, me % 2
    across = [2 * (chip ^ step) + core for step in range(CHIPS)]
    return chip, core, across, 2 * chip + (1 - core)


def meet(others):
    barrier = pltpu.get_barrier_semaphore()
    for dev in others:
        pl.semaphore_signal(barrier, inc=1, device_id={'cp': dev}, device_id_type=MESH)
    pl.semaphore_wait(barrier, len(others))


def remote(src, dst, send_sem, recv_sem, dev):
    return pltpu.make_async_remote_copy(src_ref=src, dst_ref=dst, send_sem=send_sem, recv_sem=recv_sem,
                                        device_id={'cp': dev}, device_id_type=MESH)


def layer_kernel(resharded, a_ref, bias_ref, cos_ref, sin_ref, k4_ref, v4_ref, *refs):
    if resharded:
        kin_ref, vin_ref, wq_ref, wk_ref, wv_ref, wo_ref = refs[:6]
        refs = refs[6:]
    else:
        wq_ref, wk_ref, wv_ref, wo_ref = refs[:4]
        refs = refs[4:]
    (y_ref, knew_ref, vnew_ref, xn, wbuf, wo, kb, vb, vt, msg, got, peer_new, newk, newvt, qt,
     s_even, s_odd, m_even, m_odd, acc, m_run, l_run, o_send, o_all,
     w_sem, wo_sem, loc_sem, kv_send, kv_recv, pair_send, pair_recv, q_send, q_recv,
     new_send, new_recv, o_ssem, o_rsem) = refs
    chip, core, across, partner = peers()
    scale2 = HEAD ** -0.5 * LOG2E
    tok = a_ref.shape[0]
    chunk = kb.shape[1]
    rows = qt.shape[2]
    n_buf = wbuf.shape[0]
    n_q, n_k = wq_ref.shape[1] // COL, wk_ref.shape[1] // COL
    n_blk = n_q + 2 * n_k
    n_items = SLOTS * GROUP

    def fetch(blk):
        slot = blk % n_buf

        @pl.when(blk < n_q)
        def _():
            pltpu.make_async_copy(wq_ref.at[:, pl.ds(blk * COL, COL)], wbuf.at[slot], w_sem.at[slot]).start()

        @pl.when((blk >= n_q) & (blk < n_q + n_k))
        def _():
            pltpu.make_async_copy(wk_ref.at[:, pl.ds((blk - n_q) * COL, COL)], wbuf.at[slot], w_sem.at[slot]).start()

        @pl.when((blk >= n_q + n_k) & (blk < n_blk))
        def _():
            pltpu.make_async_copy(wv_ref.at[:, pl.ds((blk - n_q - n_k) * COL, COL)], wbuf.at[slot], w_sem.at[slot]).start()

    for b in range(n_buf):
        pltpu.make_async_copy(wq_ref.at[:, b * COL:(b + 1) * COL], wbuf.at[b], w_sem.at[b]).start()
    meet(across[1:] + [partner])

    own = [pltpu.make_async_copy(k4_ref.at[chip], kb.at[0], loc_sem.at[0]),
           pltpu.make_async_copy(v4_ref.at[chip], vb.at[0], loc_sem.at[1])]
    for c in own:
        c.start()

    def kv_copy(step, which):
        src, dst = (k4_ref, kb) if which == 0 else (v4_ref, vb)
        return remote(src.at[chip ^ step], dst.at[2 * step], kv_send.at[step - 1, which], kv_recv.at[step - 1, which],
                      across[step])

    def pair_copy(step, which):
        dst = kb if which == 0 else vb
        if step == 0:
            src = (k4_ref if which == 0 else v4_ref).at[chip]
        else:
            src = dst.at[2 * step]
        return remote(src, dst.at[2 * step + 1], pair_send.at[step, which], pair_recv.at[step, which], partner)

    if resharded:
        loads = []
        for j in range(1, SLOTS):
            loads.append((pltpu.make_async_copy(kin_ref.at[j], kb.at[j], loc_sem.at[2 * j]),
                          pltpu.make_async_copy(vin_ref.at[j], vb.at[j], loc_sem.at[2 * j + 1])))
    else:
        for which in range(2):
            pair_copy(0, which).start()
        kv_copy(1, 0).start()
        kv_copy(2, 0).start()

    if resharded:
        xn[...] = norm_rows(a_ref[...].astype(jnp.float32))
    else:
        xn[...] = a_ref[...]

    def project(blk, carry):
        slot = blk % n_buf
        pltpu.make_async_copy(wbuf.at[slot], wbuf.at[slot], w_sem.at[slot]).wait()
        raw = (jnp.dot(xn[...], wbuf[slot], preferred_element_type=jnp.float32) + bias_ref[blk]).astype(jnp.bfloat16)
        fetch(blk + n_buf)
        is_v = blk >= n_q + n_k
        for half in range(2):
            head = 2 * blk + half
            plain = raw[:, half * HEAD:(half + 1) * HEAD]
            wide = plain.astype(jnp.float32)
            roped = (wide * cos_ref[...] + pltpu.roll(wide, HEAD // 2, 1) * sin_ref[...]).astype(jnp.bfloat16)
            value = jnp.where(is_v, plain, roped)
            is_q = blk < n_q
            kv_idx = head - 2 * n_q
            grp = jnp.where(is_q, head // GROUP, kv_idx % KV_HEADS)
            idx = jnp.where(is_q, head % GROUP, GROUP + kv_idx // KV_HEADS)
            msg[grp, idx] = value
        return carry

    lax.fori_loop(0, n_blk, project, 0)

    q_copies = [remote(msg.at[chip ^ s], got.at[s - 1], q_send.at[s - 1], q_recv.at[s - 1], across[s]) for s in range(1, CHIPS)]
    for c in q_copies:
        c.start()
    wo_load = pltpu.make_async_copy(wo_ref, wo, wo_sem)
    if resharded:
        for pair in loads:
            for c in pair:
                c.start()
    else:
        for step, which in ((1, 1), (2, 1), (3, 0), (3, 1)):
            kv_copy(step, which).start()
    wo_load.start()
    for c in range(KV_HEADS):
        knew_ref[c] = msg[c, GROUP]
        vnew_ref[c] = msg[c, GROUP + 1]
    acc[...] = jnp.zeros_like(acc)
    m_run[...] = jnp.full_like(m_run, -jnp.inf)
    l_run[...] = jnp.zeros_like(l_run)
    for c in q_copies:
        c.wait_recv()
    new_copies = [remote(msg.at[chip, pl.ds(GROUP, 2)], peer_new.at[0], new_send.at[0], new_recv.at[0], partner)]
    for s in range(1, CHIPS):
        new_copies.append(remote(got.at[s - 1, pl.ds(GROUP, 2)], peer_new.at[s], new_send.at[s], new_recv.at[s], partner))
    for c in new_copies:
        c.start()
    for g in range(GROUP):
        cols = jnp.concatenate([msg[chip, g]] + [got[s - 1, g] for s in range(1, CHIPS)], axis=0)
        qt[g] = cols.T

    def ready(j):
        for jj in range(SLOTS):
            @pl.when(j == jj)
            def _():
                if jj == 0:
                    for c in own:
                        c.wait()
                elif resharded:
                    for c in loads[jj - 1]:
                        c.wait()
                elif jj % 2 == 0:
                    for which in range(2):
                        kv_copy(jj // 2, which).wait_recv()
                        pair_copy(jj // 2, which).start()
                else:
                    for which in range(2):
                        pair_copy(jj // 2, which).wait_recv()

        vt[j % 2] = vb[j].T

    def score(item, s_dst, m_dst):
        j, g = item // GROUP, item % GROUP
        part = jnp.full((8, rows), -jnp.inf, jnp.float32)
        for t in range(chunk // 256):
            s_blk = jnp.dot(kb[j, t * 256:(t + 1) * 256, :], qt[g], preferred_element_type=jnp.float32)
            s_dst[t * 256:(t + 1) * 256, :] = s_blk
            part = jnp.maximum(part, jnp.max(s_blk.reshape(32, 8, rows), axis=0))
        m_dst[...] = part

    def absorb(item, s_src, m_src):
        j, g = item // GROUP, item % GROUP
        m_old = m_run[g]
        m_new = jnp.maximum(m_old, jnp.max(m_src[...], axis=0, keepdims=True))
        alpha = jnp.exp2((m_old - m_new) * scale2)
        shift = m_new * scale2
        l_part = jnp.zeros((8, rows), jnp.float32)
        out = jnp.zeros((HEAD, rows), jnp.float32)
        for t in range(chunk // 256):
            p = jnp.exp2(s_src[t * 256:(t + 1) * 256, :] * scale2 - shift)
            l_part = l_part + jnp.sum(p.reshape(32, 8, rows), axis=0)
            out = out + jnp.dot(vt[j % 2, :, t * 256:(t + 1) * 256], p.astype(jnp.bfloat16),
                                preferred_element_type=jnp.float32)
        acc[g] = acc[g] * alpha + out
        l_run[g] = l_run[g] * alpha + l_part
        m_run[g] = m_new

    ready(0)
    score(0, s_even, m_even)

    def pair(i, carry):
        first = 2 * i
        nxt = first + 2

        @pl.when((first + 1) % GROUP == 0)
        def _():
            ready((first + 1) // GROUP)

        @pl.when((nxt % GROUP == 0) & (nxt < n_items))
        def _():
            ready(nxt // GROUP)

        score(first + 1, s_odd, m_odd)
        absorb(first, s_even, m_even)
        score(jnp.minimum(nxt, n_items - 1), s_even, m_even)
        absorb(first + 1, s_odd, m_odd)
        return carry

    lax.fori_loop(0, n_items // 2, pair, 0)

    for c in new_copies:
        c.wait_recv()
    for s in range(CHIPS):
        mine = (msg.at[chip], GROUP) if s == 0 else (got.at[s - 1], GROUP)
        for r in range(2):
            at = (r * CHIPS + s) * tok
            if r == 0:
                nk, nv = mine[0][mine[1]], mine[0][mine[1] + 1]
            else:
                nk, nv = peer_new[s, 0], peer_new[s, 1]
            newk[at:at + tok, :] = nk
            newvt[at:at + tok, :] = nv

    new_len = newk.shape[0]
    key_i = lax.broadcasted_iota(jnp.int32, (new_len, rows), 0)
    qry_i = lax.broadcasted_iota(jnp.int32, (new_len, rows), 1)
    blk = key_i // tok
    k_pos = (2 * (chip ^ (blk % CHIPS)) + (core ^ (blk // CHIPS))) * tok + key_i % tok
    q_pos = (2 * (chip ^ (qry_i // tok)) + core) * tok + qry_i % tok
    visible = k_pos <= q_pos

    for g in range(GROUP):
        s = jnp.dot(newk[...], qt[g], preferred_element_type=jnp.float32)
        s = jnp.where(visible, s, -jnp.inf)
        m_old = m_run[g]
        m_new = jnp.maximum(m_old, jnp.max(s, axis=0, keepdims=True))
        alpha = jnp.exp2((m_old - m_new) * scale2)
        p = jnp.exp2(s * scale2 - m_new * scale2)
        total = jnp.sum(l_run[g] * alpha, axis=0, keepdims=True) + jnp.sum(p, axis=0, keepdims=True)
        fresh = lax.dot_general(newvt[...], p.astype(jnp.bfloat16), (((0,), (0,)), ((), ())),
                                preferred_element_type=jnp.float32)
        out = ((acc[g] * alpha + fresh) / total).T.astype(jnp.bfloat16)
        for s_i in range(CHIPS):
            o_send[s_i, :, g * HEAD:(g + 1) * HEAD] = out[s_i * tok:(s_i + 1) * tok, :]

    wide_cols = GROUP * HEAD
    here = pl.ds(pl.multiple_of(chip * wide_cols, HEAD), wide_cols)
    o_copies = [remote(o_send.at[s], o_all.at[:, here], o_ssem.at[s - 1], o_rsem.at[s - 1], across[s]) for s in range(1, CHIPS)]
    for c in o_copies:
        c.start()
    o_all[:, here] = o_send[0]
    wo_load.wait()
    for c in o_copies:
        c.wait_recv()

    def out_proj(blk, carry):
        cols = pl.ds(pl.multiple_of(blk * COL, COL), COL)
        y = jnp.dot(o_all[...], wo[:, cols], preferred_element_type=jnp.float32).astype(jnp.bfloat16)
        if not resharded:
            y = (a_ref[:, cols].astype(jnp.float32) + y.astype(jnp.float32)).astype(jnp.bfloat16)
        y_ref[:, cols] = y
        return carry

    lax.fori_loop(0, wo.shape[1] // COL, out_proj, 0)

    for c in q_copies + new_copies + o_copies:
        c.wait_send()
    if not resharded:
        for step in range(CHIPS):
            for which in range(2):
                pair_copy(step, which).wait_send()
                if step:
                    kv_copy(step, which).wait_send()


def run_layer(a, bias, cos_t, sin_t, k4, v4, k_in, v_in, w_q, w_k, w_v, w_o, collective_id):
    resharded = k_in is not None
    tok, width = a.shape
    chunk = k4.shape[1]
    rows = CHIPS * tok
    bf16, f32 = jnp.bfloat16, jnp.float32
    vmem = pl.BlockSpec(memory_space=pltpu.VMEM)
    hbm = pl.BlockSpec(memory_space=pl.ANY)
    dma = pltpu.SemaphoreType.DMA
    caches = (k4, v4, k_in, v_in) if resharded else (k4, v4)
    return pl.pallas_call(
        functools.partial(layer_kernel, resharded),
        out_shape=[jax.ShapeDtypeStruct((tok, width), bf16),
                   jax.ShapeDtypeStruct((KV_HEADS, tok, HEAD), bf16),
                   jax.ShapeDtypeStruct((KV_HEADS, tok, HEAD), bf16)],
        in_specs=[vmem] * 4 + [hbm] * (len(caches) + 4),
        out_specs=[vmem] * 3,
        scratch_shapes=[
            pltpu.VMEM((tok, width), bf16),
            pltpu.VMEM((4, width, COL), bf16),
            pltpu.VMEM(w_o.shape, bf16),
            pltpu.VMEM((SLOTS, chunk, HEAD), bf16),
            pltpu.VMEM((SLOTS, chunk, HEAD), bf16),
            pltpu.VMEM((2, HEAD, chunk), bf16),
            pltpu.VMEM((KV_HEADS, GROUP + 2, tok, HEAD), bf16),
            pltpu.VMEM((CHIPS - 1, GROUP + 2, tok, HEAD), bf16),
            pltpu.VMEM((CHIPS, 2, tok, HEAD), bf16),
            pltpu.VMEM((2 * rows, HEAD), bf16),
            pltpu.VMEM((2 * rows, HEAD), bf16),
            pltpu.VMEM((GROUP, HEAD, rows), bf16),
            pltpu.VMEM((chunk, rows), f32),
            pltpu.VMEM((chunk, rows), f32),
            pltpu.VMEM((8, rows), f32),
            pltpu.VMEM((8, rows), f32),
            pltpu.VMEM((GROUP, HEAD, rows), f32),
            pltpu.VMEM((GROUP, 1, rows), f32),
            pltpu.VMEM((GROUP, 8, rows), f32),
            pltpu.VMEM((CHIPS, tok, GROUP * HEAD), bf16),
            pltpu.VMEM((tok, CHIPS * GROUP * HEAD), bf16),
            dma((4,)), dma, dma((2 * SLOTS,)),
            dma((CHIPS - 1, 2)), dma((CHIPS - 1, 2)), dma((CHIPS, 2)), dma((CHIPS, 2)),
            dma((CHIPS - 1,)), dma((CHIPS - 1,)), dma((CHIPS,)), dma((CHIPS,)),
            dma((CHIPS - 1,)), dma((CHIPS - 1,)),
        ],
        compiler_params=pltpu.CompilerParams(collective_id=collective_id, has_side_effects=True, vmem_limit_bytes=60 * MIB),
        name="layer",
    )(a, bias, cos_t, sin_t, *caches, w_q, w_k, w_v, w_o)


def mlp_kernel(h_ref, k4_ref, v4_ref, gate_ref, up_ref, down_ref, g_ref, kout_ref, vout_ref,
               u, wg, wu, wd, acc, theirs, w_sem, u_send, u_recv, part_send, part_recv, kv_send, kv_recv, pair_send, pair_recv):
    chip, core, across, partner = peers()
    tok = h_ref.shape[0]
    n_buf = wg.shape[0]
    steps = gate_ref.shape[1] // (2 * COL)

    def copies(i):
        slot = i % n_buf
        cols = pl.ds(pl.multiple_of((core * steps + i) * COL, COL), COL)
        return (pltpu.make_async_copy(gate_ref.at[:, cols], wg.at[slot], w_sem.at[slot, 0]),
                pltpu.make_async_copy(up_ref.at[:, cols], wu.at[slot], w_sem.at[slot, 1]),
                pltpu.make_async_copy(down_ref.at[cols, :], wd.at[slot], w_sem.at[slot, 2]))

    for b in range(n_buf):
        for c in copies(b):
            c.start()
    meet(across[1:] + [partner])
    u[:tok, :] = norm_rows(h_ref[...].astype(jnp.float32))
    u_copy = remote(u.at[pl.ds(0, tok)], u.at[pl.ds(tok, tok)], u_send, u_recv, partner)
    u_copy.start()

    def kv_copy(step, which):
        src, dst = (k4_ref, kout_ref) if which == 0 else (v4_ref, vout_ref)
        return remote(src.at[chip ^ step], dst.at[2 * step], kv_send.at[step - 1, which], kv_recv.at[step - 1, which],
                      across[step])

    def pair_copy(step, which):
        dst = kout_ref if which == 0 else vout_ref
        src = (k4_ref if which == 0 else v4_ref).at[chip] if step == 0 else dst.at[2 * step]
        return remote(src, dst.at[2 * step + 1], pair_send.at[step, which], pair_recv.at[step, which], partner)

    for step in range(1, CHIPS):
        for which in range(2):
            kv_copy(step, which).start()
    for which in range(2):
        pair_copy(0, which).start()
    acc[...] = jnp.zeros_like(acc)
    u_copy.wait_recv()

    def relay(step):
        for which in range(2):
            kv_copy(step, which).wait_recv()
            pair_copy(step, which).start()

    def block(i, carry):
        slot = i % n_buf
        for c in copies(i):
            c.wait()
        gate = jnp.dot(u[...], wg[slot], preferred_element_type=jnp.float32).astype(jnp.bfloat16).astype(jnp.float32)
        up = jnp.dot(u[...], wu[slot], preferred_element_type=jnp.float32).astype(jnp.bfloat16).astype(jnp.float32)
        mixed = (gate * jax.nn.sigmoid(gate) * up).astype(jnp.bfloat16)
        acc[...] += jnp.dot(mixed, wd[slot], preferred_element_type=jnp.float32)

        @pl.when(i + n_buf < steps)
        def _():
            for c in copies(i + n_buf):
                c.start()

        @pl.when(i == steps - 12)
        def _():
            relay(1)
            relay(2)

        @pl.when(i == steps - 5)
        def _():
            relay(3)

        return carry

    lax.fori_loop(0, steps, block, 0)
    part_copy = remote(acc.at[pl.ds(tok, tok)], theirs, part_send, part_recv, partner)
    part_copy.start()
    part_copy.wait_recv()
    g_ref[...] = (h_ref[...].astype(jnp.float32) + (acc[:tok, :] + theirs[...])).astype(jnp.bfloat16)
    for step in range(CHIPS):
        for which in range(2):
            pair_copy(step, which).wait()
            if step:
                kv_copy(step, which).wait_send()
    u_copy.wait_send()
    part_copy.wait_send()


def run_mlp(h, k4, v4, w_gate, w_up, w_down, collective_id):
    tok, width = h.shape
    chunk = k4.shape[1]
    bf16, f32 = jnp.bfloat16, jnp.float32
    vmem = pl.BlockSpec(memory_space=pltpu.VMEM)
    hbm = pl.BlockSpec(memory_space=pl.ANY)
    dma = pltpu.SemaphoreType.DMA
    n_buf = 4
    slots = jax.ShapeDtypeStruct((SLOTS, chunk, HEAD), bf16)
    return pl.pallas_call(
        mlp_kernel,
        out_shape=[jax.ShapeDtypeStruct((tok, width), bf16), slots, slots],
        in_specs=[vmem] + [hbm] * 5,
        out_specs=[vmem, hbm, hbm],
        scratch_shapes=[
            pltpu.VMEM((2 * tok, width), bf16),
            pltpu.VMEM((n_buf, width, COL), bf16),
            pltpu.VMEM((n_buf, width, COL), bf16),
            pltpu.VMEM((n_buf, COL, width), bf16),
            pltpu.VMEM((2 * tok, width), f32),
            pltpu.VMEM((tok, width), f32),
            dma((n_buf, 3)), dma, dma, dma, dma,
            dma((CHIPS - 1, 2)), dma((CHIPS - 1, 2)), dma((CHIPS, 2)), dma((CHIPS, 2)),
        ],
        compiler_params=pltpu.CompilerParams(collective_id=collective_id, has_side_effects=True, vmem_limit_bytes=60 * MIB),
        name="mlp",
    )(h, k4, v4, w_gate, w_up, w_down)


def heads_first(cache):
    return lax.optimization_barrier(jnp.transpose(cache, (1, 0, 2)))


def pack_bias(b_q, b_k):
    wide = jnp.concatenate([b_q.astype(jnp.float32), b_k.astype(jnp.float32), jnp.zeros(b_k.shape, jnp.float32)])
    return wide.reshape(-1, 1, COL)


def solution(mesh):
    axis_size = mesh.shape['cp']
    rows_spec = P(('dp', 'cp'), None)
    cache_spec = P(('dp', 'cp'), None, None)
    mat_spec = P(None, None)
    vec_spec = P(None)
    layer_specs = (cache_spec, cache_spec, mat_spec, vec_spec, mat_spec, vec_spec, mat_spec, mat_spec)
    in_specs = (rows_spec,) + layer_specs + (mat_spec, mat_spec, mat_spec) + layer_specs
    out_specs = (rows_spec, rows_spec, cache_spec, cache_spec, cache_spec, cache_spec)

    def forward(x_in, cache_k1, cache_v1, w_q1, b_q1, w_k1, b_k1, w_v1, w_o1, w_gate, w_up, w_down, cache_k2, cache_v2, w_q2, b_q2, w_k2, b_k2, w_v2, w_o2):
        me = lax.axis_index('cp')
        tok = x_in.shape[0]
        positions = axis_size * cache_k1.shape[0] + me * tok + jnp.arange(tok)
        cos_t, sin_t = rope_tables(positions)
        k4a, v4a = heads_first(cache_k1), heads_first(cache_v1)
        k4b, v4b = heads_first(cache_k2), heads_first(cache_v2)
        resid_h, k_one, v_one = run_layer(x_in, pack_bias(b_q1, b_k1), cos_t, sin_t, k4a, v4a, None, None,
                                          w_q1, w_k1, w_v1, w_o1, 1)
        hidden, k_in, v_in = run_mlp(resid_h, k4b, v4b, w_gate, w_up, w_down, 2)
        y_two, k_two, v_two = run_layer(hidden, pack_bias(b_q2, b_k2), cos_t, sin_t, k4b, v4b, k_in, v_in,
                                        w_q2, w_k2, w_v2, w_o2, 3)
        back = lambda t: jnp.transpose(t, (1, 0, 2))
        return hidden, y_two, back(k_one), back(v_one), back(k_two), back(v_two)

    return jax.shard_map(forward, mesh=mesh, in_specs=in_specs, out_specs=out_specs, check_vma=False)
```

```python
import functools

import jax
import jax.numpy as jnp
import numpy as np
from jax import lax
from jax.experimental import pallas as pl
from jax.experimental.pallas import tpu as pltpu
from jax.sharding import PartitionSpec as P

ROPE_THETA = 500000.0
NORM_EPS = 1e-5
LOG2E = 1.4426950408889634
KV_HEADS = 4
HEAD = 128
GROUP = 7
CHIPS = 4
COL = 256
SLOTS = 2 * CHIPS
MIB = 1024 * 1024
MESH = pl.DeviceIdType.MESH


@functools.lru_cache(maxsize=None)
def rope_table(first, count):
    with jax.ensure_compile_time_eval():
        half_dim = HEAD // 2
        inv_freq = 1.0 / (ROPE_THETA ** (jnp.arange(half_dim, dtype=jnp.float32) * (2.0 / HEAD)))
        angles = (first + jnp.arange(count)).astype(jnp.float32)[:, None] * inv_freq[None, :]
        cos_t, sin_t = jnp.cos(angles), jnp.sin(angles)
        return np.asarray(jnp.concatenate([cos_t, cos_t, -sin_t, sin_t], axis=-1))


def norm_rows(wide):
    return (wide * lax.rsqrt(jnp.mean(wide * wide, axis=-1, keepdims=True) + NORM_EPS)).astype(jnp.bfloat16)


def peers():
    me = lax.axis_index('cp')
    chip, core = me // 2, me % 2
    across = [2 * (chip ^ step) + core for step in range(CHIPS)]
    return chip, core, across, 2 * chip + (1 - core)


def meet(others):
    barrier = pltpu.get_barrier_semaphore()
    for dev in others:
        pl.semaphore_signal(barrier, inc=1, device_id={'cp': dev}, device_id_type=MESH)
    pl.semaphore_wait(barrier, len(others))


def remote(src, dst, send_sem, recv_sem, dev):
    return pltpu.make_async_remote_copy(src_ref=src, dst_ref=dst, send_sem=send_sem, recv_sem=recv_sem,
                                        device_id={'cp': dev}, device_id_type=MESH)


def layer_kernel(resharded, a_ref, bias_ref, trig_ref, k4_ref, v4_ref, *refs):
    if resharded:
        kin_ref, vin_ref, wq_ref, wk_ref, wv_ref, wo_ref = refs[:6]
        refs = refs[6:]
    else:
        wq_ref, wk_ref, wv_ref, wo_ref = refs[:4]
        refs = refs[4:]
    (y_ref, knew_ref, vnew_ref, xn, trig, wkv, wo, kb, vb, vt, msg, got, peer_new, newk, newv, qt,
     s_even, s_odd, m_even, m_odd, acc, m_run, l_run, o_send, o_all,
     trig_sem, w_sem, wo_sem, loc_sem, kv_send, kv_recv, pair_send, pair_recv, q_send, q_recv,
     new_send, new_recv, o_ssem, o_rsem) = refs
    chip, core, across, partner = peers()
    me = 2 * chip + core
    scale2 = HEAD ** -0.5 * LOG2E
    tok = a_ref.shape[0]
    chunk = kb.shape[1]
    rows = qt.shape[2]
    wide_cols = GROUP * HEAD
    n_q = wq_ref.shape[1]
    n_items = SLOTS * GROUP
    n_first = (SLOTS - 2) * GROUP
    bias_at = (n_q + wk_ref.shape[1]) if resharded else 0

    def wq_copy(n):
        cols = pl.ds(pl.multiple_of((chip ^ (CHIPS - 1 - n)) * wide_cols, HEAD), wide_cols)
        return pltpu.make_async_copy(wq_ref.at[:, cols], wo.at[:, n * wide_cols:(n + 1) * wide_cols], w_sem.at[2 + n])

    kv_loads = [pltpu.make_async_copy(wk_ref, wkv.at[0], w_sem.at[0]), pltpu.make_async_copy(wv_ref, wkv.at[1], w_sem.at[1])]
    trig_load = pltpu.make_async_copy(trig_ref.at[pl.ds(me * tok, tok)], trig, trig_sem)
    trig_load.start()
    for c in kv_loads + [wq_copy(n) for n in range(CHIPS)]:
        c.start()
    meet(across[1:] + [partner])

    own = [pltpu.make_async_copy(k4_ref.at[chip], kb.at[0], loc_sem.at[0]),
           pltpu.make_async_copy(v4_ref.at[chip], vb.at[0], loc_sem.at[1])]
    for c in own:
        c.start()

    def kv_copy(step, which):
        src, dst = (k4_ref, kb) if which == 0 else (v4_ref, vb)
        return remote(src.at[chip ^ step], dst.at[2 * step], kv_send.at[step - 1, which], kv_recv.at[step - 1, which],
                      across[step])

    def pair_copy(step, which):
        dst = kb if which == 0 else vb
        if step == 0:
            src = (k4_ref if which == 0 else v4_ref).at[chip]
        else:
            src = dst.at[2 * step]
        return remote(src, dst.at[2 * step + 1], pair_send.at[step, which], pair_recv.at[step, which], partner)

    if resharded:
        loads = []
        for j in range(1, SLOTS):
            loads.append((pltpu.make_async_copy(kin_ref.at[j], kb.at[j], loc_sem.at[2 * j]),
                          pltpu.make_async_copy(vin_ref.at[j], vb.at[j], loc_sem.at[2 * j + 1])))
    else:
        for which in range(2):
            pair_copy(0, which).start()
        kv_copy(1, 0).start()
        kv_copy(2, 0).start()

    if resharded:
        xn[...] = norm_rows(a_ref[...].astype(jnp.float32))
    else:
        xn[...] = a_ref[...]

    trig_load.wait()

    def rope(plain):
        wide = plain.astype(jnp.float32)
        return (wide * trig[:, :HEAD] + pltpu.roll(wide, HEAD // 2, 1) * trig[:, HEAD:]).astype(jnp.bfloat16)

    kv_loads[0].wait()
    k_pre = (jnp.dot(xn[...], wkv[0], preferred_element_type=jnp.float32)
             + bias_ref[:, bias_at + n_q:bias_at + n_q + KV_HEADS * HEAD]).astype(jnp.bfloat16)
    for c in range(KV_HEADS):
        knew_ref[c] = rope(k_pre[:, c * HEAD:(c + 1) * HEAD])
    kv_loads[1].wait()
    v_pre = jnp.dot(xn[...], wkv[1], preferred_element_type=jnp.float32).astype(jnp.bfloat16)
    for c in range(KV_HEADS):
        vnew_ref[c] = v_pre[:, c * HEAD:(c + 1) * HEAD]

    def q_copy(n):
        return remote(msg.at[n], got.at[n], q_send.at[n], q_recv.at[n], 2 * (chip ^ (CHIPS - 1 - n)) + core)

    def project(n, carry):
        pltpu.make_async_copy(wo.at[:, :wide_cols], wo.at[:, :wide_cols], w_sem.at[2 + n]).wait()
        grp = chip ^ (CHIPS - 1 - n)
        cols = pl.ds(pl.multiple_of(n * wide_cols, HEAD), wide_cols)
        bias = bias_ref[:, pl.ds(pl.multiple_of(bias_at + grp * wide_cols, HEAD), wide_cols)]
        q_pre = (jnp.dot(xn[...], wo[:, cols], preferred_element_type=jnp.float32) + bias).astype(jnp.bfloat16)
        for g in range(GROUP):
            msg[n, g] = rope(q_pre[:, g * HEAD:(g + 1) * HEAD])
        msg[n, GROUP] = knew_ref[grp]
        msg[n, GROUP + 1] = vnew_ref[grp]

        @pl.when(n < CHIPS - 1)
        def _():
            q_copy(n).start()

        return carry

    lax.fori_loop(0, CHIPS, project, 0)
    q_copies = [q_copy(n) for n in range(CHIPS - 1)]
    parts = [msg.at[CHIPS - 1]] + [got.at[CHIPS - 1 - s] for s in range(1, CHIPS)]
    wo_load = pltpu.make_async_copy(wo_ref, wo, wo_sem)
    if resharded:
        for pair in loads:
            for c in pair:
                c.start()
    else:
        for step, which in ((1, 1), (2, 1), (3, 0), (3, 1)):
            kv_copy(step, which).start()
    wo_load.start()
    acc[...] = jnp.zeros_like(acc)
    m_run[...] = jnp.full_like(m_run, -jnp.inf)
    l_run[...] = jnp.zeros_like(l_run)
    for c in q_copies:
        c.wait_recv()
    new_copies = [remote(parts[s].at[pl.ds(GROUP, 2)], peer_new.at[s], new_send.at[s], new_recv.at[s], partner) for s in range(CHIPS)]
    for c in new_copies:
        c.start()
    for g in range(GROUP):
        qt[g] = jnp.concatenate([p[g] for p in parts], axis=0).T
    for s in range(CHIPS):
        newk[s * tok:(s + 1) * tok, :] = parts[s][GROUP]
        newv[s * tok:(s + 1) * tok, :] = parts[s][GROUP + 1]

    def ready(j):
        for jj in range(SLOTS):
            @pl.when(j == jj)
            def _():
                if jj == 0:
                    for c in own:
                        c.wait()
                elif resharded:
                    for c in loads[jj - 1]:
                        c.wait()
                elif jj % 2 == 0:
                    for which in range(2):
                        kv_copy(jj // 2, which).wait_recv()
                        pair_copy(jj // 2, which).start()
                else:
                    for which in range(2):
                        pair_copy(jj // 2, which).wait_recv()

        vt[j % 2] = vb[j].T

    def place(item):
        late = item - n_first
        is_late = late >= 0
        return jnp.where(is_late, SLOTS - 2 + late % 2, item // GROUP), jnp.where(is_late, late // 2, item % GROUP)

    def score(item, s_dst, m_dst):
        j, g = place(item)
        part = jnp.full((8, rows), -jnp.inf, jnp.float32)
        for t in range(chunk // 256):
            s_blk = jnp.dot(kb[j, t * 256:(t + 1) * 256, :], qt[g], preferred_element_type=jnp.float32)
            s_dst[t * 256:(t + 1) * 256, :] = s_blk
            part = jnp.maximum(part, jnp.max(s_blk.reshape(32, 8, rows), axis=0))
        m_dst[...] = part

    def absorb(item, s_src, m_src):
        j, g = place(item)
        m_old = m_run[g]
        m_new = jnp.maximum(m_old, jnp.max(m_src[...], axis=0, keepdims=True))
        alpha = jnp.exp2((m_old - m_new) * scale2)
        shift = m_new * scale2
        l_part = jnp.zeros((8, rows), jnp.float32)
        out = jnp.zeros((HEAD, rows), jnp.float32)
        for t in range(chunk // 256):
            p = jnp.exp2(s_src[t * 256:(t + 1) * 256, :] * scale2 - shift)
            l_part = l_part + jnp.sum(p.reshape(32, 8, rows), axis=0)
            out = out + jnp.dot(vt[j % 2, :, t * 256:(t + 1) * 256], p.astype(jnp.bfloat16),
                                preferred_element_type=jnp.float32)
        acc[g] = acc[g] * alpha + out
        l_run[g] = l_run[g] * alpha + l_part
        m_run[g] = m_new

    ready(0)
    score(0, s_even, m_even)

    new_len = newk.shape[0]

    def visible():
        key_i = lax.broadcasted_iota(jnp.int32, (new_len, rows), 0)
        qry_i = lax.broadcasted_iota(jnp.int32, (new_len, rows), 1)
        blk = key_i // tok
        k_pos = (2 * (chip ^ (blk % CHIPS)) + (core ^ (blk // CHIPS))) * tok + key_i % tok
        q_pos = (2 * (chip ^ (qry_i // tok)) + core) * tok + qry_i % tok
        return k_pos <= q_pos

    def o_copy(g, s):
        src = o_send.at[g, s]
        dst = o_all.at[:, pl.ds(pl.multiple_of(chip * wide_cols + g * HEAD, HEAD), HEAD)]
        return remote(src, dst, o_ssem.at[g, s - 1], o_rsem.at[g, s - 1], across[s])

    def finish(g):
        s = jnp.dot(newk[...], qt[g], preferred_element_type=jnp.float32)
        s = jnp.where(visible(), s, -jnp.inf)
        m_old = m_run[g]
        m_new = jnp.maximum(m_old, jnp.max(s, axis=0, keepdims=True))
        alpha = jnp.exp2((m_old - m_new) * scale2)
        p = jnp.exp2(s * scale2 - m_new * scale2)
        total = jnp.sum(l_run[g] * alpha, axis=0, keepdims=True) + jnp.sum(p, axis=0, keepdims=True)
        fresh = lax.dot_general(newv[...], p.astype(jnp.bfloat16), (((0,), (0,)), ((), ())),
                                preferred_element_type=jnp.float32)
        out = ((acc[g] * alpha + fresh) / total).T.astype(jnp.bfloat16)
        for s_i in range(1, CHIPS):
            o_send[g, s_i] = out[s_i * tok:(s_i + 1) * tok, :]
            o_copy(g, s_i).start()
        o_all[:, pl.ds(pl.multiple_of(chip * wide_cols + g * HEAD, HEAD), HEAD)] = out[:tok, :]

    def step(item, carry):
        nxt = item + 1
        early = (nxt < n_first) & (nxt % GROUP == 0)

        @pl.when(early | (nxt == n_first) | (nxt == n_first + 1))
        def _():
            ready(place(nxt)[0])

        @pl.when(item == n_first)
        def _():
            for c in new_copies:
                c.wait_recv()
            for s in range(CHIPS):
                at = (CHIPS + s) * tok
                newk[at:at + tok, :] = peer_new[s, 0]
                newv[at:at + tok, :] = peer_new[s, 1]

        after = jnp.minimum(nxt, n_items - 1)

        @pl.when(item % 2 == 0)
        def _():
            score(after, s_odd, m_odd)
            absorb(item, s_even, m_even)

        @pl.when(item % 2 == 1)
        def _():
            score(after, s_even, m_even)
            absorb(item, s_odd, m_odd)

        @pl.when((item > n_first) & ((item - n_first) % 2 == 1))
        def _():
            finish((item - n_first) // 2)

        return carry

    lax.fori_loop(0, n_items, step, 0)
    o_copies = [o_copy(g, s) for g in range(GROUP) for s in range(1, CHIPS)]
    wo_load.wait()
    for c in o_copies:
        c.wait_recv()

    def out_proj(blk, carry):
        cols = pl.ds(pl.multiple_of(blk * COL, COL), COL)
        y = jnp.dot(o_all[...], wo[:, cols], preferred_element_type=jnp.float32).astype(jnp.bfloat16)
        if not resharded:
            y = (a_ref[:, cols].astype(jnp.float32) + y.astype(jnp.float32)).astype(jnp.bfloat16)
        y_ref[:, cols] = y
        return carry

    lax.fori_loop(0, wo.shape[1] // COL, out_proj, 0)

    for c in q_copies + new_copies + o_copies:
        c.wait_send()
    if not resharded:
        for step in range(CHIPS):
            for which in range(2):
                pair_copy(step, which).wait_send()
                if step:
                    kv_copy(step, which).wait_send()


def run_layer(a, bias, trig, k4, v4, k_in, v_in, w_q, w_k, w_v, w_o, collective_id):
    resharded = k_in is not None
    tok, width = a.shape
    chunk = k4.shape[1]
    rows = CHIPS * tok
    bf16, f32 = jnp.bfloat16, jnp.float32
    vmem = pl.BlockSpec(memory_space=pltpu.VMEM)
    hbm = pl.BlockSpec(memory_space=pl.ANY)
    dma = pltpu.SemaphoreType.DMA
    caches = (k4, v4, k_in, v_in) if resharded else (k4, v4)
    return pl.pallas_call(
        functools.partial(layer_kernel, resharded),
        out_shape=[jax.ShapeDtypeStruct((tok, width), bf16),
                   jax.ShapeDtypeStruct((KV_HEADS, tok, HEAD), bf16),
                   jax.ShapeDtypeStruct((KV_HEADS, tok, HEAD), bf16)],
        in_specs=[vmem] * 2 + [hbm] * (len(caches) + 5),
        out_specs=[vmem] * 3,
        scratch_shapes=[
            pltpu.VMEM((tok, width), bf16),
            pltpu.VMEM((tok, 2 * HEAD), f32),
            pltpu.VMEM((2,) + w_k.shape, bf16),
            pltpu.VMEM(w_o.shape, bf16),
            pltpu.VMEM((SLOTS, chunk, HEAD), bf16),
            pltpu.VMEM((SLOTS, chunk, HEAD), bf16),
            pltpu.VMEM((2, HEAD, chunk), bf16),
            pltpu.VMEM((KV_HEADS, GROUP + 2, tok, HEAD), bf16),
            pltpu.VMEM((CHIPS - 1, GROUP + 2, tok, HEAD), bf16),
            pltpu.VMEM((CHIPS, 2, tok, HEAD), bf16),
            pltpu.VMEM((2 * rows, HEAD), bf16),
            pltpu.VMEM((2 * rows, HEAD), bf16),
            pltpu.VMEM((GROUP, HEAD, rows), bf16),
            pltpu.VMEM((chunk, rows), f32),
            pltpu.VMEM((chunk, rows), f32),
            pltpu.VMEM((8, rows), f32),
            pltpu.VMEM((8, rows), f32),
            pltpu.VMEM((GROUP, HEAD, rows), f32),
            pltpu.VMEM((GROUP, 1, rows), f32),
            pltpu.VMEM((GROUP, 8, rows), f32),
            pltpu.VMEM((GROUP, CHIPS, tok, HEAD), bf16),
            pltpu.VMEM((tok, CHIPS * GROUP * HEAD), bf16),
            dma, dma((2 + CHIPS,)), dma, dma((2 * SLOTS,)),
            dma((CHIPS - 1, 2)), dma((CHIPS - 1, 2)), dma((CHIPS, 2)), dma((CHIPS, 2)),
            dma((CHIPS - 1,)), dma((CHIPS - 1,)), dma((CHIPS,)), dma((CHIPS,)),
            dma((GROUP, CHIPS - 1)), dma((GROUP, CHIPS - 1)),
        ],
        compiler_params=pltpu.CompilerParams(collective_id=collective_id, has_side_effects=True, vmem_limit_bytes=60 * MIB),
        name="layer",
    )(a, bias, trig, *caches, w_q, w_k, w_v, w_o)


def mlp_kernel(h_ref, k4_ref, v4_ref, gate_ref, up_ref, down_ref, g_ref, kout_ref, vout_ref,
               u, wg, wu, wd, acc, theirs, w_sem, u_send, u_recv, part_send, part_recv, kv_send, kv_recv, pair_send, pair_recv):
    chip, core, across, partner = peers()
    tok = h_ref.shape[0]
    n_buf = wg.shape[0]
    steps = gate_ref.shape[1] // (2 * COL)

    def copies(i):
        slot = i % n_buf
        cols = pl.ds(pl.multiple_of((core * steps + i) * COL, COL), COL)
        return (pltpu.make_async_copy(gate_ref.at[:, cols], wg.at[slot], w_sem.at[slot, 0]),
                pltpu.make_async_copy(up_ref.at[:, cols], wu.at[slot], w_sem.at[slot, 1]),
                pltpu.make_async_copy(down_ref.at[cols, :], wd.at[slot], w_sem.at[slot, 2]))

    for b in range(n_buf):
        for c in copies(b):
            c.start()
    meet(across[1:] + [partner])
    u[:tok, :] = norm_rows(h_ref[...].astype(jnp.float32))
    u_copy = remote(u.at[pl.ds(0, tok)], u.at[pl.ds(tok, tok)], u_send, u_recv, partner)
    u_copy.start()

    def kv_copy(step, which):
        src, dst = (k4_ref, kout_ref) if which == 0 else (v4_ref, vout_ref)
        return remote(src.at[chip ^ step], dst.at[2 * step], kv_send.at[step - 1, which], kv_recv.at[step - 1, which],
                      across[step])

    def pair_copy(step, which):
        dst = kout_ref if which == 0 else vout_ref
        src = (k4_ref if which == 0 else v4_ref).at[chip] if step == 0 else dst.at[2 * step]
        return remote(src, dst.at[2 * step + 1], pair_send.at[step, which], pair_recv.at[step, which], partner)

    for step in range(1, CHIPS):
        for which in range(2):
            kv_copy(step, which).start()
    for which in range(2):
        pair_copy(0, which).start()
    acc[...] = jnp.zeros_like(acc)
    u_copy.wait_recv()

    def relay(step):
        for which in range(2):
            kv_copy(step, which).wait_recv()
            pair_copy(step, which).start()

    def block(i, carry):
        slot = i % n_buf
        for c in copies(i):
            c.wait()
        gate = jnp.dot(u[...], wg[slot], preferred_element_type=jnp.float32).astype(jnp.bfloat16).astype(jnp.float32)
        up = jnp.dot(u[...], wu[slot], preferred_element_type=jnp.float32).astype(jnp.bfloat16).astype(jnp.float32)
        mixed = (gate * jax.nn.sigmoid(gate) * up).astype(jnp.bfloat16)
        acc[...] += jnp.dot(mixed, wd[slot], preferred_element_type=jnp.float32)

        @pl.when(i + n_buf < steps)
        def _():
            for c in copies(i + n_buf):
                c.start()

        @pl.when(i == steps - 12)
        def _():
            relay(1)
            relay(2)

        @pl.when(i == steps - 5)
        def _():
            relay(3)

        return carry

    lax.fori_loop(0, steps, block, 0)
    part_copy = remote(acc.at[pl.ds(tok, tok)], theirs, part_send, part_recv, partner)
    part_copy.start()
    part_copy.wait_recv()
    g_ref[...] = (h_ref[...].astype(jnp.float32) + (acc[:tok, :] + theirs[...])).astype(jnp.bfloat16)
    for step in range(CHIPS):
        for which in range(2):
            pair_copy(step, which).wait()
            if step:
                kv_copy(step, which).wait_send()
    u_copy.wait_send()
    part_copy.wait_send()


def run_mlp(h, k4, v4, w_gate, w_up, w_down, collective_id):
    tok, width = h.shape
    chunk = k4.shape[1]
    bf16, f32 = jnp.bfloat16, jnp.float32
    vmem = pl.BlockSpec(memory_space=pltpu.VMEM)
    hbm = pl.BlockSpec(memory_space=pl.ANY)
    dma = pltpu.SemaphoreType.DMA
    n_buf = 4
    slots = jax.ShapeDtypeStruct((SLOTS, chunk, HEAD), bf16)
    return pl.pallas_call(
        mlp_kernel,
        out_shape=[jax.ShapeDtypeStruct((tok, width), bf16), slots, slots],
        in_specs=[vmem] + [hbm] * 5,
        out_specs=[vmem, hbm, hbm],
        scratch_shapes=[
            pltpu.VMEM((2 * tok, width), bf16),
            pltpu.VMEM((n_buf, width, COL), bf16),
            pltpu.VMEM((n_buf, width, COL), bf16),
            pltpu.VMEM((n_buf, COL, width), bf16),
            pltpu.VMEM((2 * tok, width), f32),
            pltpu.VMEM((tok, width), f32),
            dma((n_buf, 3)), dma, dma, dma, dma,
            dma((CHIPS - 1, 2)), dma((CHIPS - 1, 2)), dma((CHIPS, 2)), dma((CHIPS, 2)),
        ],
        compiler_params=pltpu.CompilerParams(collective_id=collective_id, has_side_effects=True, vmem_limit_bytes=60 * MIB),
        name="mlp",
    )(h, k4, v4, w_gate, w_up, w_down)


def heads_first(cache):
    return lax.optimization_barrier(jnp.transpose(cache, (1, 0, 2)))


def order_kernel(g_ref, y_ref, *refs):
    g_out, y_out = refs[4:6]
    g_out[...] = g_ref[...]
    y_out[...] = y_ref[...]
    for src, dst in zip(refs[:4], refs[6:]):
        for c in range(KV_HEADS):
            dst[:, c, :] = src[c]


def order_outputs(hidden, y_two, *appends):
    tok = hidden.shape[0]
    rows = [jax.ShapeDtypeStruct(t.shape, t.dtype) for t in (hidden, y_two)]
    lines = [jax.ShapeDtypeStruct((tok, KV_HEADS, HEAD), t.dtype) for t in appends]
    vmem = pl.BlockSpec(memory_space=pltpu.VMEM)
    return pl.pallas_call(order_kernel, out_shape=rows + lines, in_specs=[vmem] * 6, out_specs=[vmem] * 6,
                          name="order_outputs")(hidden, y_two, *appends)


def solution(mesh):
    axis_size = mesh.shape['cp']
    rows_spec = P(('dp', 'cp'), None)
    cache_spec = P(('dp', 'cp'), None, None)
    mat_spec = P(None, None)
    vec_spec = P(None)
    layer_specs = (cache_spec, cache_spec, mat_spec, vec_spec, mat_spec, vec_spec, mat_spec, mat_spec)
    in_specs = (rows_spec,) + layer_specs + (mat_spec, mat_spec, mat_spec) + layer_specs
    out_specs = (rows_spec, rows_spec, cache_spec, cache_spec, cache_spec, cache_spec)

    def forward(x_in, cache_k1, cache_v1, w_q1, b_q1, w_k1, b_k1, w_v1, w_o1, w_gate, w_up, w_down, cache_k2, cache_v2, w_q2, b_q2, w_k2, b_k2, w_v2, w_o2):
        n_tok = axis_size * x_in.shape[0]
        trig = rope_table(axis_size * cache_k1.shape[0], n_tok)
        bias = jnp.concatenate([b_q1, b_k1, b_q2, b_k2]).astype(jnp.float32).reshape(1, -1)
        k4a, v4a = heads_first(cache_k1), heads_first(cache_v1)
        k4b, v4b = heads_first(cache_k2), heads_first(cache_v2)
        resid_h, k_one, v_one = run_layer(x_in, bias, trig, k4a, v4a, None, None, w_q1, w_k1, w_v1, w_o1, 1)
        hidden, k_in, v_in = run_mlp(resid_h, k4b, v4b, w_gate, w_up, w_down, 2)
        y_two, k_two, v_two = run_layer(hidden, bias, trig, k4b, v4b, k_in, v_in, w_q2, w_k2, w_v2, w_o2, 3)
        return order_outputs(hidden, y_two, k_one, v_one, k_two, v_two)

    return jax.shard_map(forward, mesh=mesh, in_specs=in_specs, out_specs=out_specs, check_vma=False)
```

```python
import functools

import jax
import jax.numpy as jnp
import numpy as np
from jax import lax
from jax.experimental import pallas as pl
from jax.experimental.pallas import tpu as pltpu
from jax.sharding import PartitionSpec as P

ROPE_THETA = 500000.0
NORM_EPS = 1e-5
LOG2E = 1.4426950408889634
KV_HEADS = 4
HEAD = 128
GROUP = 7
CHIPS = 4
COL = 256
SLOTS = 2 * CHIPS
MIB = 1024 * 1024
MESH = pl.DeviceIdType.MESH


@functools.lru_cache(maxsize=None)
def rope_table(first, count):
    with jax.ensure_compile_time_eval():
        half_dim = HEAD // 2
        inv_freq = 1.0 / (ROPE_THETA ** (jnp.arange(half_dim, dtype=jnp.float32) * (2.0 / HEAD)))
        angles = (first + jnp.arange(count)).astype(jnp.float32)[:, None] * inv_freq[None, :]
        cos_t, sin_t = jnp.cos(angles), jnp.sin(angles)
        return np.asarray(jnp.concatenate([cos_t, cos_t, -sin_t, sin_t], axis=-1))


def norm_rows(wide):
    return (wide * lax.rsqrt(jnp.mean(wide * wide, axis=-1, keepdims=True) + NORM_EPS)).astype(jnp.bfloat16)


def peers():
    me = lax.axis_index('cp')
    chip, core = me // 2, me % 2
    across = [2 * (chip ^ step) + core for step in range(CHIPS)]
    return chip, core, across, 2 * chip + (1 - core)


def meet(others):
    barrier = pltpu.get_barrier_semaphore()
    for dev in others:
        pl.semaphore_signal(barrier, inc=1, device_id={'cp': dev}, device_id_type=MESH)
    pl.semaphore_wait(barrier, len(others))


def remote(src, dst, send_sem, recv_sem, dev):
    return pltpu.make_async_remote_copy(src_ref=src, dst_ref=dst, send_sem=send_sem, recv_sem=recv_sem,
                                        device_id={'cp': dev}, device_id_type=MESH)


def layer_kernel(resharded, a_ref, bias_ref, trig_ref, k4_ref, v4_ref, *refs):
    if resharded:
        kin_ref, vin_ref, wq_ref, wk_ref, wv_ref, wo_ref = refs[:6]
        refs = refs[6:]
    else:
        wq_ref, wk_ref, wv_ref, wo_ref = refs[:4]
        refs = refs[4:]
    (y_ref, knew_ref, vnew_ref, xn, trig, wkv, wo, kb, vb, vt, msg, got, peer_new, newk, newv, qt,
     s_even, s_odd, m_even, m_odd, acc, m_run, l_run, hide, o_send, o_all,
     trig_sem, w_sem, wo_sem, loc_sem, kv_send, kv_recv, pair_send, pair_recv, q_send, q_recv,
     new_send, new_recv, o_ssem, o_rsem) = refs
    chip, core, across, partner = peers()
    me = 2 * chip + core
    scale2 = HEAD ** -0.5 * LOG2E
    tok = a_ref.shape[0]
    chunk = kb.shape[1]
    rows = qt.shape[2]
    wide_cols = GROUP * HEAD
    n_q = wq_ref.shape[1]
    n_items = CHIPS * GROUP
    n_first = (CHIPS - 1) * GROUP
    bias_at = (n_q + wk_ref.shape[1]) if resharded else 0

    def wq_copy(n):
        cols = pl.ds(pl.multiple_of((chip ^ (CHIPS - 1 - n)) * wide_cols, HEAD), wide_cols)
        return pltpu.make_async_copy(wq_ref.at[:, cols], wo.at[:, n * wide_cols:(n + 1) * wide_cols], w_sem.at[2 + n])

    kv_loads = [pltpu.make_async_copy(wk_ref, wkv.at[0], w_sem.at[0]), pltpu.make_async_copy(wv_ref, wkv.at[1], w_sem.at[1])]
    trig_load = pltpu.make_async_copy(trig_ref.at[pl.ds(me * tok, tok)], trig, trig_sem)
    trig_load.start()
    for c in kv_loads + [wq_copy(n) for n in range(CHIPS)]:
        c.start()
    meet(across[1:] + [partner])

    own = [pltpu.make_async_copy(k4_ref.at[chip], kb.at[0], loc_sem.at[0]),
           pltpu.make_async_copy(v4_ref.at[chip], vb.at[0], loc_sem.at[1])]
    for c in own:
        c.start()

    def kv_copy(step, which):
        src, dst = (k4_ref, kb) if which == 0 else (v4_ref, vb)
        return remote(src.at[chip ^ step], dst.at[2 * step], kv_send.at[step - 1, which], kv_recv.at[step - 1, which],
                      across[step])

    def pair_copy(step, which):
        dst = kb if which == 0 else vb
        if step == 0:
            src = (k4_ref if which == 0 else v4_ref).at[chip]
        else:
            src = dst.at[2 * step]
        return remote(src, dst.at[2 * step + 1], pair_send.at[step, which], pair_recv.at[step, which], partner)

    if resharded:
        loads = []
        for j in range(1, SLOTS):
            loads.append((pltpu.make_async_copy(kin_ref.at[j], kb.at[j], loc_sem.at[2 * j]),
                          pltpu.make_async_copy(vin_ref.at[j], vb.at[j], loc_sem.at[2 * j + 1])))
        for pair in loads:
            for c in pair:
                c.start()
    else:
        for which in range(2):
            pair_copy(0, which).start()
        kv_copy(1, 0).start()
        kv_copy(2, 0).start()

    if resharded:
        xn[...] = norm_rows(a_ref[...].astype(jnp.float32))
    else:
        xn[...] = a_ref[...]

    trig_load.wait()

    def rope(plain):
        wide = plain.astype(jnp.float32)
        return (wide * trig[:, :HEAD] + pltpu.roll(wide, HEAD // 2, 1) * trig[:, HEAD:]).astype(jnp.bfloat16)

    kv_loads[0].wait()
    k_pre = (jnp.dot(xn[...], wkv[0], preferred_element_type=jnp.float32)
             + bias_ref[:, bias_at + n_q:bias_at + n_q + KV_HEADS * HEAD].astype(jnp.float32)).astype(jnp.bfloat16)
    for c in range(KV_HEADS):
        knew_ref[c] = rope(k_pre[:, c * HEAD:(c + 1) * HEAD])
    kv_loads[1].wait()
    v_pre = jnp.dot(xn[...], wkv[1], preferred_element_type=jnp.float32).astype(jnp.bfloat16)
    for c in range(KV_HEADS):
        vnew_ref[c] = v_pre[:, c * HEAD:(c + 1) * HEAD]

    def q_copy(n):
        return remote(msg.at[n], got.at[n], q_send.at[n], q_recv.at[n], 2 * (chip ^ (CHIPS - 1 - n)) + core)

    def project(n, carry):
        pltpu.make_async_copy(wo.at[:, :wide_cols], wo.at[:, :wide_cols], w_sem.at[2 + n]).wait()
        grp = chip ^ (CHIPS - 1 - n)
        cols = pl.ds(pl.multiple_of(n * wide_cols, HEAD), wide_cols)
        bias = bias_ref[:, pl.ds(pl.multiple_of(bias_at + grp * wide_cols, HEAD), wide_cols)].astype(jnp.float32)
        q_pre = (jnp.dot(xn[...], wo[:, cols], preferred_element_type=jnp.float32) + bias).astype(jnp.bfloat16)
        for g in range(GROUP):
            msg[n, g] = rope(q_pre[:, g * HEAD:(g + 1) * HEAD])
        msg[n, GROUP] = knew_ref[grp]
        msg[n, GROUP + 1] = vnew_ref[grp]

        @pl.when(n < CHIPS - 1)
        def _():
            q_copy(n).start()

        return carry

    lax.fori_loop(0, CHIPS, project, 0)
    q_copies = [q_copy(n) for n in range(CHIPS - 1)]
    parts = [msg.at[CHIPS - 1]] + [got.at[CHIPS - 1 - s] for s in range(1, CHIPS)]
    wo_load = pltpu.make_async_copy(wo_ref, wo, wo_sem)
    if not resharded:
        for step, which in ((1, 1), (2, 1), (3, 0), (3, 1)):
            kv_copy(step, which).start()
    wo_load.start()
    acc[...] = jnp.zeros_like(acc)
    m_run[...] = jnp.full_like(m_run, -jnp.inf)
    l_run[...] = jnp.zeros_like(l_run)
    for c in q_copies:
        c.wait_recv()
    new_copies = [remote(parts[s].at[pl.ds(GROUP, 2)], peer_new.at[s], new_send.at[s], new_recv.at[s], partner) for s in range(CHIPS)]
    for c in new_copies:
        c.start()
    for g in range(GROUP):
        qt[g] = jnp.concatenate([p[g] for p in parts], axis=0).T
    for s in range(CHIPS):
        newk[s * tok:(s + 1) * tok, :] = parts[s][GROUP]
        newv[s * tok:(s + 1) * tok, :] = parts[s][GROUP + 1]

    def ready(j):
        for jj in range(CHIPS):
            @pl.when(j == jj)
            def _():
                if jj == 0:
                    for c in own:
                        c.wait()
                elif resharded:
                    for c in loads[2 * jj - 1]:
                        c.wait()
                else:
                    for which in range(2):
                        kv_copy(jj, which).wait_recv()
                        pair_copy(jj, which).start()
        vt[j % 2, :, :chunk] = vb[2 * j].T
        for jj in range(CHIPS):
            @pl.when(j == jj)
            def _():
                if resharded:
                    for c in loads[2 * jj]:
                        c.wait()
                else:
                    for which in range(2):
                        pair_copy(jj, which).wait_recv()
        vt[j % 2, :, chunk:] = vb[2 * j + 1].T

    def place(item):
        return item // GROUP, item % GROUP

    def score(item, s_dst, m_dst):
        j, g = place(item)
        part = jnp.full((8, rows), -jnp.inf, jnp.float32)
        for t in range(2 * chunk // 256):
            at = (t * 256) % chunk
            s_blk = jnp.dot(kb[2 * j + t * 256 // chunk, at:at + 256, :], qt[g], preferred_element_type=jnp.float32)
            s_dst[t * 256:(t + 1) * 256, :] = s_blk
            part = jnp.maximum(part, jnp.max(s_blk.reshape(32, 8, rows), axis=0))
        m_dst[...] = part

    def absorb(item, s_src, m_src):
        j, g = place(item)
        m_old = m_run[g]
        m_new = jnp.maximum(m_old, jnp.max(m_src[...], axis=0, keepdims=True))
        alpha = jnp.exp2((m_old - m_new) * scale2)
        shift = m_new * scale2
        l_part = jnp.zeros((8, rows), jnp.float32)
        out = jnp.zeros((HEAD, rows), jnp.float32)
        for t in range(2 * chunk // 256):
            p = jnp.exp2(s_src[t * 256:(t + 1) * 256, :] * scale2 - shift)
            l_part = l_part + jnp.sum(p.reshape(32, 8, rows), axis=0)
            out = out + jnp.dot(vt[j % 2, :, t * 256:(t + 1) * 256], p.astype(jnp.bfloat16),
                                preferred_element_type=jnp.float32)
        acc[g] = acc[g] * alpha + out
        l_run[g] = l_run[g] * alpha + l_part
        m_run[g] = m_new

    ready(0)
    score(0, s_even, m_even)

    new_len = newk.shape[0]

    key_i = lax.broadcasted_iota(jnp.int32, (new_len, rows), 0)
    qry_i = lax.broadcasted_iota(jnp.int32, (new_len, rows), 1)
    blk = key_i // tok
    k_pos = (2 * (chip ^ (blk % CHIPS)) + (core ^ (blk // CHIPS))) * tok + key_i % tok
    q_pos = (2 * (chip ^ (qry_i // tok)) + core) * tok + qry_i % tok
    hide[...] = jnp.where(k_pos <= q_pos, 0.0, -jnp.inf)

    def o_copy(g, s):
        src = o_send.at[g, s]
        dst = o_all.at[:, pl.ds(pl.multiple_of(chip * wide_cols + g * HEAD, HEAD), HEAD)]
        return remote(src, dst, o_ssem.at[g, s - 1], o_rsem.at[g, s - 1], across[s])

    def finish(g):
        s = jnp.dot(newk[...], qt[g], preferred_element_type=jnp.float32) + hide[...]
        m_old = m_run[g]
        m_new = jnp.maximum(m_old, jnp.max(s, axis=0, keepdims=True))
        alpha = jnp.exp2((m_old - m_new) * scale2)
        p = jnp.exp2(s * scale2 - m_new * scale2)
        total = jnp.sum(l_run[g] * alpha, axis=0, keepdims=True) + jnp.sum(p, axis=0, keepdims=True)
        fresh = lax.dot_general(newv[...], p.astype(jnp.bfloat16), (((0,), (0,)), ((), ())),
                                preferred_element_type=jnp.float32)
        out = ((acc[g] * alpha + fresh) / total).T.astype(jnp.bfloat16)
        for s_i in range(1, CHIPS):
            o_send[g, s_i] = out[s_i * tok:(s_i + 1) * tok, :]
            o_copy(g, s_i).start()
        o_all[:, pl.ds(pl.multiple_of(chip * wide_cols + g * HEAD, HEAD), HEAD)] = out[:tok, :]

    def step(item, carry):
        nxt = item + 1

        @pl.when((nxt % GROUP == 0) & (nxt < n_items))
        def _():
            ready(nxt // GROUP)

        @pl.when(item == n_first)
        def _():
            for c in new_copies:
                c.wait_recv()
            for s in range(CHIPS):
                at = (CHIPS + s) * tok
                newk[at:at + tok, :] = peer_new[s, 0]
                newv[at:at + tok, :] = peer_new[s, 1]

        after = jnp.minimum(nxt, n_items - 1)

        @pl.when(item % 2 == 0)
        def _():
            score(after, s_odd, m_odd)
            absorb(item, s_even, m_even)

        @pl.when(item % 2 == 1)
        def _():
            score(after, s_even, m_even)
            absorb(item, s_odd, m_odd)

        @pl.when(item >= n_first)
        def _():
            finish(item - n_first)

        return carry

    lax.fori_loop(0, n_items, step, 0)
    o_copies = [o_copy(g, s) for g in range(GROUP) for s in range(1, CHIPS)]
    wo_load.wait()
    for c in o_copies:
        c.wait_recv()

    def out_proj(blk, carry):
        cols = pl.ds(pl.multiple_of(blk * COL, COL), COL)
        y = jnp.dot(o_all[...], wo[:, cols], preferred_element_type=jnp.float32).astype(jnp.bfloat16)
        if not resharded:
            y = (a_ref[:, cols].astype(jnp.float32) + y.astype(jnp.float32)).astype(jnp.bfloat16)
        y_ref[:, cols] = y
        return carry

    lax.fori_loop(0, wo.shape[1] // COL, out_proj, 0)

    for c in q_copies + new_copies + o_copies:
        c.wait_send()
    if not resharded:
        for step in range(CHIPS):
            for which in range(2):
                pair_copy(step, which).wait_send()
                if step:
                    kv_copy(step, which).wait_send()


def run_layer(a, bias, trig, k4, v4, k_in, v_in, w_q, w_k, w_v, w_o, collective_id):
    resharded = k_in is not None
    tok, width = a.shape
    chunk = k4.shape[1]
    rows = CHIPS * tok
    bf16, f32 = jnp.bfloat16, jnp.float32
    vmem = pl.BlockSpec(memory_space=pltpu.VMEM)
    hbm = pl.BlockSpec(memory_space=pl.ANY)
    dma = pltpu.SemaphoreType.DMA
    caches = (k4, v4, k_in, v_in) if resharded else (k4, v4)
    return pl.pallas_call(
        functools.partial(layer_kernel, resharded),
        out_shape=[jax.ShapeDtypeStruct((tok, width), bf16),
                   jax.ShapeDtypeStruct((KV_HEADS, tok, HEAD), bf16),
                   jax.ShapeDtypeStruct((KV_HEADS, tok, HEAD), bf16)],
        in_specs=[vmem] * 2 + [hbm] * (len(caches) + 5),
        out_specs=[vmem] * 3,
        scratch_shapes=[
            pltpu.VMEM((tok, width), bf16),
            pltpu.VMEM((tok, 2 * HEAD), f32),
            pltpu.VMEM((2,) + w_k.shape, bf16),
            pltpu.VMEM(w_o.shape, bf16),
            pltpu.VMEM((SLOTS, chunk, HEAD), bf16),
            pltpu.VMEM((SLOTS, chunk, HEAD), bf16),
            pltpu.VMEM((2, HEAD, 2 * chunk), bf16),
            pltpu.VMEM((KV_HEADS, GROUP + 2, tok, HEAD), bf16),
            pltpu.VMEM((CHIPS - 1, GROUP + 2, tok, HEAD), bf16),
            pltpu.VMEM((CHIPS, 2, tok, HEAD), bf16),
            pltpu.VMEM((2 * rows, HEAD), bf16),
            pltpu.VMEM((2 * rows, HEAD), bf16),
            pltpu.VMEM((GROUP, HEAD, rows), bf16),
            pltpu.VMEM((2 * chunk, rows), f32),
            pltpu.VMEM((2 * chunk, rows), f32),
            pltpu.VMEM((8, rows), f32),
            pltpu.VMEM((8, rows), f32),
            pltpu.VMEM((GROUP, HEAD, rows), f32),
            pltpu.VMEM((GROUP, 1, rows), f32),
            pltpu.VMEM((GROUP, 8, rows), f32),
            pltpu.VMEM((2 * rows, rows), f32),
            pltpu.VMEM((GROUP, CHIPS, tok, HEAD), bf16),
            pltpu.VMEM((tok, CHIPS * GROUP * HEAD), bf16),
            dma, dma((2 + CHIPS,)), dma, dma((2 * SLOTS,)),
            dma((CHIPS - 1, 2)), dma((CHIPS - 1, 2)), dma((CHIPS, 2)), dma((CHIPS, 2)),
            dma((CHIPS - 1,)), dma((CHIPS - 1,)), dma((CHIPS,)), dma((CHIPS,)),
            dma((GROUP, CHIPS - 1)), dma((GROUP, CHIPS - 1)),
        ],
        compiler_params=pltpu.CompilerParams(collective_id=collective_id, has_side_effects=True, vmem_limit_bytes=60 * MIB),
        name="layer",
    )(a, bias, trig, *caches, w_q, w_k, w_v, w_o)


def mlp_kernel(h_ref, k4_ref, v4_ref, gate_ref, up_ref, down_ref, g_ref, kout_ref, vout_ref,
               u, wg, wu, wd, acc, theirs, w_sem, u_send, u_recv, part_send, part_recv, kv_send, kv_recv, pair_send, pair_recv):
    chip, core, across, partner = peers()
    tok = h_ref.shape[0]
    n_buf = wg.shape[0]
    steps = gate_ref.shape[1] // (2 * COL)

    def copies(i):
        slot = i % n_buf
        cols = pl.ds(pl.multiple_of((core * steps + i) * COL, COL), COL)
        return (pltpu.make_async_copy(gate_ref.at[:, cols], wg.at[slot], w_sem.at[slot, 0]),
                pltpu.make_async_copy(up_ref.at[:, cols], wu.at[slot], w_sem.at[slot, 1]),
                pltpu.make_async_copy(down_ref.at[cols, :], wd.at[slot], w_sem.at[slot, 2]))

    for b in range(n_buf):
        for c in copies(b):
            c.start()
    meet(across[1:] + [partner])
    u[:tok, :] = norm_rows(h_ref[...].astype(jnp.float32))
    u_copy = remote(u.at[pl.ds(0, tok)], u.at[pl.ds(tok, tok)], u_send, u_recv, partner)
    u_copy.start()

    def kv_copy(step, which):
        src, dst = (k4_ref, kout_ref) if which == 0 else (v4_ref, vout_ref)
        return remote(src.at[chip ^ step], dst.at[2 * step], kv_send.at[step - 1, which], kv_recv.at[step - 1, which],
                      across[step])

    def pair_copy(step, which):
        dst = kout_ref if which == 0 else vout_ref
        src = (k4_ref if which == 0 else v4_ref).at[chip] if step == 0 else dst.at[2 * step]
        return remote(src, dst.at[2 * step + 1], pair_send.at[step, which], pair_recv.at[step, which], partner)

    for step in range(1, CHIPS):
        for which in range(2):
            kv_copy(step, which).start()
    for which in range(2):
        pair_copy(0, which).start()
    acc[...] = jnp.zeros_like(acc)
    u_copy.wait_recv()

    def relay(step):
        for which in range(2):
            kv_copy(step, which).wait_recv()
            pair_copy(step, which).start()

    def block(i, carry):
        slot = i % n_buf
        for c in copies(i):
            c.wait()
        gate = jnp.dot(u[...], wg[slot], preferred_element_type=jnp.float32).astype(jnp.bfloat16).astype(jnp.float32)
        up = jnp.dot(u[...], wu[slot], preferred_element_type=jnp.float32).astype(jnp.bfloat16).astype(jnp.float32)
        mixed = (gate * jax.nn.sigmoid(gate) * up).astype(jnp.bfloat16)
        acc[...] += jnp.dot(mixed, wd[slot], preferred_element_type=jnp.float32)

        @pl.when(i + n_buf < steps)
        def _():
            for c in copies(i + n_buf):
                c.start()

        @pl.when(i == steps - 12)
        def _():
            relay(1)
            relay(2)

        @pl.when(i == steps - 5)
        def _():
            relay(3)

        return carry

    lax.fori_loop(0, steps, block, 0)
    part_copy = remote(acc.at[pl.ds(tok, tok)], theirs, part_send, part_recv, partner)
    part_copy.start()
    part_copy.wait_recv()
    g_ref[...] = (h_ref[...].astype(jnp.float32) + (acc[:tok, :] + theirs[...])).astype(jnp.bfloat16)
    for step in range(CHIPS):
        for which in range(2):
            pair_copy(step, which).wait()
            if step:
                kv_copy(step, which).wait_send()
    u_copy.wait_send()
    part_copy.wait_send()


def run_mlp(h, k4, v4, w_gate, w_up, w_down, collective_id):
    tok, width = h.shape
    chunk = k4.shape[1]
    bf16, f32 = jnp.bfloat16, jnp.float32
    vmem = pl.BlockSpec(memory_space=pltpu.VMEM)
    hbm = pl.BlockSpec(memory_space=pl.ANY)
    dma = pltpu.SemaphoreType.DMA
    n_buf = 4
    slots = jax.ShapeDtypeStruct((SLOTS, chunk, HEAD), bf16)
    return pl.pallas_call(
        mlp_kernel,
        out_shape=[jax.ShapeDtypeStruct((tok, width), bf16), slots, slots],
        in_specs=[vmem] + [hbm] * 5,
        out_specs=[vmem, hbm, hbm],
        scratch_shapes=[
            pltpu.VMEM((2 * tok, width), bf16),
            pltpu.VMEM((n_buf, width, COL), bf16),
            pltpu.VMEM((n_buf, width, COL), bf16),
            pltpu.VMEM((n_buf, COL, width), bf16),
            pltpu.VMEM((2 * tok, width), f32),
            pltpu.VMEM((tok, width), f32),
            dma((n_buf, 3)), dma, dma, dma, dma,
            dma((CHIPS - 1, 2)), dma((CHIPS - 1, 2)), dma((CHIPS, 2)), dma((CHIPS, 2)),
        ],
        compiler_params=pltpu.CompilerParams(collective_id=collective_id, has_side_effects=True, vmem_limit_bytes=60 * MIB),
        name="mlp",
    )(h, k4, v4, w_gate, w_up, w_down)


def heads_first(cache):
    return lax.optimization_barrier(jnp.transpose(cache, (1, 0, 2)))


def order_kernel(g_ref, y_ref, *refs):
    g_out, y_out = refs[4:6]
    g_out[...] = g_ref[...]
    y_out[...] = y_ref[...]
    for src, dst in zip(refs[:4], refs[6:]):
        for c in range(KV_HEADS):
            dst[:, c, :] = src[c]


def order_outputs(hidden, y_two, *appends):
    tok = hidden.shape[0]
    rows = [jax.ShapeDtypeStruct(t.shape, t.dtype) for t in (hidden, y_two)]
    lines = [jax.ShapeDtypeStruct((tok, KV_HEADS, HEAD), t.dtype) for t in appends]
    vmem = pl.BlockSpec(memory_space=pltpu.VMEM)
    return pl.pallas_call(order_kernel, out_shape=rows + lines, in_specs=[vmem] * 6, out_specs=[vmem] * 6,
                          name="order_outputs")(hidden, y_two, *appends)


def solution(mesh):
    axis_size = mesh.shape['cp']
    rows_spec = P(('dp', 'cp'), None)
    cache_spec = P(('dp', 'cp'), None, None)
    mat_spec = P(None, None)
    vec_spec = P(None)
    layer_specs = (cache_spec, cache_spec, mat_spec, vec_spec, mat_spec, vec_spec, mat_spec, mat_spec)
    in_specs = (rows_spec,) + layer_specs + (mat_spec, mat_spec, mat_spec) + layer_specs
    out_specs = (rows_spec, rows_spec, cache_spec, cache_spec, cache_spec, cache_spec)

    def forward(x_in, cache_k1, cache_v1, w_q1, b_q1, w_k1, b_k1, w_v1, w_o1, w_gate, w_up, w_down, cache_k2, cache_v2, w_q2, b_q2, w_k2, b_k2, w_v2, w_o2):
        n_tok = axis_size * x_in.shape[0]
        trig = rope_table(axis_size * cache_k1.shape[0], n_tok)
        bias = jnp.concatenate([b_q1, b_k1, b_q2, b_k2]).reshape(1, -1)
        k4a, v4a = heads_first(cache_k1), heads_first(cache_v1)
        k4b, v4b = heads_first(cache_k2), heads_first(cache_v2)
        resid_h, k_one, v_one = run_layer(x_in, bias, trig, k4a, v4a, None, None, w_q1, w_k1, w_v1, w_o1, 1)
        hidden, k_in, v_in = run_mlp(resid_h, k4b, v4b, w_gate, w_up, w_down, 2)
        y_two, k_two, v_two = run_layer(hidden, bias, trig, k4b, v4b, k_in, v_in, w_q2, w_k2, w_v2, w_o2, 3)
        return order_outputs(hidden, y_two, k_one, v_one, k_two, v_two)

    return jax.shard_map(forward, mesh=mesh, in_specs=in_specs, out_specs=out_specs, check_vma=False)
```

```python
import functools

import jax
import jax.numpy as jnp
import numpy as np
from jax import lax
from jax.experimental import pallas as pl
from jax.experimental.pallas import tpu as pltpu
from jax.sharding import PartitionSpec as P

ROPE_THETA = 500000.0
NORM_EPS = 1e-5
LOG2E = 1.4426950408889634
KV_HEADS = 4
HEAD = 128
GROUP = 7
CHIPS = 4
COL = 256
SLOTS = 2 * CHIPS
MIB = 1024 * 1024
VMEM_ALL = 67_000_000
MESH = pl.DeviceIdType.MESH


@functools.lru_cache(maxsize=None)
def rope_table(first, count):
    with jax.ensure_compile_time_eval():
        half_dim = HEAD // 2
        inv_freq = 1.0 / (ROPE_THETA ** (jnp.arange(half_dim, dtype=jnp.float32) * (2.0 / HEAD)))
        angles = (first + jnp.arange(count)).astype(jnp.float32)[:, None] * inv_freq[None, :]
        cos_t, sin_t = jnp.cos(angles), jnp.sin(angles)
        return np.asarray(jnp.concatenate([cos_t, cos_t, -sin_t, sin_t], axis=-1))


def norm_rows(wide):
    return (wide * lax.rsqrt(jnp.mean(wide * wide, axis=-1, keepdims=True) + NORM_EPS)).astype(jnp.bfloat16)


def peers():
    me = lax.axis_index('cp')
    chip, core = me // 2, me % 2
    across = [2 * (chip ^ step) + core for step in range(CHIPS)]
    return chip, core, across, 2 * chip + (1 - core)


def meet(others):
    barrier = pltpu.get_barrier_semaphore()
    for dev in others:
        pl.semaphore_signal(barrier, inc=1, device_id={'cp': dev}, device_id_type=MESH)
    pl.semaphore_wait(barrier, len(others))


def remote(src, dst, send_sem, recv_sem, dev):
    return pltpu.make_async_remote_copy(src_ref=src, dst_ref=dst, send_sem=send_sem, recv_sem=recv_sem,
                                        device_id={'cp': dev}, device_id_type=MESH)


PIECE = 256
RING = 4


def pack_start(src_ref, raw, sem):
    for i in range(RING):
        pltpu.make_async_copy(src_ref.at[pl.ds(i * PIECE, PIECE)], raw.at[i], sem.at[i]).start()


def pack_heads(src_ref, raw, tmp, sem, put):
    n = src_ref.shape[0] // PIECE

    def piece(i, carry):
        slot = i % RING
        pltpu.make_async_copy(raw.at[slot], raw.at[slot], sem.at[slot]).wait()
        for part in range(2):
            half = PIECE // 2
            flat = jnp.swapaxes(raw[slot, part * half:(part + 1) * half], 0, 1)
            for c in range(KV_HEADS):
                tmp[c, part * half:(part + 1) * half, :] = flat[c]

        @pl.when(i + RING < n)
        def _():
            pltpu.make_async_copy(src_ref.at[pl.ds((i + RING) * PIECE, PIECE)], raw.at[slot], sem.at[slot]).start()

        put(pl.ds(pl.multiple_of(i * PIECE, PIECE), PIECE))
        return carry

    lax.fori_loop(0, n, piece, 0)


def layer_kernel(resharded, a_ref, bias_ref, trig_ref, kin_ref, vin_ref, wq_ref, wk_ref, wv_ref, wo_ref, *refs):
    if not resharded:
        raw_k, raw_v, tmp, k_out, v_out, raw_sem = refs[-6:]
        refs = refs[:-6]
    (y_ref, knew_ref, vnew_ref, xn, trig, wkv, wo, kb, vb, vt, msg, got, peer_new, newk, newv, qt,
     s_even, s_odd, m_even, m_odd, acc, m_run, l_run, hide, o_send, o_all, y_acc,
     trig_sem, w_sem, wo_sem, loc_sem, kv_send, kv_recv, pair_send, pair_recv, q_send, q_recv,
     new_send, new_recv, o_ssem, o_rsem) = refs
    chip, core, across, partner = peers()
    me = 2 * chip + core
    scale2 = HEAD ** -0.5 * LOG2E
    tok = a_ref.shape[0]
    chunk = kb.shape[1]
    rows = qt.shape[2]
    wide_cols = GROUP * HEAD
    n_q = wq_ref.shape[1]
    n_items = CHIPS * GROUP
    n_first = (CHIPS - 1) * GROUP
    bias_at = (n_q + wk_ref.shape[1]) if resharded else 0

    def wq_copy(n):
        cols = pl.ds(pl.multiple_of((chip ^ (CHIPS - 1 - n)) * wide_cols, HEAD), wide_cols)
        return pltpu.make_async_copy(wq_ref.at[:, cols], wo.at[:, n * wide_cols:(n + 1) * wide_cols], w_sem.at[2 + n])

    kv_loads = [pltpu.make_async_copy(wk_ref, wkv.at[0], w_sem.at[0]), pltpu.make_async_copy(wv_ref, wkv.at[1], w_sem.at[1])]
    trig_load = pltpu.make_async_copy(trig_ref.at[pl.ds(me * tok, tok)], trig, trig_sem)
    if not resharded:
        pack_start(kin_ref, raw_k, raw_sem.at[0])
        pack_start(vin_ref, raw_v, raw_sem.at[1])
    trig_load.start()
    for c in kv_loads + [wq_copy(n) for n in range(CHIPS)]:
        c.start()
    meet(across[1:] + [partner])

    halves = [pl.ds(h * (chunk // 2), chunk // 2) for h in range(2)]

    def kv_copy(step, which, h):
        src, dst = (k_out, kb) if which == 0 else (v_out, vb)
        return remote(src.at[step - 1, halves[h]], dst.at[2 * step, halves[h]], kv_send.at[step - 1, which, h],
                      kv_recv.at[step - 1, which, h], across[step])

    def pair_copy(step, which, h):
        dst = kb if which == 0 else vb
        return remote(dst.at[2 * step, halves[h]], dst.at[2 * step + 1, halves[h]], pair_send.at[step, which, h],
                      pair_recv.at[step, which, h], partner)

    if resharded:
        loads = []
        for j in range(SLOTS):
            loads.append((pltpu.make_async_copy(kin_ref.at[j], kb.at[j], loc_sem.at[2 * j]),
                          pltpu.make_async_copy(vin_ref.at[j], vb.at[j], loc_sem.at[2 * j + 1])))
        for pair in loads:
            for c in pair:
                c.start()
    else:
        def put(mine, out):
            def store(span):
                mine[0, span, :] = tmp[chip]
                for step in range(1, CHIPS):
                    out[step - 1, span, :] = tmp[chip ^ step]
            return store

        pack_heads(kin_ref, raw_k, tmp, raw_sem.at[0], put(kb, k_out))
        for h in range(2):
            for step in (1, 2):
                kv_copy(step, 0, h).start()
        pack_heads(vin_ref, raw_v, tmp, raw_sem.at[1], put(vb, v_out))
        for which in range(2):
            for h in range(2):
                pair_copy(0, which, h).start()

    if resharded:
        xn[...] = norm_rows(a_ref[...].astype(jnp.float32))
    else:
        xn[...] = a_ref[...]

    trig_load.wait()

    def rope(plain):
        wide = plain.astype(jnp.float32)
        return (wide * trig[:, :HEAD] + pltpu.roll(wide, HEAD // 2, 1) * trig[:, HEAD:]).astype(jnp.bfloat16)

    kv_loads[0].wait()
    k_pre = (jnp.dot(xn[...], wkv[0], preferred_element_type=jnp.float32)
             + bias_ref[:, bias_at + n_q:bias_at + n_q + KV_HEADS * HEAD].astype(jnp.float32)).astype(jnp.bfloat16)
    for c in range(KV_HEADS):
        knew_ref[c] = rope(k_pre[:, c * HEAD:(c + 1) * HEAD])
    kv_loads[1].wait()
    v_pre = jnp.dot(xn[...], wkv[1], preferred_element_type=jnp.float32).astype(jnp.bfloat16)
    for c in range(KV_HEADS):
        vnew_ref[c] = v_pre[:, c * HEAD:(c + 1) * HEAD]

    def q_copy(n):
        return remote(msg.at[n], got.at[n], q_send.at[n], q_recv.at[n], 2 * (chip ^ (CHIPS - 1 - n)) + core)

    def project(n, carry):
        pltpu.make_async_copy(wo.at[:, :wide_cols], wo.at[:, :wide_cols], w_sem.at[2 + n]).wait()
        grp = chip ^ (CHIPS - 1 - n)
        cols = pl.ds(pl.multiple_of(n * wide_cols, HEAD), wide_cols)
        bias = bias_ref[:, pl.ds(pl.multiple_of(bias_at + grp * wide_cols, HEAD), wide_cols)].astype(jnp.float32)
        q_pre = (jnp.dot(xn[...], wo[:, cols], preferred_element_type=jnp.float32) + bias).astype(jnp.bfloat16)
        for g in range(GROUP):
            msg[n, g] = rope(q_pre[:, g * HEAD:(g + 1) * HEAD])
        msg[n, GROUP] = knew_ref[grp]
        msg[n, GROUP + 1] = vnew_ref[grp]

        @pl.when(n < CHIPS - 1)
        def _():
            q_copy(n).start()

        return carry

    lax.fori_loop(0, CHIPS, project, 0)
    q_copies = [q_copy(n) for n in range(CHIPS - 1)]
    parts = [msg.at[CHIPS - 1]] + [got.at[CHIPS - 1 - s] for s in range(1, CHIPS)]
    wo_load = pltpu.make_async_copy(wo_ref, wo, wo_sem)
    if not resharded:
        for h in range(2):
            for step in (1, 2):
                kv_copy(step, 1, h).start()
        for h in range(2):
            for which in range(2):
                kv_copy(3, which, h).start()
    wo_load.start()
    acc[...] = jnp.zeros_like(acc)
    m_run[...] = jnp.full_like(m_run, -jnp.inf)
    l_run[...] = jnp.zeros_like(l_run)
    for c in q_copies:
        c.wait_recv()
    new_copies = [remote(parts[s].at[pl.ds(GROUP, 2)], peer_new.at[s], new_send.at[s], new_recv.at[s], partner) for s in range(CHIPS)]
    for c in new_copies:
        c.start()
    for g in range(GROUP):
        qt[g] = jnp.concatenate([p[g] for p in parts], axis=0).T
    for s in range(CHIPS):
        newk[s * tok:(s + 1) * tok, :] = parts[s][GROUP]
        newv[s * tok:(s + 1) * tok, :] = parts[s][GROUP + 1]

    def ready(j):
        for jj in range(CHIPS):
            @pl.when(j == jj)
            def _():
                if resharded:
                    for c in loads[2 * jj]:
                        c.wait()
                elif jj:
                    for h in range(2):
                        for which in range(2):
                            kv_copy(jj, which, h).wait_recv()
                            pair_copy(jj, which, h).start()
        vt[j % 2, :, :chunk] = vb[2 * j].T
        for jj in range(CHIPS):
            @pl.when(j == jj)
            def _():
                if resharded:
                    for c in loads[2 * jj + 1]:
                        c.wait()
                else:
                    for h in range(2):
                        for which in range(2):
                            pair_copy(jj, which, h).wait_recv()
        vt[j % 2, :, chunk:] = vb[2 * j + 1].T

    def place(item):
        return item // GROUP, item % GROUP

    def score(item, s_dst, m_dst):
        j, g = place(item)
        part = jnp.full((8, rows), -jnp.inf, jnp.float32)
        for t in range(2 * chunk // 256):
            at = (t * 256) % chunk
            s_blk = jnp.dot(kb[2 * j + t * 256 // chunk, at:at + 256, :], qt[g], preferred_element_type=jnp.float32)
            s_dst[t * 256:(t + 1) * 256, :] = s_blk
            part = jnp.maximum(part, jnp.max(s_blk.reshape(32, 8, rows), axis=0))
        m_dst[...] = part

    def absorb(item, s_src, m_src):
        j, g = place(item)
        m_old = m_run[g]
        m_new = jnp.maximum(m_old, jnp.max(m_src[...], axis=0, keepdims=True))
        alpha = jnp.exp2((m_old - m_new) * scale2)
        shift = m_new * scale2
        l_part = jnp.zeros((8, rows), jnp.float32)
        out = jnp.zeros((HEAD, rows), jnp.float32)
        for t in range(2 * chunk // 256):
            p = jnp.exp2(s_src[t * 256:(t + 1) * 256, :] * scale2 - shift)
            l_part = l_part + jnp.sum(p.reshape(32, 8, rows), axis=0)
            out = out + jnp.dot(vt[j % 2, :, t * 256:(t + 1) * 256], p.astype(jnp.bfloat16),
                                preferred_element_type=jnp.float32)
        acc[g] = acc[g] * alpha + out
        l_run[g] = l_run[g] * alpha + l_part
        m_run[g] = m_new

    ready(0)
    score(0, s_even, m_even)

    new_len = newk.shape[0]

    key_i = lax.broadcasted_iota(jnp.int32, (new_len, rows), 0)
    qry_i = lax.broadcasted_iota(jnp.int32, (new_len, rows), 1)
    blk = key_i // tok
    k_pos = (2 * (chip ^ (blk % CHIPS)) + (core ^ (blk // CHIPS))) * tok + key_i % tok
    q_pos = (2 * (chip ^ (qry_i // tok)) + core) * tok + qry_i % tok
    hide[...] = jnp.where(k_pos <= q_pos, 0.0, -jnp.inf)

    def o_copy(g, s):
        src = o_send.at[g, s]
        dst = o_all.at[:, pl.ds(pl.multiple_of(chip * wide_cols + g * HEAD, HEAD), HEAD)]
        return remote(src, dst, o_ssem.at[g, s - 1], o_rsem.at[g, s - 1], across[s])

    def finish(g):
        s = jnp.dot(newk[...], qt[g], preferred_element_type=jnp.float32) + hide[...]
        m_old = m_run[g]
        m_new = jnp.maximum(m_old, jnp.max(s, axis=0, keepdims=True))
        alpha = jnp.exp2((m_old - m_new) * scale2)
        p = jnp.exp2(s * scale2 - m_new * scale2)
        total = jnp.sum(l_run[g] * alpha, axis=0, keepdims=True) + jnp.sum(p, axis=0, keepdims=True)
        fresh = lax.dot_general(newv[...], p.astype(jnp.bfloat16), (((0,), (0,)), ((), ())),
                                preferred_element_type=jnp.float32)
        out = ((acc[g] * alpha + fresh) / total).T.astype(jnp.bfloat16)
        for s_i in range(1, CHIPS):
            o_send[g, s_i] = out[s_i * tok:(s_i + 1) * tok, :]
            o_copy(g, s_i).start()
        o_all[:, pl.ds(pl.multiple_of(chip * wide_cols + g * HEAD, HEAD), HEAD)] = out[:tok, :]

    def step(item, carry):
        nxt = item + 1

        @pl.when((nxt % GROUP == 0) & (nxt < n_items))
        def _():
            ready(nxt // GROUP)

        @pl.when(item == n_first)
        def _():
            for c in new_copies:
                c.wait_recv()
            for s in range(CHIPS):
                at = (CHIPS + s) * tok
                newk[at:at + tok, :] = peer_new[s, 0]
                newv[at:at + tok, :] = peer_new[s, 1]

        after = jnp.minimum(nxt, n_items - 1)

        @pl.when(item % 2 == 0)
        def _():
            score(after, s_odd, m_odd)
            absorb(item, s_even, m_even)

        @pl.when(item % 2 == 1)
        def _():
            score(after, s_even, m_even)
            absorb(item, s_odd, m_odd)

        @pl.when(item >= n_first)
        def _():
            finish(item - n_first)

        return carry

    lax.fori_loop(0, n_items, step, 0)
    o_copies = [o_copy(g, s) for g in range(GROUP) for s in range(1, CHIPS)]
    last = 3 * (GROUP - 1)
    wo_load.wait()
    for c in o_copies[:last]:
        c.wait_recv()

    def heads(s, first, count):
        at = pl.multiple_of((chip ^ s) * wide_cols + first * HEAD, HEAD)
        return pl.ds(at, count * HEAD)

    def early_proj(blk, carry):
        cols = pl.ds(pl.multiple_of(blk * COL, COL), COL)
        total = jnp.zeros((tok, COL), jnp.float32)
        for s in range(CHIPS):
            part = heads(s, 0, GROUP if s == 0 else GROUP - 1)
            total = total + jnp.dot(o_all[:, part], wo[part, cols], preferred_element_type=jnp.float32)
        y_acc[:, cols] = total
        return carry

    lax.fori_loop(0, wo.shape[1] // COL, early_proj, 0)
    for c in o_copies[last:]:
        c.wait_recv()

    def out_proj(blk, carry):
        cols = pl.ds(pl.multiple_of(blk * 2 * COL, 2 * COL), 2 * COL)
        total = y_acc[:, cols]
        for s in range(1, CHIPS):
            part = heads(s, GROUP - 1, 1)
            total = total + jnp.dot(o_all[:, part], wo[part, cols], preferred_element_type=jnp.float32)
        y = total.astype(jnp.bfloat16)
        if not resharded:
            y = (a_ref[:, cols].astype(jnp.float32) + y.astype(jnp.float32)).astype(jnp.bfloat16)
        y_ref[:, cols] = y
        return carry

    lax.fori_loop(0, wo.shape[1] // (2 * COL), out_proj, 0)

    for c in q_copies + new_copies + o_copies:
        c.wait_send()
    if not resharded:
        for step in range(CHIPS):
            for which in range(2):
                for h in range(2):
                    pair_copy(step, which, h).wait_send()
                    if step:
                        kv_copy(step, which, h).wait_send()


def run_layer(resharded, a, bias, trig, k_in, v_in, w_q, w_k, w_v, w_o, collective_id):
    tok, width = a.shape
    chunk = k_in.shape[1] if resharded else k_in.shape[0]
    rows = CHIPS * tok
    bf16, f32 = jnp.bfloat16, jnp.float32
    vmem = pl.BlockSpec(memory_space=pltpu.VMEM)
    hbm = pl.BlockSpec(memory_space=pl.ANY)
    dma = pltpu.SemaphoreType.DMA
    packing = [] if resharded else [
        pltpu.VMEM((RING, PIECE, KV_HEADS, HEAD), bf16),
        pltpu.VMEM((RING, PIECE, KV_HEADS, HEAD), bf16),
        pltpu.VMEM((KV_HEADS, PIECE, HEAD), bf16),
        pltpu.VMEM((CHIPS - 1, chunk, HEAD), bf16),
        pltpu.VMEM((CHIPS - 1, chunk, HEAD), bf16),
        dma((2, RING)),
    ]
    return pl.pallas_call(
        functools.partial(layer_kernel, resharded),
        out_shape=[jax.ShapeDtypeStruct((tok, width), bf16),
                   jax.ShapeDtypeStruct((KV_HEADS, tok, HEAD), bf16),
                   jax.ShapeDtypeStruct((KV_HEADS, tok, HEAD), bf16)],
        in_specs=[vmem] * 2 + [hbm] * 7,
        out_specs=[vmem] * 3,
        scratch_shapes=[
            pltpu.VMEM((tok, width), bf16),
            pltpu.VMEM((tok, 2 * HEAD), f32),
            pltpu.VMEM((2,) + w_k.shape, bf16),
            pltpu.VMEM(w_o.shape, bf16),
            pltpu.VMEM((SLOTS, chunk, HEAD), bf16),
            pltpu.VMEM((SLOTS, chunk, HEAD), bf16),
            pltpu.VMEM((2, HEAD, 2 * chunk), bf16),
            pltpu.VMEM((KV_HEADS, GROUP + 2, tok, HEAD), bf16),
            pltpu.VMEM((CHIPS - 1, GROUP + 2, tok, HEAD), bf16),
            pltpu.VMEM((CHIPS, 2, tok, HEAD), bf16),
            pltpu.VMEM((2 * rows, HEAD), bf16),
            pltpu.VMEM((2 * rows, HEAD), bf16),
            pltpu.VMEM((GROUP, HEAD, rows), bf16),
            pltpu.VMEM((2 * chunk, rows), f32),
            pltpu.VMEM((2 * chunk, rows), f32),
            pltpu.VMEM((8, rows), f32),
            pltpu.VMEM((8, rows), f32),
            pltpu.VMEM((GROUP, HEAD, rows), f32),
            pltpu.VMEM((GROUP, 1, rows), f32),
            pltpu.VMEM((GROUP, 8, rows), f32),
            pltpu.VMEM((2 * rows, rows), f32),
            pltpu.VMEM((GROUP, CHIPS, tok, HEAD), bf16),
            pltpu.VMEM((tok, CHIPS * GROUP * HEAD), bf16),
            pltpu.VMEM((tok, width), f32),
            dma, dma((2 + CHIPS,)), dma, dma((2 * SLOTS,)),
            dma((CHIPS - 1, 2, 2)), dma((CHIPS - 1, 2, 2)), dma((CHIPS, 2, 2)), dma((CHIPS, 2, 2)),
            dma((CHIPS - 1,)), dma((CHIPS - 1,)), dma((CHIPS,)), dma((CHIPS,)),
            dma((GROUP, CHIPS - 1)), dma((GROUP, CHIPS - 1)),
        ] + packing,
        compiler_params=pltpu.CompilerParams(collective_id=collective_id, has_side_effects=True, vmem_limit_bytes=VMEM_ALL),
        name="layer",
    )(a, bias, trig, k_in, v_in, w_q, w_k, w_v, w_o)


def mlp_kernel(h_ref, kin_ref, vin_ref, gate_ref, up_ref, down_ref, g_ref, kout_ref, vout_ref,
               u, wg, wu, wd, acc, theirs, w_sem, u_send, u_recv, part_send, part_recv, kv_send, kv_recv, pair_send, pair_recv,
               raw_k, raw_v, tmp, k_out, v_out, raw_sem, own_sem):
    chip, core, across, partner = peers()
    tok = h_ref.shape[0]
    n_buf = wg.shape[0]
    steps = gate_ref.shape[1] // (2 * COL)

    def copies(i):
        slot = i % n_buf
        cols = pl.ds(pl.multiple_of((core * steps + i) * COL, COL), COL)
        return (pltpu.make_async_copy(gate_ref.at[:, cols], wg.at[slot], w_sem.at[slot, 0]),
                pltpu.make_async_copy(up_ref.at[:, cols], wu.at[slot], w_sem.at[slot, 1]),
                pltpu.make_async_copy(down_ref.at[cols, :], wd.at[slot], w_sem.at[slot, 2]))

    pack_start(kin_ref, raw_k, raw_sem.at[0])
    pack_start(vin_ref, raw_v, raw_sem.at[1])
    for b in range(n_buf):
        for c in copies(b):
            c.start()
    meet(across[1:] + [partner])
    u[:tok, :] = norm_rows(h_ref[...].astype(jnp.float32))
    u_copy = remote(u.at[pl.ds(0, tok)], u.at[pl.ds(tok, tok)], u_send, u_recv, partner)
    u_copy.start()

    def kv_copy(step, which):
        src, dst = (k_out, kout_ref) if which == 0 else (v_out, vout_ref)
        return remote(src.at[step], dst.at[2 * step], kv_send.at[step - 1, which], kv_recv.at[step - 1, which],
                      across[step])

    def pair_copy(step, which):
        dst = kout_ref if which == 0 else vout_ref
        src = (k_out if which == 0 else v_out).at[0] if step == 0 else dst.at[2 * step]
        return remote(src, dst.at[2 * step + 1], pair_send.at[step, which], pair_recv.at[step, which], partner)

    def put(out):
        def store(span):
            for step in range(CHIPS):
                out[step, span, :] = tmp[chip ^ step]
        return store

    acc[...] = jnp.zeros_like(acc)
    own = [pltpu.make_async_copy(k_out.at[0], kout_ref.at[0], own_sem.at[0]),
           pltpu.make_async_copy(v_out.at[0], vout_ref.at[0], own_sem.at[1])]
    for which, (src, raw, out) in enumerate(((kin_ref, raw_k, k_out), (vin_ref, raw_v, v_out))):
        pack_heads(src, raw, tmp, raw_sem.at[which], put(out))
        for step in range(1, CHIPS):
            kv_copy(step, which).start()
        pair_copy(0, which).start()
        own[which].start()
    u_copy.wait_recv()

    def relay(step):
        for which in range(2):
            kv_copy(step, which).wait_recv()
            pair_copy(step, which).start()

    def block(i, carry):
        slot = i % n_buf
        for c in copies(i):
            c.wait()
        gate = jnp.dot(u[...], wg[slot], preferred_element_type=jnp.float32).astype(jnp.bfloat16).astype(jnp.float32)
        up = jnp.dot(u[...], wu[slot], preferred_element_type=jnp.float32).astype(jnp.bfloat16).astype(jnp.float32)
        mixed = (gate * jax.nn.sigmoid(gate) * up).astype(jnp.bfloat16)
        acc[...] += jnp.dot(mixed, wd[slot], preferred_element_type=jnp.float32)

        @pl.when(i + n_buf < steps)
        def _():
            for c in copies(i + n_buf):
                c.start()

        @pl.when(i == steps - 12)
        def _():
            relay(1)
            relay(2)

        @pl.when(i == steps - 5)
        def _():
            relay(3)

        return carry

    lax.fori_loop(0, steps, block, 0)
    part_copy = remote(acc.at[pl.ds(tok, tok)], theirs, part_send, part_recv, partner)
    part_copy.start()
    part_copy.wait_recv()
    g_ref[...] = (h_ref[...].astype(jnp.float32) + (acc[:tok, :] + theirs[...])).astype(jnp.bfloat16)
    for step in range(CHIPS):
        for which in range(2):
            pair_copy(step, which).wait()
            if step:
                kv_copy(step, which).wait_send()
    for c in own:
        c.wait()
    u_copy.wait_send()
    part_copy.wait_send()


def run_mlp(h, cache_k, cache_v, w_gate, w_up, w_down, collective_id):
    tok, width = h.shape
    chunk = cache_k.shape[0]
    bf16, f32 = jnp.bfloat16, jnp.float32
    vmem = pl.BlockSpec(memory_space=pltpu.VMEM)
    hbm = pl.BlockSpec(memory_space=pl.ANY)
    dma = pltpu.SemaphoreType.DMA
    n_buf = 4
    slots = jax.ShapeDtypeStruct((SLOTS, chunk, HEAD), bf16)
    return pl.pallas_call(
        mlp_kernel,
        out_shape=[jax.ShapeDtypeStruct((tok, width), bf16), slots, slots],
        in_specs=[vmem] + [hbm] * 5,
        out_specs=[vmem, hbm, hbm],
        scratch_shapes=[
            pltpu.VMEM((2 * tok, width), bf16),
            pltpu.VMEM((n_buf, width, COL), bf16),
            pltpu.VMEM((n_buf, width, COL), bf16),
            pltpu.VMEM((n_buf, COL, width), bf16),
            pltpu.VMEM((2 * tok, width), f32),
            pltpu.VMEM((tok, width), f32),
            dma((n_buf, 3)), dma, dma, dma, dma,
            dma((CHIPS - 1, 2)), dma((CHIPS - 1, 2)), dma((CHIPS, 2)), dma((CHIPS, 2)),
            pltpu.VMEM((RING, PIECE, KV_HEADS, HEAD), bf16),
            pltpu.VMEM((RING, PIECE, KV_HEADS, HEAD), bf16),
            pltpu.VMEM((KV_HEADS, PIECE, HEAD), bf16),
            pltpu.VMEM((CHIPS, chunk, HEAD), bf16),
            pltpu.VMEM((CHIPS, chunk, HEAD), bf16),
            dma((2, RING)), dma((2,)),
        ],
        compiler_params=pltpu.CompilerParams(collective_id=collective_id, has_side_effects=True, vmem_limit_bytes=60 * MIB),
        name="mlp",
    )(h, cache_k, cache_v, w_gate, w_up, w_down)


def order_kernel(g_ref, y_ref, *refs):
    g_out, y_out = refs[4:6]
    g_out[...] = g_ref[...]
    y_out[...] = y_ref[...]
    for src, dst in zip(refs[:4], refs[6:]):
        for c in range(KV_HEADS):
            dst[:, c, :] = src[c]


def order_outputs(hidden, y_two, *appends):
    tok = hidden.shape[0]
    rows = [jax.ShapeDtypeStruct(t.shape, t.dtype) for t in (hidden, y_two)]
    lines = [jax.ShapeDtypeStruct((tok, KV_HEADS, HEAD), t.dtype) for t in appends]
    vmem = pl.BlockSpec(memory_space=pltpu.VMEM)
    return pl.pallas_call(order_kernel, out_shape=rows + lines, in_specs=[vmem] * 6, out_specs=[vmem] * 6,
                          name="order_outputs")(hidden, y_two, *appends)


def solution(mesh):
    axis_size = mesh.shape['cp']
    rows_spec = P(('dp', 'cp'), None)
    cache_spec = P(('dp', 'cp'), None, None)
    mat_spec = P(None, None)
    vec_spec = P(None)
    layer_specs = (cache_spec, cache_spec, mat_spec, vec_spec, mat_spec, vec_spec, mat_spec, mat_spec)
    in_specs = (rows_spec,) + layer_specs + (mat_spec, mat_spec, mat_spec) + layer_specs
    out_specs = (rows_spec, rows_spec, cache_spec, cache_spec, cache_spec, cache_spec)

    def forward(x_in, cache_k1, cache_v1, w_q1, b_q1, w_k1, b_k1, w_v1, w_o1, w_gate, w_up, w_down, cache_k2, cache_v2, w_q2, b_q2, w_k2, b_k2, w_v2, w_o2):
        n_tok = axis_size * x_in.shape[0]
        trig = rope_table(axis_size * cache_k1.shape[0], n_tok)
        bias = jnp.concatenate([b_q1, b_k1, b_q2, b_k2]).reshape(1, -1)
        resid_h, k_one, v_one = run_layer(False, x_in, bias, trig, cache_k1, cache_v1, w_q1, w_k1, w_v1, w_o1, 1)
        hidden, k_in, v_in = run_mlp(resid_h, cache_k2, cache_v2, w_gate, w_up, w_down, 2)
        y_two, k_two, v_two = run_layer(True, hidden, bias, trig, k_in, v_in, w_q2, w_k2, w_v2, w_o2, 3)
        return order_outputs(hidden, y_two, k_one, v_one, k_two, v_two)

    return jax.shard_map(forward, mesh=mesh, in_specs=in_specs, out_specs=out_specs, check_vma=False)
```

```python
import functools

import jax
import jax.numpy as jnp
import numpy as np
from jax import lax
from jax.experimental import pallas as pl
from jax.experimental.pallas import tpu as pltpu
from jax.sharding import PartitionSpec as P

ROPE_THETA = 500000.0
NORM_EPS = 1e-5
LOG2E = 1.4426950408889634
KV_HEADS = 4
HEAD = 128
GROUP = 7
CHIPS = 4
COL = 256
SLOTS = 2 * CHIPS
MIB = 1024 * 1024
VMEM_ALL = 67_000_000
PIECE = 256
RING = 4
MESH = pl.DeviceIdType.MESH


@functools.lru_cache(maxsize=None)
def rope_table(first, count):
    with jax.ensure_compile_time_eval():
        half_dim = HEAD // 2
        inv_freq = 1.0 / (ROPE_THETA ** (jnp.arange(half_dim, dtype=jnp.float32) * (2.0 / HEAD)))
        angles = (first + jnp.arange(count)).astype(jnp.float32)[:, None] * inv_freq[None, :]
        cos_t, sin_t = jnp.cos(angles), jnp.sin(angles)
        return np.asarray(jnp.concatenate([cos_t, cos_t, -sin_t, sin_t], axis=-1))


def norm_rows(wide):
    return (wide * lax.rsqrt(jnp.mean(wide * wide, axis=-1, keepdims=True) + NORM_EPS)).astype(jnp.bfloat16)


def peers():
    me = lax.axis_index('cp')
    chip, core = me // 2, me % 2
    across = [2 * (chip ^ step) + core for step in range(CHIPS)]
    return chip, core, across, 2 * chip + (1 - core)


def meet(others):
    barrier = pltpu.get_barrier_semaphore()
    for dev in others:
        pl.semaphore_signal(barrier, inc=1, device_id={'cp': dev}, device_id_type=MESH)
    pl.semaphore_wait(barrier, len(others))


def remote(src, dst, send_sem, recv_sem, dev):
    return pltpu.make_async_remote_copy(src_ref=src, dst_ref=dst, send_sem=send_sem, recv_sem=recv_sem,
                                        device_id={'cp': dev}, device_id_type=MESH)


def pack_start(src_ref, raw, sem):
    for i in range(RING):
        pltpu.make_async_copy(src_ref.at[pl.ds(i * PIECE, PIECE)], raw.at[i], sem.at[i]).start()


def pack_heads(src_ref, dst_ref, raw, tmp, sem, out_sem):
    n = src_ref.shape[0] // PIECE

    def put(i, slot):
        span = pl.ds(pl.multiple_of(i * PIECE, PIECE), PIECE)
        return pltpu.make_async_copy(tmp.at[slot], dst_ref.at[:, span], out_sem.at[slot])

    def piece(i, carry):
        slot = i % RING
        side = i % 2
        pltpu.make_async_copy(raw.at[slot], raw.at[slot], sem.at[slot]).wait()

        @pl.when(i >= 2)
        def _():
            put(i - 2, side).wait()

        for part in range(2):
            half = PIECE // 2
            flat = jnp.swapaxes(raw[slot, part * half:(part + 1) * half], 0, 1)
            for c in range(KV_HEADS):
                tmp[side, c, part * half:(part + 1) * half, :] = flat[c]

        @pl.when(i + RING < n)
        def _():
            pltpu.make_async_copy(src_ref.at[pl.ds((i + RING) * PIECE, PIECE)], raw.at[slot], sem.at[slot]).start()

        put(i, side).start()
        return carry

    lax.fori_loop(0, n, piece, 0)
    put(n - 2, 0).wait()
    put(n - 1, 1).wait()


def layer_kernel(resharded, a_ref, bias_ref, trig_ref, k4_ref, v4_ref, *refs):
    if resharded:
        kin_ref, vin_ref, wq_ref, wk_ref, wv_ref, wo_ref = refs[:6]
        refs = refs[6:]
    else:
        knext_ref, vnext_ref, wq_ref, wk_ref, wv_ref, wo_ref = refs[:6]
        refs = refs[6:]
        kpack_ref, vpack_ref = refs[3:5]
        raw, tmp, raw_sem, out_sem = refs[-4:]
        refs = refs[:3] + refs[5:-4]
    (y_ref, knew_ref, vnew_ref, xn, trig, wkv, wo, kb, vb, vt, msg, got, peer_new, newk, newv, qt,
     s_even, s_odd, m_even, m_odd, acc, m_run, l_run, hide, o_send, o_all, y_acc,
     trig_sem, w_sem, wo_sem, loc_sem, kv_send, kv_recv, pair_send, pair_recv, q_send, q_recv,
     new_send, new_recv, o_ssem, o_rsem) = refs
    chip, core, across, partner = peers()
    me = 2 * chip + core
    scale2 = HEAD ** -0.5 * LOG2E
    tok = a_ref.shape[0]
    chunk = kb.shape[1]
    rows = qt.shape[2]
    wide_cols = GROUP * HEAD
    n_q = wq_ref.shape[1]
    n_items = CHIPS * GROUP
    n_first = (CHIPS - 1) * GROUP
    bias_at = (n_q + wk_ref.shape[1]) if resharded else 0

    def wq_copy(n):
        cols = pl.ds(pl.multiple_of((chip ^ (CHIPS - 1 - n)) * wide_cols, HEAD), wide_cols)
        return pltpu.make_async_copy(wq_ref.at[:, cols], wo.at[:, n * wide_cols:(n + 1) * wide_cols], w_sem.at[2 + n])

    kv_loads = [pltpu.make_async_copy(wk_ref, wkv.at[0], w_sem.at[0]), pltpu.make_async_copy(wv_ref, wkv.at[1], w_sem.at[1])]
    trig_load = pltpu.make_async_copy(trig_ref.at[pl.ds(me * tok, tok)], trig, trig_sem)
    trig_load.start()
    for c in kv_loads + [wq_copy(n) for n in range(CHIPS)]:
        c.start()
    meet(across[1:] + [partner])

    own = [pltpu.make_async_copy(k4_ref.at[chip], kb.at[0], loc_sem.at[0]),
           pltpu.make_async_copy(v4_ref.at[chip], vb.at[0], loc_sem.at[1])]
    for c in own:
        c.start()

    def kv_copy(step, which):
        src, dst = (k4_ref, kb) if which == 0 else (v4_ref, vb)
        return remote(src.at[chip ^ step], dst.at[2 * step], kv_send.at[step - 1, which], kv_recv.at[step - 1, which],
                      across[step])

    def pair_copy(step, which):
        dst = kb if which == 0 else vb
        if step == 0:
            src = (k4_ref if which == 0 else v4_ref).at[chip]
        else:
            src = dst.at[2 * step]
        return remote(src, dst.at[2 * step + 1], pair_send.at[step, which], pair_recv.at[step, which], partner)

    if resharded:
        loads = []
        for j in range(1, SLOTS):
            loads.append((pltpu.make_async_copy(kin_ref.at[j], kb.at[j], loc_sem.at[2 * j]),
                          pltpu.make_async_copy(vin_ref.at[j], vb.at[j], loc_sem.at[2 * j + 1])))
        for pair in loads:
            for c in pair:
                c.start()
    else:
        for which in range(2):
            pair_copy(0, which).start()
        kv_copy(1, 0).start()
        kv_copy(2, 0).start()

    if resharded:
        xn[...] = norm_rows(a_ref[...].astype(jnp.float32))
    else:
        xn[...] = a_ref[...]

    trig_load.wait()

    def rope(plain):
        wide = plain.astype(jnp.float32)
        return (wide * trig[:, :HEAD] + pltpu.roll(wide, HEAD // 2, 1) * trig[:, HEAD:]).astype(jnp.bfloat16)

    kv_loads[0].wait()
    k_pre = (jnp.dot(xn[...], wkv[0], preferred_element_type=jnp.float32)
             + bias_ref[:, bias_at + n_q:bias_at + n_q + KV_HEADS * HEAD].astype(jnp.float32)).astype(jnp.bfloat16)
    for c in range(KV_HEADS):
        knew_ref[c] = rope(k_pre[:, c * HEAD:(c + 1) * HEAD])
    kv_loads[1].wait()
    v_pre = jnp.dot(xn[...], wkv[1], preferred_element_type=jnp.float32).astype(jnp.bfloat16)
    for c in range(KV_HEADS):
        vnew_ref[c] = v_pre[:, c * HEAD:(c + 1) * HEAD]

    def q_copy(n):
        return remote(msg.at[n], got.at[n], q_send.at[n], q_recv.at[n], 2 * (chip ^ (CHIPS - 1 - n)) + core)

    def project(n, carry):
        pltpu.make_async_copy(wo.at[:, :wide_cols], wo.at[:, :wide_cols], w_sem.at[2 + n]).wait()
        grp = chip ^ (CHIPS - 1 - n)
        cols = pl.ds(pl.multiple_of(n * wide_cols, HEAD), wide_cols)
        bias = bias_ref[:, pl.ds(pl.multiple_of(bias_at + grp * wide_cols, HEAD), wide_cols)].astype(jnp.float32)
        q_pre = (jnp.dot(xn[...], wo[:, cols], preferred_element_type=jnp.float32) + bias).astype(jnp.bfloat16)
        for g in range(GROUP):
            msg[n, g] = rope(q_pre[:, g * HEAD:(g + 1) * HEAD])
        msg[n, GROUP] = knew_ref[grp]
        msg[n, GROUP + 1] = vnew_ref[grp]

        @pl.when(n < CHIPS - 1)
        def _():
            q_copy(n).start()

        return carry

    lax.fori_loop(0, CHIPS, project, 0)
    q_copies = [q_copy(n) for n in range(CHIPS - 1)]
    parts = [msg.at[CHIPS - 1]] + [got.at[CHIPS - 1 - s] for s in range(1, CHIPS)]
    wo_load = pltpu.make_async_copy(wo_ref, wo, wo_sem)
    if not resharded:
        for step, which in ((1, 1), (2, 1), (3, 0), (3, 1)):
            kv_copy(step, which).start()
    wo_load.start()
    acc[...] = jnp.zeros_like(acc)
    m_run[...] = jnp.full_like(m_run, -jnp.inf)
    l_run[...] = jnp.zeros_like(l_run)
    for c in q_copies:
        c.wait_recv()
    new_copies = [remote(parts[s].at[pl.ds(GROUP, 2)], peer_new.at[s], new_send.at[s], new_recv.at[s], partner) for s in range(CHIPS)]
    for c in new_copies:
        c.start()
    for g in range(GROUP):
        qt[g] = jnp.concatenate([p[g] for p in parts], axis=0).T
    for s in range(CHIPS):
        newk[s * tok:(s + 1) * tok, :] = parts[s][GROUP]
        newv[s * tok:(s + 1) * tok, :] = parts[s][GROUP + 1]

    def relay(step):
        for which in range(2):
            kv_copy(step, which).wait_recv()
            pair_copy(step, which).start()

    def ready(j):
        for jj in range(CHIPS):
            @pl.when(j == jj)
            def _():
                if jj == 0:
                    for c in own:
                        c.wait()
                elif resharded:
                    for c in loads[2 * jj - 1]:
                        c.wait()
                elif jj != 2:
                    relay(jj)
        vt[j % 2, :, :chunk] = vb[2 * j].T
        for jj in range(CHIPS):
            @pl.when(j == jj)
            def _():
                if resharded:
                    for c in loads[2 * jj]:
                        c.wait()
                else:
                    for which in range(2):
                        pair_copy(jj, which).wait_recv()
        vt[j % 2, :, chunk:] = vb[2 * j + 1].T

    def place(item):
        return item // GROUP, item % GROUP

    def score(item, s_dst, m_dst):
        j, g = place(item)
        part = jnp.full((8, rows), -jnp.inf, jnp.float32)
        for t in range(2 * chunk // 256):
            at = (t * 256) % chunk
            s_blk = jnp.dot(kb[2 * j + t * 256 // chunk, at:at + 256, :], qt[g], preferred_element_type=jnp.float32)
            s_dst[t * 256:(t + 1) * 256, :] = s_blk
            part = jnp.maximum(part, jnp.max(s_blk.reshape(32, 8, rows), axis=0))
        m_dst[...] = part

    def absorb(item, s_src, m_src):
        j, g = place(item)
        m_old = m_run[g]
        m_new = jnp.maximum(m_old, jnp.max(m_src[...], axis=0, keepdims=True))
        alpha = jnp.exp2((m_old - m_new) * scale2)
        shift = m_new * scale2
        l_part = jnp.zeros((8, rows), jnp.float32)
        out = jnp.zeros((HEAD, rows), jnp.float32)
        for t in range(2 * chunk // 256):
            p = jnp.exp2(s_src[t * 256:(t + 1) * 256, :] * scale2 - shift)
            l_part = l_part + jnp.sum(p.reshape(32, 8, rows), axis=0)
            out = out + jnp.dot(vt[j % 2, :, t * 256:(t + 1) * 256], p.astype(jnp.bfloat16),
                                preferred_element_type=jnp.float32)
        acc[g] = acc[g] * alpha + out
        l_run[g] = l_run[g] * alpha + l_part
        m_run[g] = m_new

    ready(0)
    score(0, s_even, m_even)

    new_len = newk.shape[0]

    key_i = lax.broadcasted_iota(jnp.int32, (new_len, rows), 0)
    qry_i = lax.broadcasted_iota(jnp.int32, (new_len, rows), 1)
    blk = key_i // tok
    k_pos = (2 * (chip ^ (blk % CHIPS)) + (core ^ (blk // CHIPS))) * tok + key_i % tok
    q_pos = (2 * (chip ^ (qry_i // tok)) + core) * tok + qry_i % tok
    hide[...] = jnp.where(k_pos <= q_pos, 0.0, -jnp.inf)

    def o_copy(g, s):
        src = o_send.at[g, s]
        dst = o_all.at[:, pl.ds(pl.multiple_of(chip * wide_cols + g * HEAD, HEAD), HEAD)]
        return remote(src, dst, o_ssem.at[g, s - 1], o_rsem.at[g, s - 1], across[s])

    def finish(g):
        s = jnp.dot(newk[...], qt[g], preferred_element_type=jnp.float32) + hide[...]
        m_old = m_run[g]
        m_new = jnp.maximum(m_old, jnp.max(s, axis=0, keepdims=True))
        alpha = jnp.exp2((m_old - m_new) * scale2)
        p = jnp.exp2(s * scale2 - m_new * scale2)
        total = jnp.sum(l_run[g] * alpha, axis=0, keepdims=True) + jnp.sum(p, axis=0, keepdims=True)
        fresh = lax.dot_general(newv[...], p.astype(jnp.bfloat16), (((0,), (0,)), ((), ())),
                                preferred_element_type=jnp.float32)
        out = ((acc[g] * alpha + fresh) / total).T.astype(jnp.bfloat16)
        for s_i in range(1, CHIPS):
            o_send[g, s_i] = out[s_i * tok:(s_i + 1) * tok, :]
            o_copy(g, s_i).start()
        o_all[:, pl.ds(pl.multiple_of(chip * wide_cols + g * HEAD, HEAD), HEAD)] = out[:tok, :]

    def step(item, carry):
        nxt = item + 1

        if not resharded:
            @pl.when(nxt == GROUP)
            def _():
                for src, dst in ((knext_ref, kpack_ref), (vnext_ref, vpack_ref)):
                    pack_start(src, raw, raw_sem)
                    pack_heads(src, dst, raw, tmp, raw_sem, out_sem)

            @pl.when(nxt == GROUP + 4)
            def _():
                relay(2)

        @pl.when((nxt % GROUP == 0) & (nxt < n_items))
        def _():
            ready(nxt // GROUP)

        @pl.when(item == n_first)
        def _():
            for c in new_copies:
                c.wait_recv()
            for s in range(CHIPS):
                at = (CHIPS + s) * tok
                newk[at:at + tok, :] = peer_new[s, 0]
                newv[at:at + tok, :] = peer_new[s, 1]

        after = jnp.minimum(nxt, n_items - 1)

        @pl.when(item % 2 == 0)
        def _():
            score(after, s_odd, m_odd)
            absorb(item, s_even, m_even)

        @pl.when(item % 2 == 1)
        def _():
            score(after, s_even, m_even)
            absorb(item, s_odd, m_odd)

        @pl.when(item >= n_first)
        def _():
            finish(item - n_first)

        return carry

    lax.fori_loop(0, n_items, step, 0)
    o_copies = [o_copy(g, s) for g in range(GROUP) for s in range(1, CHIPS)]
    last = 3 * (GROUP - 1)
    wo_load.wait()
    for c in o_copies[:last]:
        c.wait_recv()

    def heads(s, first, count):
        at = pl.multiple_of((chip ^ s) * wide_cols + first * HEAD, HEAD)
        return pl.ds(at, count * HEAD)

    def early_proj(blk, carry):
        cols = pl.ds(pl.multiple_of(blk * COL, COL), COL)
        total = jnp.zeros((tok, COL), jnp.float32)
        for s in range(CHIPS):
            part = heads(s, 0, GROUP if s == 0 else GROUP - 1)
            total = total + jnp.dot(o_all[:, part], wo[part, cols], preferred_element_type=jnp.float32)
        y_acc[:, cols] = total
        return carry

    lax.fori_loop(0, wo.shape[1] // COL, early_proj, 0)
    for c in o_copies[last:]:
        c.wait_recv()

    def out_proj(blk, carry):
        cols = pl.ds(pl.multiple_of(blk * 2 * COL, 2 * COL), 2 * COL)
        total = y_acc[:, cols]
        for s in range(1, CHIPS):
            part = heads(s, GROUP - 1, 1)
            total = total + jnp.dot(o_all[:, part], wo[part, cols], preferred_element_type=jnp.float32)
        y = total.astype(jnp.bfloat16)
        if not resharded:
            y = (a_ref[:, cols].astype(jnp.float32) + y.astype(jnp.float32)).astype(jnp.bfloat16)
        y_ref[:, cols] = y
        return carry

    lax.fori_loop(0, wo.shape[1] // (2 * COL), out_proj, 0)

    for c in q_copies + new_copies + o_copies:
        c.wait_send()
    if not resharded:
        for step in range(CHIPS):
            for which in range(2):
                pair_copy(step, which).wait_send()
                if step:
                    kv_copy(step, which).wait_send()


def run_layer(resharded, a, bias, trig, k4, v4, k_in, v_in, w_q, w_k, w_v, w_o, collective_id):
    tok, width = a.shape
    chunk = k4.shape[1]
    rows = CHIPS * tok
    bf16, f32 = jnp.bfloat16, jnp.float32
    vmem = pl.BlockSpec(memory_space=pltpu.VMEM)
    hbm = pl.BlockSpec(memory_space=pl.ANY)
    dma = pltpu.SemaphoreType.DMA
    packed = [] if resharded else [jax.ShapeDtypeStruct(k4.shape, bf16)] * 2
    packing = [] if resharded else [
        pltpu.VMEM((RING, PIECE, KV_HEADS, HEAD), bf16),
        pltpu.VMEM((2, KV_HEADS, PIECE, HEAD), bf16),
        dma((RING,)), dma((2,)),
    ]
    return pl.pallas_call(
        functools.partial(layer_kernel, resharded),
        out_shape=[jax.ShapeDtypeStruct((tok, width), bf16),
                   jax.ShapeDtypeStruct((KV_HEADS, tok, HEAD), bf16),
                   jax.ShapeDtypeStruct((KV_HEADS, tok, HEAD), bf16)] + packed,
        in_specs=[vmem] * 2 + [hbm] * 9,
        out_specs=[vmem] * 3 + [hbm] * len(packed),
        scratch_shapes=[
            pltpu.VMEM((tok, width), bf16),
            pltpu.VMEM((tok, 2 * HEAD), f32),
            pltpu.VMEM((2,) + w_k.shape, bf16),
            pltpu.VMEM(w_o.shape, bf16),
            pltpu.VMEM((SLOTS, chunk, HEAD), bf16),
            pltpu.VMEM((SLOTS, chunk, HEAD), bf16),
            pltpu.VMEM((2, HEAD, 2 * chunk), bf16),
            pltpu.VMEM((KV_HEADS, GROUP + 2, tok, HEAD), bf16),
            pltpu.VMEM((CHIPS - 1, GROUP + 2, tok, HEAD), bf16),
            pltpu.VMEM((CHIPS, 2, tok, HEAD), bf16),
            pltpu.VMEM((2 * rows, HEAD), bf16),
            pltpu.VMEM((2 * rows, HEAD), bf16),
            pltpu.VMEM((GROUP, HEAD, rows), bf16),
            pltpu.VMEM((2 * chunk, rows), f32),
            pltpu.VMEM((2 * chunk, rows), f32),
            pltpu.VMEM((8, rows), f32),
            pltpu.VMEM((8, rows), f32),
            pltpu.VMEM((GROUP, HEAD, rows), f32),
            pltpu.VMEM((GROUP, 1, rows), f32),
            pltpu.VMEM((GROUP, 8, rows), f32),
            pltpu.VMEM((2 * rows, rows), f32),
            pltpu.VMEM((GROUP, CHIPS, tok, HEAD), bf16),
            pltpu.VMEM((tok, CHIPS * GROUP * HEAD), bf16),
            pltpu.VMEM((tok, width), f32),
            dma, dma((2 + CHIPS,)), dma, dma((2 * SLOTS,)),
            dma((CHIPS - 1, 2)), dma((CHIPS - 1, 2)), dma((CHIPS, 2)), dma((CHIPS, 2)),
            dma((CHIPS - 1,)), dma((CHIPS - 1,)), dma((CHIPS,)), dma((CHIPS,)),
            dma((GROUP, CHIPS - 1)), dma((GROUP, CHIPS - 1)),
        ] + packing,
        compiler_params=pltpu.CompilerParams(collective_id=collective_id, has_side_effects=True, vmem_limit_bytes=VMEM_ALL),
        name="layer",
    )(a, bias, trig, k4, v4, k_in, v_in, w_q, w_k, w_v, w_o)


def mlp_kernel(h_ref, k4_ref, v4_ref, gate_ref, up_ref, down_ref, g_ref, kout_ref, vout_ref,
               u, wg, wu, wd, acc, theirs, w_sem, u_send, u_recv, part_send, part_recv, kv_send, kv_recv, pair_send, pair_recv):
    chip, core, across, partner = peers()
    tok = h_ref.shape[0]
    n_buf = wg.shape[0]
    steps = gate_ref.shape[1] // (2 * COL)

    def copies(i):
        slot = i % n_buf
        cols = pl.ds(pl.multiple_of((core * steps + i) * COL, COL), COL)
        return (pltpu.make_async_copy(gate_ref.at[:, cols], wg.at[slot], w_sem.at[slot, 0]),
                pltpu.make_async_copy(up_ref.at[:, cols], wu.at[slot], w_sem.at[slot, 1]),
                pltpu.make_async_copy(down_ref.at[cols, :], wd.at[slot], w_sem.at[slot, 2]))

    for b in range(n_buf):
        for c in copies(b):
            c.start()
    meet(across[1:] + [partner])
    u[:tok, :] = norm_rows(h_ref[...].astype(jnp.float32))
    u_copy = remote(u.at[pl.ds(0, tok)], u.at[pl.ds(tok, tok)], u_send, u_recv, partner)
    u_copy.start()

    def kv_copy(step, which):
        src, dst = (k4_ref, kout_ref) if which == 0 else (v4_ref, vout_ref)
        return remote(src.at[chip ^ step], dst.at[2 * step], kv_send.at[step - 1, which], kv_recv.at[step - 1, which],
                      across[step])

    def pair_copy(step, which):
        dst = kout_ref if which == 0 else vout_ref
        src = (k4_ref if which == 0 else v4_ref).at[chip] if step == 0 else dst.at[2 * step]
        return remote(src, dst.at[2 * step + 1], pair_send.at[step, which], pair_recv.at[step, which], partner)

    for step in range(1, CHIPS):
        for which in range(2):
            kv_copy(step, which).start()
    for which in range(2):
        pair_copy(0, which).start()
    acc[...] = jnp.zeros_like(acc)
    u_copy.wait_recv()

    def relay(step):
        for which in range(2):
            kv_copy(step, which).wait_recv()
            pair_copy(step, which).start()

    def block(i, carry):
        slot = i % n_buf
        for c in copies(i):
            c.wait()
        gate = jnp.dot(u[...], wg[slot], preferred_element_type=jnp.float32).astype(jnp.bfloat16).astype(jnp.float32)
        up = jnp.dot(u[...], wu[slot], preferred_element_type=jnp.float32).astype(jnp.bfloat16).astype(jnp.float32)
        mixed = (gate * jax.nn.sigmoid(gate) * up).astype(jnp.bfloat16)
        acc[...] += jnp.dot(mixed, wd[slot], preferred_element_type=jnp.float32)

        @pl.when(i + n_buf < steps)
        def _():
            for c in copies(i + n_buf):
                c.start()

        @pl.when(i == steps - 12)
        def _():
            relay(1)
            relay(2)

        @pl.when(i == steps - 5)
        def _():
            relay(3)

        return carry

    lax.fori_loop(0, steps, block, 0)
    part_copy = remote(acc.at[pl.ds(tok, tok)], theirs, part_send, part_recv, partner)
    part_copy.start()
    part_copy.wait_recv()
    g_ref[...] = (h_ref[...].astype(jnp.float32) + (acc[:tok, :] + theirs[...])).astype(jnp.bfloat16)
    for step in range(CHIPS):
        for which in range(2):
            pair_copy(step, which).wait()
            if step:
                kv_copy(step, which).wait_send()
    u_copy.wait_send()
    part_copy.wait_send()


def run_mlp(h, k4, v4, w_gate, w_up, w_down, collective_id):
    tok, width = h.shape
    chunk = k4.shape[1]
    bf16, f32 = jnp.bfloat16, jnp.float32
    vmem = pl.BlockSpec(memory_space=pltpu.VMEM)
    hbm = pl.BlockSpec(memory_space=pl.ANY)
    dma = pltpu.SemaphoreType.DMA
    n_buf = 4
    slots = jax.ShapeDtypeStruct((SLOTS, chunk, HEAD), bf16)
    return pl.pallas_call(
        mlp_kernel,
        out_shape=[jax.ShapeDtypeStruct((tok, width), bf16), slots, slots],
        in_specs=[vmem] + [hbm] * 5,
        out_specs=[vmem, hbm, hbm],
        scratch_shapes=[
            pltpu.VMEM((2 * tok, width), bf16),
            pltpu.VMEM((n_buf, width, COL), bf16),
            pltpu.VMEM((n_buf, width, COL), bf16),
            pltpu.VMEM((n_buf, COL, width), bf16),
            pltpu.VMEM((2 * tok, width), f32),
            pltpu.VMEM((tok, width), f32),
            dma((n_buf, 3)), dma, dma, dma, dma,
            dma((CHIPS - 1, 2)), dma((CHIPS - 1, 2)), dma((CHIPS, 2)), dma((CHIPS, 2)),
        ],
        compiler_params=pltpu.CompilerParams(collective_id=collective_id, has_side_effects=True, vmem_limit_bytes=60 * MIB),
        name="mlp",
    )(h, k4, v4, w_gate, w_up, w_down)


def heads_first(cache):
    return lax.optimization_barrier(jnp.transpose(cache, (1, 0, 2)))


def order_kernel(g_ref, y_ref, *refs):
    g_out, y_out = refs[4:6]
    g_out[...] = g_ref[...]
    y_out[...] = y_ref[...]
    for src, dst in zip(refs[:4], refs[6:]):
        for c in range(KV_HEADS):
            dst[:, c, :] = src[c]


def order_outputs(hidden, y_two, *appends):
    tok = hidden.shape[0]
    rows = [jax.ShapeDtypeStruct(t.shape, t.dtype) for t in (hidden, y_two)]
    lines = [jax.ShapeDtypeStruct((tok, KV_HEADS, HEAD), t.dtype) for t in appends]
    vmem = pl.BlockSpec(memory_space=pltpu.VMEM)
    return pl.pallas_call(order_kernel, out_shape=rows + lines, in_specs=[vmem] * 6, out_specs=[vmem] * 6,
                          name="order_outputs")(hidden, y_two, *appends)


def solution(mesh):
    axis_size = mesh.shape['cp']
    rows_spec = P(('dp', 'cp'), None)
    cache_spec = P(('dp', 'cp'), None, None)
    mat_spec = P(None, None)
    vec_spec = P(None)
    layer_specs = (cache_spec, cache_spec, mat_spec, vec_spec, mat_spec, vec_spec, mat_spec, mat_spec)
    in_specs = (rows_spec,) + layer_specs + (mat_spec, mat_spec, mat_spec) + layer_specs
    out_specs = (rows_spec, rows_spec, cache_spec, cache_spec, cache_spec, cache_spec)

    def forward(x_in, cache_k1, cache_v1, w_q1, b_q1, w_k1, b_k1, w_v1, w_o1, w_gate, w_up, w_down, cache_k2, cache_v2, w_q2, b_q2, w_k2, b_k2, w_v2, w_o2):
        n_tok = axis_size * x_in.shape[0]
        trig = rope_table(axis_size * cache_k1.shape[0], n_tok)
        bias = jnp.concatenate([b_q1, b_k1, b_q2, b_k2]).reshape(1, -1)
        k4a, v4a = heads_first(cache_k1), heads_first(cache_v1)
        resid_h, k_one, v_one, k4b, v4b = run_layer(False, x_in, bias, trig, k4a, v4a, cache_k2, cache_v2, w_q1, w_k1, w_v1, w_o1, 1)
        hidden, k_in, v_in = run_mlp(resid_h, k4b, v4b, w_gate, w_up, w_down, 2)
        y_two, k_two, v_two = run_layer(True, hidden, bias, trig, k4b, v4b, k_in, v_in, w_q2, w_k2, w_v2, w_o2, 3)
        return order_outputs(hidden, y_two, k_one, v_one, k_two, v_two)

    return jax.shard_map(forward, mesh=mesh, in_specs=in_specs, out_specs=out_specs, check_vma=False)
```

```python
import functools

import jax
import jax.numpy as jnp
import numpy as np
from jax import lax
from jax.experimental import pallas as pl
from jax.experimental.pallas import tpu as pltpu
from jax.sharding import PartitionSpec as P

ROPE_THETA = 500000.0
NORM_EPS = 1e-5
LOG2E = 1.4426950408889634
KV_HEADS = 4
HEAD = 128
GROUP = 7
CHIPS = 4
COL = 256
SLOTS = 2 * CHIPS
MIB = 1024 * 1024
VMEM_ALL = 67_000_000
PIECE = 256
RING = 4
MESH = pl.DeviceIdType.MESH


@functools.lru_cache(maxsize=None)
def rope_table(first, count):
    with jax.ensure_compile_time_eval():
        half_dim = HEAD // 2
        inv_freq = 1.0 / (ROPE_THETA ** (jnp.arange(half_dim, dtype=jnp.float32) * (2.0 / HEAD)))
        angles = (first + jnp.arange(count)).astype(jnp.float32)[:, None] * inv_freq[None, :]
        cos_t, sin_t = jnp.cos(angles), jnp.sin(angles)
        return np.asarray(jnp.concatenate([cos_t, cos_t, -sin_t, sin_t], axis=-1))


def norm_rows(wide):
    return (wide * lax.rsqrt(jnp.mean(wide * wide, axis=-1, keepdims=True) + NORM_EPS)).astype(jnp.bfloat16)


def peers():
    me = lax.axis_index('cp')
    chip, core = me // 2, me % 2
    across = [2 * (chip ^ step) + core for step in range(CHIPS)]
    return chip, core, across, 2 * chip + (1 - core)


def meet(others):
    barrier = pltpu.get_barrier_semaphore()
    for dev in others:
        pl.semaphore_signal(barrier, inc=1, device_id={'cp': dev}, device_id_type=MESH)
    pl.semaphore_wait(barrier, len(others))


def remote(src, dst, send_sem, recv_sem, dev):
    return pltpu.make_async_remote_copy(src_ref=src, dst_ref=dst, send_sem=send_sem, recv_sem=recv_sem,
                                        device_id={'cp': dev}, device_id_type=MESH)


def pack_start(src_ref, raw, sem):
    for i in range(RING):
        pltpu.make_async_copy(src_ref.at[pl.ds(i * PIECE, PIECE)], raw.at[i], sem.at[i]).start()


def pack_heads(src_ref, dst_ref, raw, tmp, sem, out_sem):
    n = src_ref.shape[0] // PIECE

    def put(i, slot):
        span = pl.ds(pl.multiple_of(i * PIECE, PIECE), PIECE)
        return pltpu.make_async_copy(tmp.at[slot], dst_ref.at[:, span], out_sem.at[slot])

    def piece(i, carry):
        slot = i % RING
        side = i % 2
        pltpu.make_async_copy(raw.at[slot], raw.at[slot], sem.at[slot]).wait()

        @pl.when(i >= 2)
        def _():
            put(i - 2, side).wait()

        for part in range(2):
            half = PIECE // 2
            flat = jnp.swapaxes(raw[slot, part * half:(part + 1) * half], 0, 1)
            for c in range(KV_HEADS):
                tmp[side, c, part * half:(part + 1) * half, :] = flat[c]

        @pl.when(i + RING < n)
        def _():
            pltpu.make_async_copy(src_ref.at[pl.ds((i + RING) * PIECE, PIECE)], raw.at[slot], sem.at[slot]).start()

        put(i, side).start()
        return carry

    lax.fori_loop(0, n, piece, 0)
    put(n - 2, 0).wait()
    put(n - 1, 1).wait()


def layer_kernel(resharded, a_ref, bias_ref, trig_ref, k4_ref, v4_ref, *refs):
    if resharded:
        kin_ref, vin_ref, wq_ref, wk_ref, wv_ref, wo_ref = refs[:6]
        refs = refs[6:]
    else:
        knext_ref, vnext_ref, wq_ref, wk_ref, wv_ref, wo_ref = refs[:6]
        refs = refs[6:]
        kpack_ref, vpack_ref = refs[3:5]
        raw, tmp, raw_sem, out_sem = refs[-4:]
        refs = refs[:3] + refs[5:-4]
    (y_ref, knew_ref, vnew_ref, xn, trig, wkv, wo, kb, vb, vt, msg, got, peer_new, newk, newv, qt,
     s_even, s_odd, m_even, m_odd, acc, m_run, l_run, hide, o_send, o_all, y_acc,
     trig_sem, w_sem, wo_sem, loc_sem, kv_send, kv_recv, pair_send, pair_recv, q_send, q_recv,
     new_send, new_recv, o_ssem, o_rsem, kvm_send, kvm_recv) = refs
    chip, core, across, partner = peers()
    me = 2 * chip + core
    scale2 = HEAD ** -0.5 * LOG2E
    tok = a_ref.shape[0]
    chunk = kb.shape[1]
    rows = qt.shape[2]
    wide_cols = GROUP * HEAD
    n_q = wq_ref.shape[1]
    n_items = CHIPS * GROUP
    n_first = (CHIPS - 1) * GROUP
    bias_at = (n_q + wk_ref.shape[1]) if resharded else 0

    def wq_copy(n):
        cols = pl.ds(pl.multiple_of((chip ^ (CHIPS - 1 - n)) * wide_cols, HEAD), wide_cols)
        return pltpu.make_async_copy(wq_ref.at[:, cols], wo.at[:, n * wide_cols:(n + 1) * wide_cols], w_sem.at[2 + n])

    kv_loads = [pltpu.make_async_copy(wk_ref, wkv.at[0], w_sem.at[0]), pltpu.make_async_copy(wv_ref, wkv.at[1], w_sem.at[1])]
    trig_load = pltpu.make_async_copy(trig_ref.at[pl.ds(me * tok, tok)], trig, trig_sem)
    trig_load.start()
    for c in [wq_copy(n) for n in range(CHIPS)] + kv_loads:
        c.start()
    meet(across[1:] + [partner])

    own = [pltpu.make_async_copy(k4_ref.at[chip], kb.at[0], loc_sem.at[0]),
           pltpu.make_async_copy(v4_ref.at[chip], vb.at[0], loc_sem.at[1])]
    for c in own:
        c.start()

    def kv_copy(step, which):
        src, dst = (k4_ref, kb) if which == 0 else (v4_ref, vb)
        return remote(src.at[chip ^ step], dst.at[2 * step], kv_send.at[step - 1, which], kv_recv.at[step - 1, which],
                      across[step])

    def pair_copy(step, which):
        dst = kb if which == 0 else vb
        if step == 0:
            src = (k4_ref if which == 0 else v4_ref).at[chip]
        else:
            src = dst.at[2 * step]
        return remote(src, dst.at[2 * step + 1], pair_send.at[step, which], pair_recv.at[step, which], partner)

    if resharded:
        loads = []
        for j in range(1, SLOTS):
            loads.append((pltpu.make_async_copy(kin_ref.at[j], kb.at[j], loc_sem.at[2 * j]),
                          pltpu.make_async_copy(vin_ref.at[j], vb.at[j], loc_sem.at[2 * j + 1])))
        for pair in loads:
            for c in pair:
                c.start()
    else:
        for which in range(2):
            pair_copy(0, which).start()
        kv_copy(1, 0).start()
        kv_copy(2, 0).start()

    if resharded:
        xn[...] = norm_rows(a_ref[...].astype(jnp.float32))
    else:
        xn[...] = a_ref[...]

    trig_load.wait()

    def rope(plain):
        wide = plain.astype(jnp.float32)
        return (wide * trig[:, :HEAD] + pltpu.roll(wide, HEAD // 2, 1) * trig[:, HEAD:]).astype(jnp.bfloat16)

    def q_copy(n):
        return remote(msg.at[n, pl.ds(0, GROUP)], got.at[n, pl.ds(0, GROUP)], q_send.at[n], q_recv.at[n],
                      2 * (chip ^ (CHIPS - 1 - n)) + core)

    def project(n, carry):
        pltpu.make_async_copy(wo.at[:, :wide_cols], wo.at[:, :wide_cols], w_sem.at[2 + n]).wait()
        grp = chip ^ (CHIPS - 1 - n)
        cols = pl.ds(pl.multiple_of(n * wide_cols, HEAD), wide_cols)
        bias = bias_ref[:, pl.ds(pl.multiple_of(bias_at + grp * wide_cols, HEAD), wide_cols)].astype(jnp.float32)
        q_pre = (jnp.dot(xn[...], wo[:, cols], preferred_element_type=jnp.float32) + bias).astype(jnp.bfloat16)
        for g in range(GROUP):
            msg[n, g] = rope(q_pre[:, g * HEAD:(g + 1) * HEAD])
        @pl.when(n < CHIPS - 1)
        def _():
            q_copy(n).start()

        return carry

    if not resharded:
        pack_start(knext_ref, raw, raw_sem)
    lax.fori_loop(0, CHIPS, project, 0)
    kv_loads[0].wait()
    k_pre = (jnp.dot(xn[...], wkv[0], preferred_element_type=jnp.float32)
             + bias_ref[:, bias_at + n_q:bias_at + n_q + KV_HEADS * HEAD].astype(jnp.float32)).astype(jnp.bfloat16)
    for c in range(KV_HEADS):
        knew_ref[c] = rope(k_pre[:, c * HEAD:(c + 1) * HEAD])
    kv_loads[1].wait()
    v_pre = jnp.dot(xn[...], wkv[1], preferred_element_type=jnp.float32).astype(jnp.bfloat16)
    for c in range(KV_HEADS):
        vnew_ref[c] = v_pre[:, c * HEAD:(c + 1) * HEAD]

    kv_msgs = []
    for n in range(CHIPS):
        grp = chip ^ (CHIPS - 1 - n)
        msg[n, GROUP] = knew_ref[grp]
        msg[n, GROUP + 1] = vnew_ref[grp]
        if n < CHIPS - 1:
            kv_msgs.append(remote(msg.at[n, pl.ds(GROUP, 2)], got.at[n, pl.ds(GROUP, 2)], kvm_send.at[n], kvm_recv.at[n],
                                  2 * grp + core))
            kv_msgs[-1].start()
    q_copies = [q_copy(n) for n in range(CHIPS - 1)]
    parts = [msg.at[CHIPS - 1]] + [got.at[CHIPS - 1 - s] for s in range(1, CHIPS)]
    wo_load = pltpu.make_async_copy(wo_ref, wo, wo_sem)
    if not resharded:
        for step, which in ((1, 1), (2, 1), (3, 0), (3, 1)):
            kv_copy(step, which).start()
    if not resharded:
        pack_heads(knext_ref, kpack_ref, raw, tmp, raw_sem, out_sem)
        pack_start(vnext_ref, raw, raw_sem)
        pack_heads(vnext_ref, vpack_ref, raw, tmp, raw_sem, out_sem)
    wo_load.start()
    acc[...] = jnp.zeros_like(acc)
    m_run[...] = jnp.full_like(m_run, -jnp.inf)
    l_run[...] = jnp.zeros_like(l_run)
    for c in q_copies:
        c.wait_recv()
    new_copies = [remote(parts[s].at[pl.ds(GROUP, 2)], peer_new.at[s], new_send.at[s], new_recv.at[s], partner) for s in range(CHIPS)]
    for g in range(GROUP):
        qt[g] = jnp.concatenate([p[g] for p in parts], axis=0).T
    def relay(step):
        for which in range(2):
            kv_copy(step, which).wait_recv()
            pair_copy(step, which).start()

    def ready(j):
        for jj in range(CHIPS):
            @pl.when(j == jj)
            def _():
                if jj == 0:
                    for c in own:
                        c.wait()
                elif resharded:
                    for c in loads[2 * jj - 1]:
                        c.wait()
                elif jj != 2:
                    relay(jj)
        vt[j % 2, :, :chunk] = vb[2 * j].T
        for jj in range(CHIPS):
            @pl.when(j == jj)
            def _():
                if resharded:
                    for c in loads[2 * jj]:
                        c.wait()
                else:
                    for which in range(2):
                        pair_copy(jj, which).wait_recv()
        vt[j % 2, :, chunk:] = vb[2 * j + 1].T

    def place(item):
        return item // GROUP, item % GROUP

    def score(item, s_dst, m_dst):
        j, g = place(item)
        part = jnp.full((8, rows), -jnp.inf, jnp.float32)
        for t in range(2 * chunk // 256):
            at = (t * 256) % chunk
            s_blk = jnp.dot(kb[2 * j + t * 256 // chunk, at:at + 256, :], qt[g], preferred_element_type=jnp.float32)
            s_dst[t * 256:(t + 1) * 256, :] = s_blk
            part = jnp.maximum(part, jnp.max(s_blk.reshape(32, 8, rows), axis=0))
        m_dst[...] = part

    def absorb(item, s_src, m_src):
        j, g = place(item)
        m_old = m_run[g]
        m_new = jnp.maximum(m_old, jnp.max(m_src[...], axis=0, keepdims=True))
        alpha = jnp.exp2((m_old - m_new) * scale2)
        shift = m_new * scale2
        l_part = jnp.zeros((8, rows), jnp.float32)
        out = jnp.zeros((HEAD, rows), jnp.float32)
        for t in range(2 * chunk // 256):
            p = jnp.exp2(s_src[t * 256:(t + 1) * 256, :] * scale2 - shift)
            l_part = l_part + jnp.sum(p.reshape(32, 8, rows), axis=0)
            out = out + jnp.dot(vt[j % 2, :, t * 256:(t + 1) * 256], p.astype(jnp.bfloat16),
                                preferred_element_type=jnp.float32)
        acc[g] = acc[g] * alpha + out
        l_run[g] = l_run[g] * alpha + l_part
        m_run[g] = m_new

    ready(0)
    score(0, s_even, m_even)

    new_len = newk.shape[0]

    key_i = lax.broadcasted_iota(jnp.int32, (new_len, rows), 0)
    qry_i = lax.broadcasted_iota(jnp.int32, (new_len, rows), 1)
    blk = key_i // tok
    k_pos = (2 * (chip ^ (blk % CHIPS)) + (core ^ (blk // CHIPS))) * tok + key_i % tok
    q_pos = (2 * (chip ^ (qry_i // tok)) + core) * tok + qry_i % tok
    hide[...] = jnp.where(k_pos <= q_pos, 0.0, -jnp.inf)

    def o_copy(g, s):
        src = o_send.at[g, s]
        dst = o_all.at[:, pl.ds(pl.multiple_of(chip * wide_cols + g * HEAD, HEAD), HEAD)]
        return remote(src, dst, o_ssem.at[g, s - 1], o_rsem.at[g, s - 1], across[s])

    def finish(g):
        s = jnp.dot(newk[...], qt[g], preferred_element_type=jnp.float32) + hide[...]
        m_old = m_run[g]
        m_new = jnp.maximum(m_old, jnp.max(s, axis=0, keepdims=True))
        alpha = jnp.exp2((m_old - m_new) * scale2)
        p = jnp.exp2(s * scale2 - m_new * scale2)
        total = jnp.sum(l_run[g] * alpha, axis=0, keepdims=True) + jnp.sum(p, axis=0, keepdims=True)
        fresh = lax.dot_general(newv[...], p.astype(jnp.bfloat16), (((0,), (0,)), ((), ())),
                                preferred_element_type=jnp.float32)
        out = ((acc[g] * alpha + fresh) / total).T.astype(jnp.bfloat16)
        for s_i in range(1, CHIPS):
            o_send[g, s_i] = out[s_i * tok:(s_i + 1) * tok, :]
            o_copy(g, s_i).start()
        o_all[:, pl.ds(pl.multiple_of(chip * wide_cols + g * HEAD, HEAD), HEAD)] = out[:tok, :]

    def step(item, carry):
        nxt = item + 1

        if not resharded:
            @pl.when(nxt == GROUP + 4)
            def _():
                relay(2)

        @pl.when((nxt % GROUP == 0) & (nxt < n_items))
        def _():
            ready(nxt // GROUP)

        @pl.when(item == 2)
        def _():
            for c in kv_msgs:
                c.wait_recv()
            for c in new_copies:
                c.start()
            for s in range(CHIPS):
                newk[s * tok:(s + 1) * tok, :] = parts[s][GROUP]
                newv[s * tok:(s + 1) * tok, :] = parts[s][GROUP + 1]

        @pl.when(item == n_first)
        def _():
            for c in new_copies:
                c.wait_recv()
            for s in range(CHIPS):
                at = (CHIPS + s) * tok
                newk[at:at + tok, :] = peer_new[s, 0]
                newv[at:at + tok, :] = peer_new[s, 1]

        after = jnp.minimum(nxt, n_items - 1)

        @pl.when(item % 2 == 0)
        def _():
            score(after, s_odd, m_odd)
            absorb(item, s_even, m_even)

        @pl.when(item % 2 == 1)
        def _():
            score(after, s_even, m_even)
            absorb(item, s_odd, m_odd)

        @pl.when(item >= n_first)
        def _():
            finish(item - n_first)

        return carry

    lax.fori_loop(0, n_items, step, 0)
    o_copies = [o_copy(g, s) for g in range(GROUP) for s in range(1, CHIPS)]
    last = 3 * (GROUP - 1)
    wo_load.wait()
    for c in o_copies[:last]:
        c.wait_recv()

    def heads(s, first, count):
        at = pl.multiple_of((chip ^ s) * wide_cols + first * HEAD, HEAD)
        return pl.ds(at, count * HEAD)

    def early_proj(blk, carry):
        cols = pl.ds(pl.multiple_of(blk * COL, COL), COL)
        total = jnp.zeros((tok, COL), jnp.float32)
        for s in range(CHIPS):
            part = heads(s, 0, GROUP if s == 0 else GROUP - 1)
            total = total + jnp.dot(o_all[:, part], wo[part, cols], preferred_element_type=jnp.float32)
        y_acc[:, cols] = total
        return carry

    lax.fori_loop(0, wo.shape[1] // COL, early_proj, 0)
    for c in o_copies[last:]:
        c.wait_recv()

    def out_proj(blk, carry):
        cols = pl.ds(pl.multiple_of(blk * 2 * COL, 2 * COL), 2 * COL)
        total = y_acc[:, cols]
        for s in range(1, CHIPS):
            part = heads(s, GROUP - 1, 1)
            total = total + jnp.dot(o_all[:, part], wo[part, cols], preferred_element_type=jnp.float32)
        y = total.astype(jnp.bfloat16)
        if not resharded:
            y = (a_ref[:, cols].astype(jnp.float32) + y.astype(jnp.float32)).astype(jnp.bfloat16)
        y_ref[:, cols] = y
        return carry

    lax.fori_loop(0, wo.shape[1] // (2 * COL), out_proj, 0)

    for c in q_copies + kv_msgs + new_copies + o_copies:
        c.wait_send()
    if not resharded:
        for step in range(CHIPS):
            for which in range(2):
                pair_copy(step, which).wait_send()
                if step:
                    kv_copy(step, which).wait_send()


def run_layer(resharded, a, bias, trig, k4, v4, k_in, v_in, w_q, w_k, w_v, w_o, collective_id):
    tok, width = a.shape
    chunk = k4.shape[1]
    rows = CHIPS * tok
    bf16, f32 = jnp.bfloat16, jnp.float32
    vmem = pl.BlockSpec(memory_space=pltpu.VMEM)
    hbm = pl.BlockSpec(memory_space=pl.ANY)
    dma = pltpu.SemaphoreType.DMA
    packed = [] if resharded else [jax.ShapeDtypeStruct(k4.shape, bf16)] * 2
    packing = [] if resharded else [
        pltpu.VMEM((RING, PIECE, KV_HEADS, HEAD), bf16),
        pltpu.VMEM((2, KV_HEADS, PIECE, HEAD), bf16),
        dma((RING,)), dma((2,)),
    ]
    return pl.pallas_call(
        functools.partial(layer_kernel, resharded),
        out_shape=[jax.ShapeDtypeStruct((tok, width), bf16),
                   jax.ShapeDtypeStruct((KV_HEADS, tok, HEAD), bf16),
                   jax.ShapeDtypeStruct((KV_HEADS, tok, HEAD), bf16)] + packed,
        in_specs=[vmem] * 2 + [hbm] * 9,
        out_specs=[vmem] * 3 + [hbm] * len(packed),
        scratch_shapes=[
            pltpu.VMEM((tok, width), bf16),
            pltpu.VMEM((tok, 2 * HEAD), f32),
            pltpu.VMEM((2,) + w_k.shape, bf16),
            pltpu.VMEM(w_o.shape, bf16),
            pltpu.VMEM((SLOTS, chunk, HEAD), bf16),
            pltpu.VMEM((SLOTS, chunk, HEAD), bf16),
            pltpu.VMEM((2, HEAD, 2 * chunk), bf16),
            pltpu.VMEM((KV_HEADS, GROUP + 2, tok, HEAD), bf16),
            pltpu.VMEM((CHIPS - 1, GROUP + 2, tok, HEAD), bf16),
            pltpu.VMEM((CHIPS, 2, tok, HEAD), bf16),
            pltpu.VMEM((2 * rows, HEAD), bf16),
            pltpu.VMEM((2 * rows, HEAD), bf16),
            pltpu.VMEM((GROUP, HEAD, rows), bf16),
            pltpu.VMEM((2 * chunk, rows), f32),
            pltpu.VMEM((2 * chunk, rows), f32),
            pltpu.VMEM((8, rows), f32),
            pltpu.VMEM((8, rows), f32),
            pltpu.VMEM((GROUP, HEAD, rows), f32),
            pltpu.VMEM((GROUP, 1, rows), f32),
            pltpu.VMEM((GROUP, 8, rows), f32),
            pltpu.VMEM((2 * rows, rows), f32),
            pltpu.VMEM((GROUP, CHIPS, tok, HEAD), bf16),
            pltpu.VMEM((tok, CHIPS * GROUP * HEAD), bf16),
            pltpu.VMEM((tok, width), f32),
            dma, dma((2 + CHIPS,)), dma, dma((2 * SLOTS,)),
            dma((CHIPS - 1, 2)), dma((CHIPS - 1, 2)), dma((CHIPS, 2)), dma((CHIPS, 2)),
            dma((CHIPS - 1,)), dma((CHIPS - 1,)), dma((CHIPS,)), dma((CHIPS,)),
            dma((GROUP, CHIPS - 1)), dma((GROUP, CHIPS - 1)), dma((CHIPS - 1,)), dma((CHIPS - 1,)),
        ] + packing,
        compiler_params=pltpu.CompilerParams(collective_id=collective_id, has_side_effects=True, vmem_limit_bytes=VMEM_ALL),
        name="layer",
    )(a, bias, trig, k4, v4, k_in, v_in, w_q, w_k, w_v, w_o)


def mlp_kernel(h_ref, k4_ref, v4_ref, gate_ref, up_ref, down_ref, g_ref, kout_ref, vout_ref,
               u, wg, wu, wd, acc, theirs, w_sem, u_send, u_recv, part_send, part_recv, kv_send, kv_recv, pair_send, pair_recv):
    chip, core, across, partner = peers()
    tok = h_ref.shape[0]
    n_buf = wg.shape[0]
    steps = gate_ref.shape[1] // (2 * COL)

    def copies(i):
        slot = i % n_buf
        cols = pl.ds(pl.multiple_of((core * steps + i) * COL, COL), COL)
        return (pltpu.make_async_copy(gate_ref.at[:, cols], wg.at[slot], w_sem.at[slot, 0]),
                pltpu.make_async_copy(up_ref.at[:, cols], wu.at[slot], w_sem.at[slot, 1]),
                pltpu.make_async_copy(down_ref.at[cols, :], wd.at[slot], w_sem.at[slot, 2]))

    for b in range(n_buf):
        for c in copies(b):
            c.start()
    meet(across[1:] + [partner])
    u[:tok, :] = norm_rows(h_ref[...].astype(jnp.float32))
    u_copy = remote(u.at[pl.ds(0, tok)], u.at[pl.ds(tok, tok)], u_send, u_recv, partner)
    u_copy.start()

    def kv_copy(step, which):
        src, dst = (k4_ref, kout_ref) if which == 0 else (v4_ref, vout_ref)
        return remote(src.at[chip ^ step], dst.at[2 * step], kv_send.at[step - 1, which], kv_recv.at[step - 1, which],
                      across[step])

    def pair_copy(step, which):
        dst = kout_ref if which == 0 else vout_ref
        src = (k4_ref if which == 0 else v4_ref).at[chip] if step == 0 else dst.at[2 * step]
        return remote(src, dst.at[2 * step + 1], pair_send.at[step, which], pair_recv.at[step, which], partner)

    for step in range(1, CHIPS):
        for which in range(2):
            kv_copy(step, which).start()
    for which in range(2):
        pair_copy(0, which).start()
    acc[...] = jnp.zeros_like(acc)
    u_copy.wait_recv()

    def relay(step):
        for which in range(2):
            kv_copy(step, which).wait_recv()
            pair_copy(step, which).start()

    def block(i, carry):
        slot = i % n_buf
        for c in copies(i):
            c.wait()
        gate = jnp.dot(u[...], wg[slot], preferred_element_type=jnp.float32).astype(jnp.bfloat16).astype(jnp.float32)
        up = jnp.dot(u[...], wu[slot], preferred_element_type=jnp.float32).astype(jnp.bfloat16).astype(jnp.float32)
        mixed = (gate * jax.nn.sigmoid(gate) * up).astype(jnp.bfloat16)
        acc[...] += jnp.dot(mixed, wd[slot], preferred_element_type=jnp.float32)

        @pl.when(i + n_buf < steps)
        def _():
            for c in copies(i + n_buf):
                c.start()

        @pl.when(i == steps - 12)
        def _():
            relay(1)
            relay(2)

        @pl.when(i == steps - 5)
        def _():
            relay(3)

        return carry

    lax.fori_loop(0, steps, block, 0)
    part_copy = remote(acc.at[pl.ds(tok, tok)], theirs, part_send, part_recv, partner)
    part_copy.start()
    part_copy.wait_recv()
    g_ref[...] = (h_ref[...].astype(jnp.float32) + (acc[:tok, :] + theirs[...])).astype(jnp.bfloat16)
    for step in range(CHIPS):
        for which in range(2):
            pair_copy(step, which).wait()
            if step:
                kv_copy(step, which).wait_send()
    u_copy.wait_send()
    part_copy.wait_send()


def run_mlp(h, k4, v4, w_gate, w_up, w_down, collective_id):
    tok, width = h.shape
    chunk = k4.shape[1]
    bf16, f32 = jnp.bfloat16, jnp.float32
    vmem = pl.BlockSpec(memory_space=pltpu.VMEM)
    hbm = pl.BlockSpec(memory_space=pl.ANY)
    dma = pltpu.SemaphoreType.DMA
    n_buf = 4
    slots = jax.ShapeDtypeStruct((SLOTS, chunk, HEAD), bf16)
    return pl.pallas_call(
        mlp_kernel,
        out_shape=[jax.ShapeDtypeStruct((tok, width), bf16), slots, slots],
        in_specs=[vmem] + [hbm] * 5,
        out_specs=[vmem, hbm, hbm],
        scratch_shapes=[
            pltpu.VMEM((2 * tok, width), bf16),
            pltpu.VMEM((n_buf, width, COL), bf16),
            pltpu.VMEM((n_buf, width, COL), bf16),
            pltpu.VMEM((n_buf, COL, width), bf16),
            pltpu.VMEM((2 * tok, width), f32),
            pltpu.VMEM((tok, width), f32),
            dma((n_buf, 3)), dma, dma, dma, dma,
            dma((CHIPS - 1, 2)), dma((CHIPS - 1, 2)), dma((CHIPS, 2)), dma((CHIPS, 2)),
        ],
        compiler_params=pltpu.CompilerParams(collective_id=collective_id, has_side_effects=True, vmem_limit_bytes=60 * MIB),
        name="mlp",
    )(h, k4, v4, w_gate, w_up, w_down)


def heads_first(cache):
    return lax.optimization_barrier(jnp.transpose(cache, (1, 0, 2)))


def order_kernel(g_ref, y_ref, *refs):
    g_out, y_out = refs[4:6]
    g_out[...] = g_ref[...]
    y_out[...] = y_ref[...]
    for src, dst in zip(refs[:4], refs[6:]):
        for c in range(KV_HEADS):
            dst[:, c, :] = src[c]


def order_outputs(hidden, y_two, *appends):
    tok = hidden.shape[0]
    rows = [jax.ShapeDtypeStruct(t.shape, t.dtype) for t in (hidden, y_two)]
    lines = [jax.ShapeDtypeStruct((tok, KV_HEADS, HEAD), t.dtype) for t in appends]
    vmem = pl.BlockSpec(memory_space=pltpu.VMEM)
    return pl.pallas_call(order_kernel, out_shape=rows + lines, in_specs=[vmem] * 6, out_specs=[vmem] * 6,
                          name="order_outputs")(hidden, y_two, *appends)


def solution(mesh):
    axis_size = mesh.shape['cp']
    rows_spec = P(('dp', 'cp'), None)
    cache_spec = P(('dp', 'cp'), None, None)
    mat_spec = P(None, None)
    vec_spec = P(None)
    layer_specs = (cache_spec, cache_spec, mat_spec, vec_spec, mat_spec, vec_spec, mat_spec, mat_spec)
    in_specs = (rows_spec,) + layer_specs + (mat_spec, mat_spec, mat_spec) + layer_specs
    out_specs = (rows_spec, rows_spec, cache_spec, cache_spec, cache_spec, cache_spec)

    def forward(x_in, cache_k1, cache_v1, w_q1, b_q1, w_k1, b_k1, w_v1, w_o1, w_gate, w_up, w_down, cache_k2, cache_v2, w_q2, b_q2, w_k2, b_k2, w_v2, w_o2):
        n_tok = axis_size * x_in.shape[0]
        trig = rope_table(axis_size * cache_k1.shape[0], n_tok)
        bias = jnp.concatenate([b_q1, b_k1, b_q2, b_k2]).reshape(1, -1)
        k4a, v4a = heads_first(cache_k1), heads_first(cache_v1)
        resid_h, k_one, v_one, k4b, v4b = run_layer(False, x_in, bias, trig, k4a, v4a, cache_k2, cache_v2, w_q1, w_k1, w_v1, w_o1, 1)
        hidden, k_in, v_in = run_mlp(resid_h, k4b, v4b, w_gate, w_up, w_down, 2)
        y_two, k_two, v_two = run_layer(True, hidden, bias, trig, k4b, v4b, k_in, v_in, w_q2, w_k2, w_v2, w_o2, 3)
        return order_outputs(hidden, y_two, k_one, v_one, k_two, v_two)

    return jax.shard_map(forward, mesh=mesh, in_specs=in_specs, out_specs=out_specs, check_vma=False)
```

```python
import functools

import jax
import jax.numpy as jnp
import numpy as np
from jax import lax
from jax.experimental import pallas as pl
from jax.experimental.pallas import tpu as pltpu
from jax.sharding import PartitionSpec as P

ROPE_THETA = 500000.0
NORM_EPS = 1e-5
LOG2E = 1.4426950408889634
KV_HEADS = 4
HEAD = 128
GROUP = 7
CHIPS = 4
COL = 256
SLOTS = 2 * CHIPS
MIB = 1024 * 1024
VMEM_ALL = 67_000_000
PIECE = 256
RING = 4
MESH = pl.DeviceIdType.MESH


@functools.lru_cache(maxsize=None)
def rope_table(first, count):
    with jax.ensure_compile_time_eval():
        half_dim = HEAD // 2
        inv_freq = 1.0 / (ROPE_THETA ** (jnp.arange(half_dim, dtype=jnp.float32) * (2.0 / HEAD)))
        angles = (first + jnp.arange(count)).astype(jnp.float32)[:, None] * inv_freq[None, :]
        cos_t, sin_t = jnp.cos(angles), jnp.sin(angles)
        return np.asarray(jnp.concatenate([cos_t, cos_t, -sin_t, sin_t], axis=-1))


def norm_rows(wide):
    return (wide * lax.rsqrt(jnp.mean(wide * wide, axis=-1, keepdims=True) + NORM_EPS)).astype(jnp.bfloat16)


def peers():
    me = lax.axis_index('cp')
    chip, core = me // 2, me % 2
    across = [2 * (chip ^ step) + core for step in range(CHIPS)]
    return chip, core, across, 2 * chip + (1 - core)


def meet(others):
    barrier = pltpu.get_barrier_semaphore()
    for dev in others:
        pl.semaphore_signal(barrier, inc=1, device_id={'cp': dev}, device_id_type=MESH)
    pl.semaphore_wait(barrier, len(others))


def remote(src, dst, send_sem, recv_sem, dev):
    return pltpu.make_async_remote_copy(src_ref=src, dst_ref=dst, send_sem=send_sem, recv_sem=recv_sem,
                                        device_id={'cp': dev}, device_id_type=MESH)


def pack_start(src_ref, raw, sem):
    for i in range(RING):
        pltpu.make_async_copy(src_ref.at[pl.ds(i * PIECE, PIECE)], raw.at[i], sem.at[i]).start()


def pack_heads(src_ref, dst_ref, raw, tmp, sem, out_sem):
    n = src_ref.shape[0] // PIECE

    def put(i, slot):
        span = pl.ds(pl.multiple_of(i * PIECE, PIECE), PIECE)
        return pltpu.make_async_copy(tmp.at[slot], dst_ref.at[:, span], out_sem.at[slot])

    def piece(i, carry):
        slot = i % RING
        side = i % 2
        pltpu.make_async_copy(raw.at[slot], raw.at[slot], sem.at[slot]).wait()

        @pl.when(i >= 2)
        def _():
            put(i - 2, side).wait()

        for part in range(2):
            half = PIECE // 2
            flat = jnp.swapaxes(raw[slot, part * half:(part + 1) * half], 0, 1)
            for c in range(KV_HEADS):
                tmp[side, c, part * half:(part + 1) * half, :] = flat[c]

        @pl.when(i + RING < n)
        def _():
            pltpu.make_async_copy(src_ref.at[pl.ds((i + RING) * PIECE, PIECE)], raw.at[slot], sem.at[slot]).start()

        put(i, side).start()
        return carry

    lax.fori_loop(0, n, piece, 0)
    put(n - 2, 0).wait()
    put(n - 1, 1).wait()


def layer_kernel(resharded, a_ref, bq_ref, bk_ref, trig_ref, k4_ref, v4_ref, *refs):
    if resharded:
        kin_ref, vin_ref, wq_ref, wk_ref, wv_ref, wo_ref = refs[:6]
        refs = refs[6:]
    else:
        knext_ref, vnext_ref, wq_ref, wk_ref, wv_ref, wo_ref = refs[:6]
        refs = refs[6:]
        kpack_ref, vpack_ref = refs[3:5]
        raw, tmp, raw_sem, out_sem = refs[-4:]
        refs = refs[:3] + refs[5:-4]
    (y_ref, knew_ref, vnew_ref, xn, trig, wkv, wo, kb, vb, vt, msg, got, peer_new, newk, newv, qt,
     s_even, s_odd, m_even, m_odd, acc, m_run, l_run, hide, o_send, o_all, y_acc,
     trig_sem, w_sem, wo_sem, loc_sem, kv_send, kv_recv, pair_send, pair_recv, q_send, q_recv,
     new_send, new_recv, o_ssem, o_rsem, kvm_send, kvm_recv, b_q, b_k) = refs
    chip, core, across, partner = peers()
    me = 2 * chip + core
    scale2 = HEAD ** -0.5 * LOG2E
    tok = a_ref.shape[0]
    chunk = kb.shape[1]
    rows = qt.shape[2]
    wide_cols = GROUP * HEAD
    n_items = CHIPS * GROUP
    n_first = (CHIPS - 1) * GROUP

    def wq_copy(n):
        cols = pl.ds(pl.multiple_of((chip ^ (CHIPS - 1 - n)) * wide_cols, HEAD), wide_cols)
        return pltpu.make_async_copy(wq_ref.at[:, cols], wo.at[:, n * wide_cols:(n + 1) * wide_cols], w_sem.at[2 + n])

    kv_loads = [pltpu.make_async_copy(wk_ref, wkv.at[0], w_sem.at[0]), pltpu.make_async_copy(wv_ref, wkv.at[1], w_sem.at[1])]
    trig_load = pltpu.make_async_copy(trig_ref.at[pl.ds(me * tok, tok)], trig, trig_sem)
    trig_load.start()
    for c in [wq_copy(n) for n in range(CHIPS)] + kv_loads:
        c.start()
    meet(across[1:] + [partner])

    own = [pltpu.make_async_copy(k4_ref.at[chip], kb.at[0], loc_sem.at[0]),
           pltpu.make_async_copy(v4_ref.at[chip], vb.at[0], loc_sem.at[1])]
    for c in own:
        c.start()

    def kv_copy(step, which):
        src, dst = (k4_ref, kb) if which == 0 else (v4_ref, vb)
        return remote(src.at[chip ^ step], dst.at[2 * step], kv_send.at[step - 1, which], kv_recv.at[step - 1, which],
                      across[step])

    def pair_copy(step, which):
        dst = kb if which == 0 else vb
        if step == 0:
            src = (k4_ref if which == 0 else v4_ref).at[chip]
        else:
            src = dst.at[2 * step]
        return remote(src, dst.at[2 * step + 1], pair_send.at[step, which], pair_recv.at[step, which], partner)

    if resharded:
        loads = []
        for j in range(1, SLOTS):
            loads.append((pltpu.make_async_copy(kin_ref.at[j], kb.at[j], loc_sem.at[2 * j]),
                          pltpu.make_async_copy(vin_ref.at[j], vb.at[j], loc_sem.at[2 * j + 1])))
        for pair in loads:
            for c in pair:
                c.start()
    else:
        for which in range(2):
            pair_copy(0, which).start()
        kv_copy(1, 0).start()
        kv_copy(2, 0).start()

    if resharded:
        xn[...] = norm_rows(a_ref[...].astype(jnp.float32))
    else:
        xn[...] = a_ref[...]

    b_q[...] = bq_ref[...].astype(jnp.float32)
    b_k[...] = bk_ref[...].astype(jnp.float32)
    trig_load.wait()

    def rope(plain):
        wide = plain.astype(jnp.float32)
        return (wide * trig[:, :HEAD] + pltpu.roll(wide, HEAD // 2, 1) * trig[:, HEAD:]).astype(jnp.bfloat16)

    def q_copy(n):
        return remote(msg.at[n, pl.ds(0, GROUP)], got.at[n, pl.ds(0, GROUP)], q_send.at[n], q_recv.at[n],
                      2 * (chip ^ (CHIPS - 1 - n)) + core)

    def project(n, carry):
        pltpu.make_async_copy(wo.at[:, :wide_cols], wo.at[:, :wide_cols], w_sem.at[2 + n]).wait()
        grp = chip ^ (CHIPS - 1 - n)
        cols = pl.ds(pl.multiple_of(n * wide_cols, HEAD), wide_cols)
        q_pre = jnp.dot(xn[...], wo[:, cols], preferred_element_type=jnp.float32)
        for g in range(GROUP):
            row = b_q[pl.ds(grp * GROUP + g, 1), :]
            msg[n, g] = rope((q_pre[:, g * HEAD:(g + 1) * HEAD] + row).astype(jnp.bfloat16))
        @pl.when(n < CHIPS - 1)
        def _():
            q_copy(n).start()

        return carry

    if not resharded:
        pack_start(knext_ref, raw, raw_sem)
    lax.fori_loop(0, CHIPS, project, 0)
    kv_loads[0].wait()
    k_pre = jnp.dot(xn[...], wkv[0], preferred_element_type=jnp.float32)
    for c in range(KV_HEADS):
        knew_ref[c] = rope((k_pre[:, c * HEAD:(c + 1) * HEAD] + b_k[c:c + 1, :]).astype(jnp.bfloat16))
    kv_loads[1].wait()
    v_pre = jnp.dot(xn[...], wkv[1], preferred_element_type=jnp.float32).astype(jnp.bfloat16)
    for c in range(KV_HEADS):
        vnew_ref[c] = v_pre[:, c * HEAD:(c + 1) * HEAD]

    kv_msgs = []
    for n in range(CHIPS):
        grp = chip ^ (CHIPS - 1 - n)
        msg[n, GROUP] = knew_ref[grp]
        msg[n, GROUP + 1] = vnew_ref[grp]
        if n < CHIPS - 1:
            kv_msgs.append(remote(msg.at[n, pl.ds(GROUP, 2)], got.at[n, pl.ds(GROUP, 2)], kvm_send.at[n], kvm_recv.at[n],
                                  2 * grp + core))
            kv_msgs[-1].start()
    q_copies = [q_copy(n) for n in range(CHIPS - 1)]
    parts = [msg.at[CHIPS - 1]] + [got.at[CHIPS - 1 - s] for s in range(1, CHIPS)]
    wo_load = pltpu.make_async_copy(wo_ref, wo, wo_sem)
    if not resharded:
        for step, which in ((1, 1), (2, 1), (3, 0), (3, 1)):
            kv_copy(step, which).start()
    if not resharded:
        pack_heads(knext_ref, kpack_ref, raw, tmp, raw_sem, out_sem)
        pack_start(vnext_ref, raw, raw_sem)
        pack_heads(vnext_ref, vpack_ref, raw, tmp, raw_sem, out_sem)
    wo_load.start()
    acc[...] = jnp.zeros_like(acc)
    m_run[...] = jnp.full_like(m_run, -jnp.inf)
    l_run[...] = jnp.zeros_like(l_run)
    for c in q_copies:
        c.wait_recv()
    new_copies = [remote(parts[s].at[pl.ds(GROUP, 2)], peer_new.at[s], new_send.at[s], new_recv.at[s], partner) for s in range(CHIPS)]
    for g in range(GROUP):
        qt[g] = jnp.concatenate([p[g] for p in parts], axis=0).T
    def relay(step):
        for which in range(2):
            kv_copy(step, which).wait_recv()
            pair_copy(step, which).start()

    def ready(j):
        for jj in range(CHIPS):
            @pl.when(j == jj)
            def _():
                if jj == 0:
                    for c in own:
                        c.wait()
                elif resharded:
                    for c in loads[2 * jj - 1]:
                        c.wait()
                elif jj != 2:
                    relay(jj)
        vt[j % 2, :, :chunk] = vb[2 * j].T
        for jj in range(CHIPS):
            @pl.when(j == jj)
            def _():
                if resharded:
                    for c in loads[2 * jj]:
                        c.wait()
                else:
                    for which in range(2):
                        pair_copy(jj, which).wait_recv()
        vt[j % 2, :, chunk:] = vb[2 * j + 1].T

    def place(item):
        return item // GROUP, item % GROUP

    def score(item, s_dst, m_dst):
        j, g = place(item)
        part = jnp.full((8, rows), -jnp.inf, jnp.float32)
        for t in range(2 * chunk // 256):
            at = (t * 256) % chunk
            s_blk = jnp.dot(kb[2 * j + t * 256 // chunk, at:at + 256, :], qt[g], preferred_element_type=jnp.float32)
            s_dst[t * 256:(t + 1) * 256, :] = s_blk
            part = jnp.maximum(part, jnp.max(s_blk.reshape(32, 8, rows), axis=0))
        m_dst[...] = part

    def absorb(item, s_src, m_src):
        j, g = place(item)
        m_old = m_run[g]
        m_new = jnp.maximum(m_old, jnp.max(m_src[...], axis=0, keepdims=True))
        alpha = jnp.exp2((m_old - m_new) * scale2)
        shift = m_new * scale2
        l_part = jnp.zeros((8, rows), jnp.float32)
        out = jnp.zeros((HEAD, rows), jnp.float32)
        for t in range(2 * chunk // 256):
            p = jnp.exp2(s_src[t * 256:(t + 1) * 256, :] * scale2 - shift)
            l_part = l_part + jnp.sum(p.reshape(32, 8, rows), axis=0)
            out = out + jnp.dot(vt[j % 2, :, t * 256:(t + 1) * 256], p.astype(jnp.bfloat16),
                                preferred_element_type=jnp.float32)
        acc[g] = acc[g] * alpha + out
        l_run[g] = l_run[g] * alpha + l_part
        m_run[g] = m_new

    ready(0)
    score(0, s_even, m_even)

    new_len = newk.shape[0]

    key_i = lax.broadcasted_iota(jnp.int32, (new_len, rows), 0)
    qry_i = lax.broadcasted_iota(jnp.int32, (new_len, rows), 1)
    blk = key_i // tok
    k_pos = (2 * (chip ^ (blk % CHIPS)) + (core ^ (blk // CHIPS))) * tok + key_i % tok
    q_pos = (2 * (chip ^ (qry_i // tok)) + core) * tok + qry_i % tok
    hide[...] = jnp.where(k_pos <= q_pos, 0.0, -jnp.inf)

    def o_copy(g, s):
        src = o_send.at[g, s]
        dst = o_all.at[:, pl.ds(pl.multiple_of(chip * wide_cols + g * HEAD, HEAD), HEAD)]
        return remote(src, dst, o_ssem.at[g, s - 1], o_rsem.at[g, s - 1], across[s])

    def finish(g):
        s = jnp.dot(newk[...], qt[g], preferred_element_type=jnp.float32) + hide[...]
        m_old = m_run[g]
        m_new = jnp.maximum(m_old, jnp.max(s, axis=0, keepdims=True))
        alpha = jnp.exp2((m_old - m_new) * scale2)
        p = jnp.exp2(s * scale2 - m_new * scale2)
        total = jnp.sum(l_run[g] * alpha, axis=0, keepdims=True) + jnp.sum(p, axis=0, keepdims=True)
        fresh = lax.dot_general(newv[...], p.astype(jnp.bfloat16), (((0,), (0,)), ((), ())),
                                preferred_element_type=jnp.float32)
        out = ((acc[g] * alpha + fresh) / total).T.astype(jnp.bfloat16)
        for s_i in range(1, CHIPS):
            o_send[g, s_i] = out[s_i * tok:(s_i + 1) * tok, :]
            o_copy(g, s_i).start()
        o_all[:, pl.ds(pl.multiple_of(chip * wide_cols + g * HEAD, HEAD), HEAD)] = out[:tok, :]

    def step(item, carry):
        nxt = item + 1

        if not resharded:
            @pl.when(nxt == GROUP + 4)
            def _():
                relay(2)

        @pl.when((nxt % GROUP == 0) & (nxt < n_items))
        def _():
            ready(nxt // GROUP)

        @pl.when(item == 2)
        def _():
            for c in kv_msgs:
                c.wait_recv()
            for c in new_copies:
                c.start()
            for s in range(CHIPS):
                newk[s * tok:(s + 1) * tok, :] = parts[s][GROUP]
                newv[s * tok:(s + 1) * tok, :] = parts[s][GROUP + 1]

        @pl.when(item == n_first)
        def _():
            for c in new_copies:
                c.wait_recv()
            for s in range(CHIPS):
                at = (CHIPS + s) * tok
                newk[at:at + tok, :] = peer_new[s, 0]
                newv[at:at + tok, :] = peer_new[s, 1]

        after = jnp.minimum(nxt, n_items - 1)

        @pl.when(item % 2 == 0)
        def _():
            score(after, s_odd, m_odd)
            absorb(item, s_even, m_even)

        @pl.when(item % 2 == 1)
        def _():
            score(after, s_even, m_even)
            absorb(item, s_odd, m_odd)

        @pl.when(item >= n_first)
        def _():
            finish(item - n_first)

        return carry

    lax.fori_loop(0, n_items, step, 0)
    o_copies = [o_copy(g, s) for g in range(GROUP) for s in range(1, CHIPS)]
    last = 3 * (GROUP - 1)
    wo_load.wait()
    for c in o_copies[:last]:
        c.wait_recv()

    def heads(s, first, count):
        at = pl.multiple_of((chip ^ s) * wide_cols + first * HEAD, HEAD)
        return pl.ds(at, count * HEAD)

    def early_proj(blk, carry):
        cols = pl.ds(pl.multiple_of(blk * COL, COL), COL)
        total = jnp.zeros((tok, COL), jnp.float32)
        for s in range(CHIPS):
            part = heads(s, 0, GROUP if s == 0 else GROUP - 1)
            total = total + jnp.dot(o_all[:, part], wo[part, cols], preferred_element_type=jnp.float32)
        y_acc[:, cols] = total
        return carry

    lax.fori_loop(0, wo.shape[1] // COL, early_proj, 0)
    for c in o_copies[last:]:
        c.wait_recv()

    def out_proj(blk, carry):
        cols = pl.ds(pl.multiple_of(blk * 2 * COL, 2 * COL), 2 * COL)
        total = y_acc[:, cols]
        for s in range(1, CHIPS):
            part = heads(s, GROUP - 1, 1)
            total = total + jnp.dot(o_all[:, part], wo[part, cols], preferred_element_type=jnp.float32)
        y = total.astype(jnp.bfloat16)
        if not resharded:
            y = (a_ref[:, cols].astype(jnp.float32) + y.astype(jnp.float32)).astype(jnp.bfloat16)
        y_ref[:, cols] = y
        return carry

    lax.fori_loop(0, wo.shape[1] // (2 * COL), out_proj, 0)

    for c in q_copies + kv_msgs + new_copies + o_copies:
        c.wait_send()
    if not resharded:
        for step in range(CHIPS):
            for which in range(2):
                pair_copy(step, which).wait_send()
                if step:
                    kv_copy(step, which).wait_send()


def run_layer(resharded, a, b_q, b_k, trig, k4, v4, k_in, v_in, w_q, w_k, w_v, w_o, collective_id):
    tok, width = a.shape
    chunk = k4.shape[1]
    rows = CHIPS * tok
    bf16, f32 = jnp.bfloat16, jnp.float32
    vmem = pl.BlockSpec(memory_space=pltpu.VMEM)
    hbm = pl.BlockSpec(memory_space=pl.ANY)
    dma = pltpu.SemaphoreType.DMA
    packed = [] if resharded else [jax.ShapeDtypeStruct(k4.shape, bf16)] * 2
    packing = [] if resharded else [
        pltpu.VMEM((RING, PIECE, KV_HEADS, HEAD), bf16),
        pltpu.VMEM((2, KV_HEADS, PIECE, HEAD), bf16),
        dma((RING,)), dma((2,)),
    ]
    return pl.pallas_call(
        functools.partial(layer_kernel, resharded),
        out_shape=[jax.ShapeDtypeStruct((tok, width), bf16),
                   jax.ShapeDtypeStruct((KV_HEADS, tok, HEAD), bf16),
                   jax.ShapeDtypeStruct((KV_HEADS, tok, HEAD), bf16)] + packed,
        in_specs=[vmem] * 3 + [hbm] * 9,
        out_specs=[vmem] * 3 + [hbm] * len(packed),
        scratch_shapes=[
            pltpu.VMEM((tok, width), bf16),
            pltpu.VMEM((tok, 2 * HEAD), f32),
            pltpu.VMEM((2,) + w_k.shape, bf16),
            pltpu.VMEM(w_o.shape, bf16),
            pltpu.VMEM((SLOTS, chunk, HEAD), bf16),
            pltpu.VMEM((SLOTS, chunk, HEAD), bf16),
            pltpu.VMEM((2, HEAD, 2 * chunk), bf16),
            pltpu.VMEM((KV_HEADS, GROUP + 2, tok, HEAD), bf16),
            pltpu.VMEM((CHIPS - 1, GROUP + 2, tok, HEAD), bf16),
            pltpu.VMEM((CHIPS, 2, tok, HEAD), bf16),
            pltpu.VMEM((2 * rows, HEAD), bf16),
            pltpu.VMEM((2 * rows, HEAD), bf16),
            pltpu.VMEM((GROUP, HEAD, rows), bf16),
            pltpu.VMEM((2 * chunk, rows), f32),
            pltpu.VMEM((2 * chunk, rows), f32),
            pltpu.VMEM((8, rows), f32),
            pltpu.VMEM((8, rows), f32),
            pltpu.VMEM((GROUP, HEAD, rows), f32),
            pltpu.VMEM((GROUP, 1, rows), f32),
            pltpu.VMEM((GROUP, 8, rows), f32),
            pltpu.VMEM((2 * rows, rows), f32),
            pltpu.VMEM((GROUP, CHIPS, tok, HEAD), bf16),
            pltpu.VMEM((tok, CHIPS * GROUP * HEAD), bf16),
            pltpu.VMEM((tok, width), f32),
            dma, dma((2 + CHIPS,)), dma, dma((2 * SLOTS,)),
            dma((CHIPS - 1, 2)), dma((CHIPS - 1, 2)), dma((CHIPS, 2)), dma((CHIPS, 2)),
            dma((CHIPS - 1,)), dma((CHIPS - 1,)), dma((CHIPS,)), dma((CHIPS,)),
            dma((GROUP, CHIPS - 1)), dma((GROUP, CHIPS - 1)), dma((CHIPS - 1,)), dma((CHIPS - 1,)),
            pltpu.VMEM((w_q.shape[1] // HEAD, HEAD), f32), pltpu.VMEM((KV_HEADS, HEAD), f32),
        ] + packing,
        compiler_params=pltpu.CompilerParams(collective_id=collective_id, has_side_effects=True, vmem_limit_bytes=VMEM_ALL),
        name="layer",
    )(a, b_q.reshape(-1, HEAD), b_k.reshape(-1, HEAD), trig, k4, v4, k_in, v_in, w_q, w_k, w_v, w_o)


def mlp_kernel(h_ref, k4_ref, v4_ref, gate_ref, up_ref, down_ref, g_ref, kout_ref, vout_ref,
               u, wg, wu, wd, acc, theirs, w_sem, u_send, u_recv, part_send, part_recv, kv_send, kv_recv, pair_send, pair_recv):
    chip, core, across, partner = peers()
    tok = h_ref.shape[0]
    n_buf = wg.shape[0]
    steps = gate_ref.shape[1] // (2 * COL)

    def copies(i):
        slot = i % n_buf
        cols = pl.ds(pl.multiple_of((core * steps + i) * COL, COL), COL)
        return (pltpu.make_async_copy(gate_ref.at[:, cols], wg.at[slot], w_sem.at[slot, 0]),
                pltpu.make_async_copy(up_ref.at[:, cols], wu.at[slot], w_sem.at[slot, 1]),
                pltpu.make_async_copy(down_ref.at[cols, :], wd.at[slot], w_sem.at[slot, 2]))

    for b in range(n_buf):
        for c in copies(b):
            c.start()
    meet(across[1:] + [partner])
    u[:tok, :] = norm_rows(h_ref[...].astype(jnp.float32))
    u_copy = remote(u.at[pl.ds(0, tok)], u.at[pl.ds(tok, tok)], u_send, u_recv, partner)
    u_copy.start()

    def kv_copy(step, which):
        src, dst = (k4_ref, kout_ref) if which == 0 else (v4_ref, vout_ref)
        return remote(src.at[chip ^ step], dst.at[2 * step], kv_send.at[step - 1, which], kv_recv.at[step - 1, which],
                      across[step])

    def pair_copy(step, which):
        dst = kout_ref if which == 0 else vout_ref
        src = (k4_ref if which == 0 else v4_ref).at[chip] if step == 0 else dst.at[2 * step]
        return remote(src, dst.at[2 * step + 1], pair_send.at[step, which], pair_recv.at[step, which], partner)

    for step in range(1, CHIPS):
        for which in range(2):
            kv_copy(step, which).start()
    for which in range(2):
        pair_copy(0, which).start()
    acc[...] = jnp.zeros_like(acc)
    u_copy.wait_recv()

    def relay(step):
        for which in range(2):
            kv_copy(step, which).wait_recv()
            pair_copy(step, which).start()

    def block(i, carry):
        slot = i % n_buf
        for c in copies(i):
            c.wait()
        gate = jnp.dot(u[...], wg[slot], preferred_element_type=jnp.float32).astype(jnp.bfloat16).astype(jnp.float32)
        up = jnp.dot(u[...], wu[slot], preferred_element_type=jnp.float32).astype(jnp.bfloat16).astype(jnp.float32)
        mixed = (gate * jax.nn.sigmoid(gate) * up).astype(jnp.bfloat16)
        acc[...] += jnp.dot(mixed, wd[slot], preferred_element_type=jnp.float32)

        @pl.when(i + n_buf < steps)
        def _():
            for c in copies(i + n_buf):
                c.start()

        @pl.when(i == steps - 12)
        def _():
            relay(1)
            relay(2)

        @pl.when(i == steps - 5)
        def _():
            relay(3)

        return carry

    lax.fori_loop(0, steps, block, 0)
    part_copy = remote(acc.at[pl.ds(tok, tok)], theirs, part_send, part_recv, partner)
    part_copy.start()
    part_copy.wait_recv()
    g_ref[...] = (h_ref[...].astype(jnp.float32) + (acc[:tok, :] + theirs[...])).astype(jnp.bfloat16)
    for step in range(CHIPS):
        for which in range(2):
            pair_copy(step, which).wait()
            if step:
                kv_copy(step, which).wait_send()
    u_copy.wait_send()
    part_copy.wait_send()


def run_mlp(h, k4, v4, w_gate, w_up, w_down, collective_id):
    tok, width = h.shape
    chunk = k4.shape[1]
    bf16, f32 = jnp.bfloat16, jnp.float32
    vmem = pl.BlockSpec(memory_space=pltpu.VMEM)
    hbm = pl.BlockSpec(memory_space=pl.ANY)
    dma = pltpu.SemaphoreType.DMA
    n_buf = 4
    slots = jax.ShapeDtypeStruct((SLOTS, chunk, HEAD), bf16)
    return pl.pallas_call(
        mlp_kernel,
        out_shape=[jax.ShapeDtypeStruct((tok, width), bf16), slots, slots],
        in_specs=[vmem] + [hbm] * 5,
        out_specs=[vmem, hbm, hbm],
        scratch_shapes=[
            pltpu.VMEM((2 * tok, width), bf16),
            pltpu.VMEM((n_buf, width, COL), bf16),
            pltpu.VMEM((n_buf, width, COL), bf16),
            pltpu.VMEM((n_buf, COL, width), bf16),
            pltpu.VMEM((2 * tok, width), f32),
            pltpu.VMEM((tok, width), f32),
            dma((n_buf, 3)), dma, dma, dma, dma,
            dma((CHIPS - 1, 2)), dma((CHIPS - 1, 2)), dma((CHIPS, 2)), dma((CHIPS, 2)),
        ],
        compiler_params=pltpu.CompilerParams(collective_id=collective_id, has_side_effects=True, vmem_limit_bytes=60 * MIB),
        name="mlp",
    )(h, k4, v4, w_gate, w_up, w_down)


def heads_first(cache):
    return lax.optimization_barrier(jnp.transpose(cache, (1, 0, 2)))


def order_kernel(g_ref, y_ref, *refs):
    g_out, y_out = refs[4:6]
    g_out[...] = g_ref[...]
    y_out[...] = y_ref[...]
    for src, dst in zip(refs[:4], refs[6:]):
        for c in range(KV_HEADS):
            dst[:, c, :] = src[c]


def order_outputs(hidden, y_two, *appends):
    tok = hidden.shape[0]
    rows = [jax.ShapeDtypeStruct(t.shape, t.dtype) for t in (hidden, y_two)]
    lines = [jax.ShapeDtypeStruct((tok, KV_HEADS, HEAD), t.dtype) for t in appends]
    vmem = pl.BlockSpec(memory_space=pltpu.VMEM)
    return pl.pallas_call(order_kernel, out_shape=rows + lines, in_specs=[vmem] * 6, out_specs=[vmem] * 6,
                          name="order_outputs")(hidden, y_two, *appends)


def solution(mesh):
    axis_size = mesh.shape['cp']
    rows_spec = P(('dp', 'cp'), None)
    cache_spec = P(('dp', 'cp'), None, None)
    mat_spec = P(None, None)
    vec_spec = P(None)
    layer_specs = (cache_spec, cache_spec, mat_spec, vec_spec, mat_spec, vec_spec, mat_spec, mat_spec)
    in_specs = (rows_spec,) + layer_specs + (mat_spec, mat_spec, mat_spec) + layer_specs
    out_specs = (rows_spec, rows_spec, cache_spec, cache_spec, cache_spec, cache_spec)

    def forward(x_in, cache_k1, cache_v1, w_q1, b_q1, w_k1, b_k1, w_v1, w_o1, w_gate, w_up, w_down, cache_k2, cache_v2, w_q2, b_q2, w_k2, b_k2, w_v2, w_o2):
        n_tok = axis_size * x_in.shape[0]
        trig = rope_table(axis_size * cache_k1.shape[0], n_tok)
        k4a, v4a = heads_first(cache_k1), heads_first(cache_v1)
        resid_h, k_one, v_one, k4b, v4b = run_layer(False, x_in, b_q1, b_k1, trig, k4a, v4a, cache_k2, cache_v2, w_q1, w_k1, w_v1, w_o1, 1)
        hidden, k_in, v_in = run_mlp(resid_h, k4b, v4b, w_gate, w_up, w_down, 2)
        y_two, k_two, v_two = run_layer(True, hidden, b_q2, b_k2, trig, k4b, v4b, k_in, v_in, w_q2, w_k2, w_v2, w_o2, 3)
        return order_outputs(hidden, y_two, k_one, v_one, k_two, v_two)

    return jax.shard_map(forward, mesh=mesh, in_specs=in_specs, out_specs=out_specs, check_vma=False)
```
